8 devices in a mesh: dp: 1 (over z), fsdp: 8 (over y, x, core).
Axes of the slice: x: 2, y: 2, z: 1, core: 2. Of those that a mesh axis runs over, the one named last changes fastest.
Arguments:
- tok_ids: int32 [48, 384], P(('dp', 'fsdp'))
- grad_out: bfloat16 [48, 384, 2048], P(('dp', 'fsdp'))
- emb_table: bfloat16 [163840, 2048], P('fsdp')
- norm_gain: bfloat16 [2048], P('fsdp')
- w_query: bfloat16 [2048, 3072], P('fsdp')
- w_kv_down: bfloat16 [2048, 576], P('fsdp')
- kv_gain: bfloat16 [512], P('fsdp')
- w_kv_up: bfloat16 [512, 4096], P('fsdp')
- w_out: bfloat16 [2048, 2048], P('fsdp')
Outputs:
- output 1: bfloat16 [48, 384, 2048], P(('dp', 'fsdp'))
- output 2: bfloat16 [163840, 2048], P(('dp', 'fsdp'))
- output 3: float32 [2048], P(('dp', 'fsdp'))
- output 4: float32 [2048, 3072], P(('dp', 'fsdp'))
- output 5: float32 [2048, 576], P(('dp', 'fsdp'))
- output 6: float32 [512], P(('dp', 'fsdp'))
- output 7: float32 [512, 4096], P(('dp', 'fsdp'))
- output 8: float32 [2048, 2048], P(('dp', 'fsdp'))
All inputs are finite; a program needn't handle non-finite values.
Results may differ from the reference program's by a relative error of at most 0.011954.
Values are sent between devices in bfloat16 or wider.
A program may use at most 1 GiB of HBM per device.

```python
import math
import jax
import jax.numpy as jnp
from jax import lax

D_MODEL = 2048
N_HEADS = 16
VOCAB_SIZE = 163840
KV_RANK = 512
BATCH_SEQS = 48
SEQ_LEN = 384
NOPE_DIM = 128
ROPE_DIM = 64
VALUE_DIM = 128
HOT_IDS = 64
ROPE_THETA = 50000.0
RMS_EPS = 1e-6
ATTN_SCALE = (NOPE_DIM + ROPE_DIM) ** -0.5 * (0.1 * math.log(32.0) + 1.0) ** 2


def draw_ids(id_key):
    tok_count = BATCH_SEQS * SEQ_LEN
    kind_key, hot_key, mid_key, any_key = jax.random.split(id_key, 4)
    id_kind = jax.random.randint(kind_key, (tok_count,), 0, 4)
    hot_draw = jax.random.randint(hot_key, (tok_count,), 0, HOT_IDS)
    mid_draw = jax.random.randint(mid_key, (tok_count,), 0, VOCAB_SIZE // 8)
    any_draw = jax.random.randint(any_key, (tok_count,), 0, VOCAB_SIZE)
    tok_list = jnp.where(id_kind == 0, hot_draw, jnp.where(id_kind == 1, mid_draw, any_draw))
    tok_list = tok_list.at[0].set(VOCAB_SIZE - 1).at[1].set(0)
    return tok_list.reshape(BATCH_SEQS, SEQ_LEN).astype(jnp.int32)


def setup_inputs(seed: int = 0, part: int = 0) -> dict:
    base_key = jax.random.key(seed)
    shared = jax.random.split(base_key, 7)
    part_keys = jax.random.split(jax.random.fold_in(base_key, part), 2)
    q_width = N_HEADS * (NOPE_DIM + ROPE_DIM)
    up_width = N_HEADS * (NOPE_DIM + VALUE_DIM)
    o_width = N_HEADS * VALUE_DIM
    emb_table = jax.random.normal(shared[0], (VOCAB_SIZE, D_MODEL), jnp.float32).astype(jnp.bfloat16)
    norm_gain = (1.0 + 0.3 * jax.random.normal(shared[1], (D_MODEL,), jnp.float32)).astype(jnp.bfloat16)
    w_query = (jax.random.normal(shared[2], (D_MODEL, q_width), jnp.float32) * D_MODEL ** -0.5).astype(jnp.bfloat16)
    w_kv_down = (jax.random.normal(shared[3], (D_MODEL, KV_RANK + ROPE_DIM), jnp.float32) * D_MODEL ** -0.5).astype(jnp.bfloat16)
    kv_gain = (1.0 + 0.3 * jax.random.normal(shared[4], (KV_RANK,), jnp.float32)).astype(jnp.bfloat16)
    w_kv_up = (jax.random.normal(shared[5], (KV_RANK, up_width), jnp.float32) * KV_RANK ** -0.5).astype(jnp.bfloat16)
    w_out = (jax.random.normal(shared[6], (o_width, D_MODEL), jnp.float32) * o_width ** -0.5).astype(jnp.bfloat16)
    tok_ids = draw_ids(part_keys[0])
    grad_out = jax.random.normal(part_keys[1], (BATCH_SEQS, SEQ_LEN, D_MODEL), jnp.float32).astype(jnp.bfloat16)
    return {'tok_ids': tok_ids, 'grad_out': grad_out, 'emb_table': emb_table, 'norm_gain': norm_gain, 'w_query': w_query, 'w_kv_down': w_kv_down, 'kv_gain': kv_gain, 'w_kv_up': w_kv_up, 'w_out': w_out}


def rms_scale(in_vals, gain_vec):
    vals_f32 = in_vals.astype(jnp.float32)
    inv_rms = lax.rsqrt(jnp.mean(vals_f32 * vals_f32, axis=-1, keepdims=True) + RMS_EPS)
    return (vals_f32 * inv_rms * gain_vec.astype(jnp.float32)).astype(jnp.bfloat16)


def rope_tables():
    positions = jnp.arange(SEQ_LEN, dtype=jnp.float32)
    inv_freq = ROPE_THETA ** (-2.0 * jnp.arange(ROPE_DIM // 2, dtype=jnp.float32) / ROPE_DIM)
    rot_angle = positions[:, None] * inv_freq[None, :]
    rot_angle = jnp.concatenate([rot_angle, rot_angle], axis=-1)
    return jnp.cos(rot_angle), jnp.sin(rot_angle)


def apply_rope(in_vals, cos_tab, sin_tab):
    half_dim = ROPE_DIM // 2
    vals_f32 = in_vals.astype(jnp.float32)
    turned = jnp.concatenate([-vals_f32[..., half_dim:], vals_f32[..., :half_dim]], axis=-1)
    return (vals_f32 * cos_tab + turned * sin_tab).astype(jnp.bfloat16)


def attend_one(q_seq, pe_seq, kv_seq):
    cos_tab, sin_tab = rope_tables()
    q_rot = apply_rope(q_seq[:, :, NOPE_DIM:], cos_tab[:, None, :], sin_tab[:, None, :])
    k_rot = apply_rope(pe_seq, cos_tab, sin_tab)
    scores = jnp.einsum('shd,thd->hst', q_seq[:, :, :NOPE_DIM].astype(jnp.float32), kv_seq[:, :, :NOPE_DIM].astype(jnp.float32))
    scores = scores + jnp.einsum('shd,td->hst', q_rot.astype(jnp.float32), k_rot.astype(jnp.float32))
    positions = jnp.arange(SEQ_LEN)
    causal = positions[:, None] >= positions[None, :]
    scores = jnp.where(causal[None, :, :], scores * ATTN_SCALE, -1e30)
    attn_probs = jax.nn.softmax(scores, axis=-1).astype(jnp.bfloat16)
    attn_mix = jnp.einsum('hst,thd->shd', attn_probs.astype(jnp.float32), kv_seq[:, :, NOPE_DIM:].astype(jnp.float32))
    return attn_mix.astype(jnp.bfloat16).reshape(SEQ_LEN, N_HEADS * VALUE_DIM)


def block_forward(rows_f32, gain_vec, w_query_f, w_down_f, kv_gain_vec, w_up_f, w_out_f):
    normed = rms_scale(rows_f32, gain_vec)
    q_proj = jnp.dot(normed.astype(jnp.float32), w_query_f, preferred_element_type=jnp.float32).astype(jnp.bfloat16)
    kv_down = jnp.dot(normed.astype(jnp.float32), w_down_f, preferred_element_type=jnp.float32).astype(jnp.bfloat16)
    latent = rms_scale(kv_down[:, :KV_RANK], kv_gain_vec)
    kv_up = jnp.dot(latent.astype(jnp.float32), w_up_f, preferred_element_type=jnp.float32).astype(jnp.bfloat16)
    seq_parts = (q_proj.reshape(BATCH_SEQS, SEQ_LEN, N_HEADS, NOPE_DIM + ROPE_DIM), kv_down[:, KV_RANK:].reshape(BATCH_SEQS, SEQ_LEN, ROPE_DIM), kv_up.reshape(BATCH_SEQS, SEQ_LEN, N_HEADS, NOPE_DIM + VALUE_DIM))
    attn_mix = lax.map(jax.checkpoint(lambda seq_item: attend_one(*seq_item)), seq_parts)
    attn_out = jnp.dot(attn_mix.reshape(BATCH_SEQS * SEQ_LEN, N_HEADS * VALUE_DIM).astype(jnp.float32), w_out_f, preferred_element_type=jnp.float32)
    return rows_f32 + attn_out


def reference(tok_ids, grad_out, emb_table, norm_gain, w_query, w_kv_down, kv_gain, w_kv_up, w_out):
    flat_ids = tok_ids.reshape(BATCH_SEQS * SEQ_LEN)
    rows_f32 = jnp.take(emb_table, flat_ids, axis=0).astype(jnp.float32)
    weight_list = tuple(weight_arr.astype(jnp.float32) for weight_arr in (norm_gain, w_query, w_kv_down, kv_gain, w_kv_up, w_out))
    out_f32, pullback = jax.vjp(block_forward, rows_f32, *weight_list)
    grad_list = pullback(grad_out.reshape(BATCH_SEQS * SEQ_LEN, D_MODEL).astype(jnp.float32))
    grad_table = jax.ops.segment_sum(grad_list[0], flat_ids, num_segments=VOCAB_SIZE).astype(jnp.bfloat16)
    block_out = out_f32.astype(jnp.bfloat16).reshape(BATCH_SEQS, SEQ_LEN, D_MODEL)
    return (block_out, grad_table, grad_list[1], grad_list[2], grad_list[3], grad_list[4], grad_list[5], grad_list[6])
```

```python
import functools
import math
import jax
import jax.numpy as jnp
import numpy as np
from jax import lax
from jax.experimental import pallas as pl
from jax.experimental.pallas import tpu as pltpu
from jax.sharding import PartitionSpec as P

NOPE_DIM = 128
ROPE_DIM = 64
VALUE_DIM = 128
ROPE_THETA = 50000.0
RMS_EPS = 1e-6
ATTN_SCALE = (NOPE_DIM + ROPE_DIM) ** -0.5 * (0.1 * math.log(32.0) + 1.0) ** 2
ROW_DIMS = (((0,), (0,)), ((), ()))
COL_DIMS = (((1,), (1,)), ((), ()))
LANES = 128
TABLE_BLOCK = 256
PICK_CHUNK = 32
PICK_RING = 4
ADD_CHUNK = 16
ADD_RING = 3
NO_ROW = 1 << 30
F32 = jnp.float32
BF16 = jnp.bfloat16
SMEM = pltpu.SMEM
ANY = pl.ANY


def params(vmem_mib, **kw):
    return pltpu.CompilerParams(vmem_limit_bytes=vmem_mib << 20, **kw)


def unique_body(shift, keys_ref, uniq_ref, rank_ref, count_ref):
    n = keys_ref.shape[0]
    unroll = 8

    def step(i, carry):
        k, prev = carry
        for j in range(unroll):
            key = keys_ref[i * unroll + j]
            row = lax.shift_right_logical(key, shift)
            k = k + (row != prev).astype(jnp.int32)
            uniq_ref[k] = row
            rank_ref[key & ((1 << shift) - 1)] = k
            prev = row
        return k, prev

    k, _ = lax.fori_loop(0, n // unroll, step, (jnp.int32(-1), jnp.int32(-1)))
    count_ref[0] = k + 1


def unique_rows(ids):
    n = ids.shape[0]
    shift = max(1, (n - 1).bit_length())
    keys = lax.sort(ids * (1 << shift) + jnp.arange(n, dtype=jnp.int32))
    smem = pl.BlockSpec(memory_space=SMEM)
    uniq, rank, count = pl.pallas_call(
        functools.partial(unique_body, shift),
        out_shape=[jax.ShapeDtypeStruct((n,), jnp.int32), jax.ShapeDtypeStruct((n,), jnp.int32), jax.ShapeDtypeStruct((1,), jnp.int32)],
        in_specs=[smem], out_specs=[smem] * 3, name="unique_rows")(keys)
    return jnp.where(jnp.arange(n, dtype=jnp.int32) < count[0], uniq, NO_ROW), rank


def pick_body(n_dev, n_tok, rows_ref, edge_ref, table_ref, out_ref, lin_ref, stage_ref, sems):
    b = pl.program_id(0)
    n_blk = pl.num_programs(0)
    rows_blk, d_model = table_ref.shape
    cols = d_model // LANES
    n_edge = edge_ref.shape[0] // n_dev

    def chunk_copy(d, k):
        slot = lax.rem(k, PICK_RING)
        return pltpu.make_async_copy(
            stage_ref.at[d, pl.ds(slot * PICK_CHUNK, PICK_CHUNK)],
            out_ref.at[pl.ds(d * n_tok + k * PICK_CHUNK, PICK_CHUNK)],
            sems.at[d, slot])

    @pl.loop(0, rows_blk // 16)
    def _(g):
        for j in range(cols):
            lin_ref[pl.ds(g * 16 * cols + j, 16, stride=cols), :] = table_ref[pl.ds(g * 16, 16), j * LANES:(j + 1) * LANES].astype(F32)

    @pl.loop(0, n_dev)
    def _(d):
        first = edge_ref[d * n_edge]
        lo = edge_ref[d * n_edge + b] - first
        hi = edge_ref[d * n_edge + b + 1] - first

        @pl.when(hi > lo)
        def _():
            @pl.loop(lo // PICK_CHUNK, (hi - 1) // PICK_CHUNK + 1)
            def _(k):
                start = jnp.maximum(lo, k * PICK_CHUNK)
                stop = jnp.minimum(hi, (k + 1) * PICK_CHUNK)

                @pl.when((start == k * PICK_CHUNK) & (k >= PICK_RING))
                def _():
                    chunk_copy(d, k - PICK_RING).wait()

                @pl.loop(start, stop)
                def _(p):
                    row = rows_ref[d * n_tok + first + p] - b * rows_blk
                    vals = lin_ref[pl.ds(pl.multiple_of(row * cols, cols), cols), :]
                    stage_ref[d, lax.rem(p, PICK_RING * PICK_CHUNK)] = vals.astype(BF16)

                @pl.when(stop == (k + 1) * PICK_CHUNK)
                def _():
                    chunk_copy(d, k).start()

    @pl.when(b == n_blk - 1)
    def _():
        @pl.loop(0, n_dev)
        def _(d):
            total = edge_ref[d * n_edge + n_blk] - edge_ref[d * n_edge]
            chunks = (total + PICK_CHUNK - 1) // PICK_CHUNK

            @pl.when(lax.rem(total, PICK_CHUNK) != 0)
            def _():
                chunk_copy(d, chunks - 1).start()

            @pl.loop(jnp.maximum(chunks - PICK_RING, 0), chunks)
            def _(k):
                chunk_copy(d, k).wait()


def pick_rows(table, rows, edges):
    n_dev, n_tok = rows.shape
    n_rows, d_model = table.shape
    cols = d_model // LANES
    return pl.pallas_call(
        functools.partial(pick_body, n_dev, n_tok),
        grid_spec=pltpu.PrefetchScalarGridSpec(
            num_scalar_prefetch=2, grid=(n_rows // TABLE_BLOCK,),
            in_specs=[pl.BlockSpec((TABLE_BLOCK, d_model), lambda b, *_: (b, 0))],
            out_specs=pl.BlockSpec(memory_space=ANY),
            scratch_shapes=[
                pltpu.VMEM((TABLE_BLOCK * cols, LANES), F32),
                pltpu.VMEM((n_dev, PICK_RING * PICK_CHUNK, cols, LANES), BF16),
                pltpu.SemaphoreType.DMA((n_dev, PICK_RING))]),
        out_shape=jax.ShapeDtypeStruct((n_dev * n_tok, cols, LANES), BF16),
        compiler_params=params(32), name="pick_rows",
        cost_estimate=pl.CostEstimate(flops=60_000_000, bytes_accessed=table.size * 2, transcendentals=0),
    )(rows.reshape(-1), edges.reshape(-1), table)


def spread_body(rank_ref, slot_ref, recv_ref, gain_ref, h0_ref, x_ref, lin_ref):
    i = pl.program_id(0)
    rows_blk, d_model = h0_ref.shape
    cols = d_model // LANES
    unroll = 8

    @pl.loop(0, rows_blk // unroll)
    def _(t0):
        for u in range(unroll):
            t = t0 * unroll + u
            lin_ref[pl.ds(pl.multiple_of(t * cols, cols), cols), :] = recv_ref[slot_ref[rank_ref[i * rows_blk + t]]].astype(F32)

    @pl.loop(0, rows_blk // 16)
    def _(g):
        tiles = [lin_ref[pl.ds(g * 16 * cols + j, 16, stride=cols), :] for j in range(cols)]
        square = tiles[0] * tiles[0]
        for v in tiles[1:]:
            square = square + v * v
        inv = lax.rsqrt(jnp.sum(square, axis=-1, keepdims=True) * (1.0 / d_model) + RMS_EPS)
        for j, v in enumerate(tiles):
            at = (pl.ds(g * 16, 16), slice(j * LANES, (j + 1) * LANES))
            h0_ref[at] = v.astype(BF16)
            x_ref[at] = (v * inv * gain_ref[:, j * LANES:(j + 1) * LANES]).astype(BF16)


def spread_rows(recv, rank, slot, gain):
    n_tok, cols, _ = recv.shape
    d_model = cols * LANES
    blk = 128
    out = jax.ShapeDtypeStruct((n_tok, d_model), BF16)
    row_spec = pl.BlockSpec((blk, d_model), lambda i, *_: (i, 0))
    return pl.pallas_call(
        spread_body,
        grid_spec=pltpu.PrefetchScalarGridSpec(
            num_scalar_prefetch=2, grid=(n_tok // blk,),
            in_specs=[pl.BlockSpec((n_tok, cols, LANES), lambda i, *_: (0, 0, 0), pipeline_mode=pl.Buffered(1)),
                      pl.BlockSpec((1, d_model), lambda i, *_: (0, 0))],
            out_specs=[row_spec, row_spec],
            scratch_shapes=[pltpu.VMEM((blk * cols, LANES), F32)]),
        out_shape=[out, out], compiler_params=params(32), name="spread_rows",
        cost_estimate=pl.CostEstimate(flops=60_000_000, bytes_accessed=n_tok * d_model * 6, transcendentals=0),
    )(rank, slot, recv, gain.reshape(1, d_model))


def rope_tables(seq_len):
    pos = np.arange(seq_len, dtype=np.float32)
    inv_freq = (np.float32(ROPE_THETA) ** (np.float32(-2.0) * np.arange(ROPE_DIM // 2, dtype=np.float32) / np.float32(ROPE_DIM))).astype(np.float32)
    angle = (pos[:, None] * inv_freq[None, :]).astype(np.float32).astype(np.float64)
    cos, sin, zero = np.cos(angle), np.sin(angle), np.zeros_like(angle)
    full = lambda lo, hi: np.concatenate([lo, hi, lo, hi], axis=1).astype(np.float32)
    return full(cos, cos), full(-sin, zero), full(zero, sin)


def turn(vals, cos, sin_lo, sin_hi, sign):
    half = ROPE_DIM // 2
    return vals * cos + sign * (pltpu.roll(vals, LANES - half, 1) * sin_lo + pltpu.roll(vals, half, 1) * sin_hi)


def attn_body(q_ref, pe_ref, kv_ref, do_ref, cos_ref, sin_lo_ref, sin_hi_ref,
              o_ref, dq_ref, dkv_ref, dpe_ref, krot_ref, dk_ref, dv_ref, dkrot_ref):
    pair = pl.program_id(1)
    seq_len = q_ref.shape[0]
    blk = 128
    low = lax.broadcasted_iota(jnp.int32, (1, LANES), 1) < ROPE_DIM

    @pl.when(pair == 0)
    def _():
        pe = pe_ref[...].astype(F32)
        pe = jnp.where(low, pe, pltpu.roll(pe, ROPE_DIM, 1))
        krot_ref[...] = turn(pe, cos_ref[...], sin_lo_ref[...], sin_hi_ref[...], 1.0).astype(BF16)
        dkrot_ref[...] = jnp.zeros_like(dkrot_ref)

    qrot = turn(q_ref[:, 2 * LANES:].astype(F32), cos_ref[...], sin_lo_ref[...], sin_hi_ref[...], 1.0)
    krot = krot_ref[...]
    causal = lax.broadcasted_iota(jnp.int32, (blk, blk), 0) >= lax.broadcasted_iota(jnp.int32, (blk, blk), 1)
    dqrots = []
    for h in range(2):
        mine = low if h == 0 else ~low
        qcat = jnp.concatenate([q_ref[:, h * LANES:(h + 1) * LANES], jnp.where(mine, qrot, 0.0).astype(BF16)], axis=1)
        kcat = jnp.concatenate([kv_ref[:, 2 * h * LANES:(2 * h + 1) * LANES], krot], axis=1)
        val = kv_ref[:, (2 * h + 1) * LANES:(2 * h + 2) * LANES]
        dout = do_ref[:, h * LANES:(h + 1) * LANES]
        dqrot = []
        for i in reversed(range(seq_len // blk)):
            here, seen = slice(i * blk, (i + 1) * blk), (i + 1) * blk
            s = lax.dot_general(qcat[here], kcat[:seen], COL_DIMS, preferred_element_type=F32) * ATTN_SCALE
            diag = jnp.where(causal, s[:, i * blk:], -1e30)
            s = diag if i == 0 else jnp.concatenate([s[:, :i * blk], diag], axis=1)
            e = jnp.exp(s - jnp.max(s, axis=-1, keepdims=True))
            p = e * (1.0 / jnp.sum(e, axis=-1, keepdims=True))
            pb = p.astype(BF16)
            o_ref[here, h * LANES:(h + 1) * LANES] = jnp.dot(pb, val[:seen], preferred_element_type=F32).astype(BF16)
            dp = lax.dot_general(dout[here], val[:seen], COL_DIMS, preferred_element_type=F32)
            ds = (p * (dp - jnp.sum(dp * p, axis=-1, keepdims=True)) * ATTN_SCALE).astype(BF16)
            dqi = jnp.dot(ds, kcat[:seen], preferred_element_type=F32)
            dq_ref[here, h * LANES:(h + 1) * LANES] = dqi[:, :LANES].astype(BF16)
            dqrot.append(dqi[:, LANES:])
            dvi = lax.dot_general(pb, dout[here], ROW_DIMS, preferred_element_type=F32)
            dki = lax.dot_general(ds, qcat[here], ROW_DIMS, preferred_element_type=F32)
            if seen == seq_len:
                dv_ref[...] = dvi
                dk_ref[...] = dki
            else:
                dv_ref[:seen] += dvi
                dk_ref[:seen] += dki
        dqrots.append(jnp.concatenate(dqrot[::-1], axis=0))
        dkv_ref[:, 2 * h * LANES:(2 * h + 1) * LANES] = dk_ref[:, :LANES].astype(BF16)
        dkv_ref[:, (2 * h + 1) * LANES:(2 * h + 2) * LANES] = dv_ref[...].astype(BF16)
        dkrot_ref[...] += dk_ref[:, LANES:]
    dqr = jnp.where(low, dqrots[0], dqrots[1]).astype(BF16).astype(F32)
    dq_ref[:, 2 * LANES:] = turn(dqr, cos_ref[...], sin_lo_ref[...], sin_hi_ref[...], -1.0).astype(BF16)

    @pl.when(pair == pl.num_programs(1) - 1)
    def _():
        both = dkrot_ref[...]
        both = (both + pltpu.roll(both, ROPE_DIM, 1)).astype(BF16).astype(F32)
        dpe = turn(both, cos_ref[...], sin_lo_ref[...], sin_hi_ref[...], -1.0)
        dpe_ref[...] = jnp.where(low, dpe, 0.0).astype(BF16)


def attend(qx, kv, d_mix, seq_count, pe_block):
    tok = qx.shape[0]
    seq_len = tok // seq_count
    pairs = d_mix.shape[1] // (2 * VALUE_DIM)
    tabs = [jnp.asarray(t) for t in rope_tables(seq_len)]
    at = lambda width: pl.BlockSpec((seq_len, width), lambda s, j: (s, j))
    tab = pl.BlockSpec((seq_len, LANES), lambda s, j: (0, 0))
    shape = lambda w: jax.ShapeDtypeStruct((tok, w), BF16)
    return pl.pallas_call(
        attn_body, grid=(seq_count, pairs),
        in_specs=[at(3 * LANES), pl.BlockSpec((seq_len, LANES), lambda s, j: (s, pe_block)), at(4 * LANES), at(2 * LANES), tab, tab, tab],
        out_specs=[at(2 * LANES), at(3 * LANES), at(4 * LANES), pl.BlockSpec((seq_len, LANES), lambda s, j: (s, 0))],
        out_shape=[shape(pairs * 2 * LANES), shape(pairs * 3 * LANES), shape(pairs * 4 * LANES), shape(LANES)],
        scratch_shapes=[pltpu.VMEM((seq_len, LANES), BF16), pltpu.VMEM((seq_len, 2 * LANES), F32),
                        pltpu.VMEM((seq_len, LANES), F32), pltpu.VMEM((seq_len, LANES), F32)],
        compiler_params=params(40), name="attention",
        cost_estimate=pl.CostEstimate(flops=tok * seq_len * pairs * 2 * 7 * 256, bytes_accessed=tok * pairs * 128 * 2 * 18, transcendentals=0),
    )(qx, qx, kv, d_mix, *tabs)


def merge_body(rank_ref, slot_ref, dx_ref, h0_ref, dy_ref, gain_ref, out_ref, dgain_ref, lin_ref, acc_ref, gacc_ref, sem):
    i = pl.program_id(0)
    rows_blk, d_model = h0_ref.shape
    cols = d_model // LANES

    @pl.when(i == 0)
    def _():
        gacc_ref[...] = jnp.zeros_like(gacc_ref)

        @pl.loop(0, acc_ref.shape[0] // 8)
        def _(r):
            acc_ref[pl.ds(r * 8, 8)] = jnp.zeros((8,) + acc_ref.shape[1:], F32)

    @pl.loop(0, rows_blk // 16)
    def _(g):
        rows = pl.ds(g * 16, 16)
        lanes = [slice(j * LANES, (j + 1) * LANES) for j in range(cols)]
        square, cross = jnp.zeros((16, LANES), F32), jnp.zeros((16, LANES), F32)
        for at in lanes:
            v = h0_ref[rows, at].astype(F32)
            square = square + v * v
            cross = cross + v * (dx_ref[rows, at].astype(F32) * gain_ref[:, at])
        inv = lax.rsqrt(jnp.sum(square, axis=-1, keepdims=True) * (1.0 / d_model) + RMS_EPS)
        mean = jnp.sum(cross, axis=-1, keepdims=True) * inv * (1.0 / d_model)
        for j, at in enumerate(lanes):
            hat = h0_ref[rows, at].astype(F32) * inv
            w = dx_ref[rows, at].astype(F32)
            gacc_ref[:, at] += w * hat
            lin_ref[pl.ds(j, 16, stride=cols), :] = inv * (w * gain_ref[:, at] - hat * mean) + dy_ref[rows, at].astype(F32)
        for t in range(16):
            r = slot_ref[rank_ref[i * rows_blk + g * 16 + t]]
            acc_ref[r] = acc_ref[r] + lin_ref[pl.ds(t * cols, cols), :]

    @pl.when(i == pl.num_programs(0) - 1)
    def _():
        dgain_ref[...] = jnp.sum(gacc_ref[...], axis=0, keepdims=True)
        copy = pltpu.make_async_copy(acc_ref, out_ref, sem)
        copy.start()
        copy.wait()


def merge_rows(dx, h0, dy, gain, rank, slot):
    n_tok, d_model = h0.shape
    cols = d_model // LANES
    blk = 128
    row_spec = pl.BlockSpec((blk, d_model), lambda i, *_: (i, 0))
    return pl.pallas_call(
        merge_body,
        grid_spec=pltpu.PrefetchScalarGridSpec(
            num_scalar_prefetch=2, grid=(n_tok // blk,),
            in_specs=[row_spec, row_spec, row_spec, pl.BlockSpec((1, d_model), lambda i, *_: (0, 0))],
            out_specs=[pl.BlockSpec(memory_space=ANY), pl.BlockSpec((1, d_model), lambda i, *_: (0, 0))],
            scratch_shapes=[pltpu.VMEM((16 * cols, LANES), F32), pltpu.VMEM((n_tok, cols, LANES), F32),
                            pltpu.VMEM((16, d_model), F32), pltpu.SemaphoreType.DMA]),
        out_shape=[jax.ShapeDtypeStruct((n_tok, cols, LANES), F32), jax.ShapeDtypeStruct((1, d_model), F32)],
        compiler_params=params(40), name="merge_rows",
        cost_estimate=pl.CostEstimate(flops=100_000_000, bytes_accessed=n_tok * d_model * 10, transcendentals=0),
    )(rank, slot, dx, h0, dy, gain.reshape(1, d_model))


def add_body(n_dev, n_tok, rows_ref, edge_ref, recv_ref, out_ref, acc_ref, ring_ref, sems):
    b = pl.program_id(0)
    n_blk = pl.num_programs(0)
    rows_blk, d_model = out_ref.shape
    cols = d_model // LANES
    n_edge = edge_ref.shape[0] // n_dev

    def chunk_copy(s, k):
        slot = lax.rem(k, ADD_RING)
        return pltpu.make_async_copy(recv_ref.at[pl.ds(s * n_tok + k * ADD_CHUNK, ADD_CHUNK)],
                                     ring_ref.at[s, pl.ds(slot * ADD_CHUNK, ADD_CHUNK)], sems.at[s, slot])

    def chunks_of(s):
        return (edge_ref[s * n_edge + n_blk] - edge_ref[s * n_edge] + ADD_CHUNK - 1) // ADD_CHUNK

    @pl.when(b == 0)
    def _():
        @pl.loop(0, n_dev)
        def _(s):
            @pl.loop(0, jnp.minimum(chunks_of(s), ADD_RING))
            def _(k):
                chunk_copy(s, k).start()

    @pl.loop(0, rows_blk * cols // 64)
    def _(r):
        acc_ref[pl.ds(r * 64, 64), :] = jnp.zeros((64, LANES), F32)

    @pl.loop(0, n_dev)
    def _(s):
        first = edge_ref[s * n_edge]
        lo = edge_ref[s * n_edge + b] - first
        hi = edge_ref[s * n_edge + b + 1] - first

        @pl.when(hi > lo)
        def _():
            @pl.loop(lo // ADD_CHUNK, (hi - 1) // ADD_CHUNK + 1)
            def _(k):
                start = jnp.maximum(lo, k * ADD_CHUNK)
                stop = jnp.minimum(hi, (k + 1) * ADD_CHUNK)

                @pl.when(start == k * ADD_CHUNK)
                def _():
                    chunk_copy(s, k).wait()

                @pl.loop(start, stop)
                def _(p):
                    row = rows_ref[s * n_tok + first + p] - b * rows_blk
                    at = pl.ds(pl.multiple_of(row * cols, cols), cols)
                    acc_ref[at, :] += ring_ref[s, lax.rem(p, ADD_RING * ADD_CHUNK)]

                @pl.when((stop == (k + 1) * ADD_CHUNK) & (k + ADD_RING < chunks_of(s)))
                def _():
                    chunk_copy(s, k + ADD_RING).start()

    @pl.loop(0, rows_blk // 16)
    def _(g):
        for j in range(cols):
            out_ref[pl.ds(g * 16, 16), j * LANES:(j + 1) * LANES] = acc_ref[pl.ds(g * 16 * cols + j, 16, stride=cols), :].astype(BF16)


def add_rows(recv, rows, edges, n_rows):
    n_dev, n_tok = rows.shape
    cols = recv.shape[1]
    d_model = cols * LANES
    return pl.pallas_call(
        functools.partial(add_body, n_dev, n_tok),
        grid_spec=pltpu.PrefetchScalarGridSpec(
            num_scalar_prefetch=2, grid=(n_rows // TABLE_BLOCK,),
            in_specs=[pl.BlockSpec(memory_space=ANY)],
            out_specs=pl.BlockSpec((TABLE_BLOCK, d_model), lambda b, *_: (b, 0)),
            scratch_shapes=[pltpu.VMEM((TABLE_BLOCK * cols, LANES), F32),
                            pltpu.VMEM((n_dev, ADD_RING * ADD_CHUNK, cols, LANES), F32),
                            pltpu.SemaphoreType.DMA((n_dev, ADD_RING))]),
        out_shape=jax.ShapeDtypeStruct((n_rows, d_model), BF16),
        compiler_params=params(32), name="add_rows",
        cost_estimate=pl.CostEstimate(flops=60_000_000, bytes_accessed=n_rows * d_model * 2, transcendentals=0),
    )(rows.reshape(-1), edges.reshape(-1), recv)


def exchange_body(caps, tok, fetch, x_ref, out_ref, via_ref, send_sems, recv_sems, hop_send, hop_recv, end_send, end_recv, own_sem):
    n_dev = len(caps)
    offs = [sum(caps[:o]) for o in range(n_dev)]
    place = lax.axis_index('fsdp')
    far, side = 6, 4
    across = lambda m: [((m ^ far) & ~1) | c for c in range(2)]

    def rows(src, dst):
        if fetch:
            return dst * tok, offs[src], caps[src]
        return offs[dst], src * tok, caps[dst]

    def remote(src, dst, sems, to):
        return pltpu.make_async_remote_copy(src, dst, sems[0], sems[1], device_id={'fsdp': to}, device_id_type=pl.DeviceIdType.MESH)

    def direct(src, dst):
        at, to, n = rows(src, dst)
        n = n // 2 if (src ^ dst) & far == far else n
        return remote(x_ref.at[pl.ds(at, n)], out_ref.at[pl.ds(to, n)], (send_sems.at[dst], recv_sems.at[src]), dst)

    def hop(src, dst):
        at, _, n = rows(src, dst)
        c = dst & 1
        return remote(x_ref.at[pl.ds(at + n // 2, n - n // 2)], via_ref.at[c, pl.ds(0, n - n // 2)], (hop_send.at[c], hop_recv.at[c]), src ^ side)

    def end(src, dst):
        _, to, n = rows(src, dst)
        return remote(via_ref.at[dst & 1, pl.ds(0, n - n // 2)], out_ref.at[pl.ds(to + n // 2, n - n // 2)], (end_send.at[dst & 1], end_recv.at[src & 1]), dst)

    for m in range(n_dev):
        @pl.when(place == m)
        def _():
            for dst in across(m):
                hop(m, dst).start()
            for k in (6, 7, 4, 5, 2, 3, 1):
                direct(m, m ^ k).start()
            at, to, n = rows(m, m)
            own = pltpu.make_async_copy(x_ref.at[pl.ds(at, n)], out_ref.at[pl.ds(to, n)], own_sem)
            own.start()
            for dst in across(m ^ side):
                hop(m ^ side, dst).wait_recv()
                end(m ^ side, dst).start()
            own.wait()
            for dst in across(m):
                hop(m, dst).wait_send()
            for k in range(1, n_dev):
                direct(m, m ^ k).wait_send()
                direct(m ^ k, m).wait_recv()
            for dst in across(m ^ side):
                end(m ^ side, dst).wait_send()
            for src in across(m):
                end(src, m).wait_recv()


def exchange(x, caps, tok, fetch):
    n_dev = len(caps)
    cols = x.shape[1:]
    n_out = tok if fetch and sum(caps) <= tok else n_dev * tok
    hbm = pl.BlockSpec(memory_space=ANY)
    pair = pltpu.SemaphoreType.DMA((2,))
    wide = pltpu.SemaphoreType.DMA((n_dev,))
    return pl.pallas_call(
        functools.partial(exchange_body, tuple(caps), tok, fetch),
        out_shape=[jax.ShapeDtypeStruct((n_out,) + cols, x.dtype), jax.ShapeDtypeStruct((2, (max(caps) + 1) // 2) + cols, x.dtype)],
        in_specs=[hbm], out_specs=[hbm, hbm],
        scratch_shapes=[wide, wide, pair, pair, pair, pair, pltpu.SemaphoreType.DMA],
        compiler_params=pltpu.CompilerParams(has_side_effects=True), name="exchange",
        cost_estimate=pl.CostEstimate(flops=200_000_000_000, bytes_accessed=x.size * 2, transcendentals=0),
    )(x)[0]


def move_body(tok, count_ref, from_ref, to_ref, x_ref, out_ref, sems):
    depth = sems.shape[0]

    @pl.loop(0, count_ref.shape[0])
    def _(o):
        n = count_ref[o]

        def copy(i):
            return pltpu.make_async_copy(x_ref.at[pl.ds(from_ref[o] + i, 1)], out_ref.at[pl.ds(to_ref[o] + i, 1)], sems.at[lax.rem(i, depth)])

        @pl.loop(0, n)
        def _(i):
            @pl.when(i >= depth)
            def _():
                copy(i - depth).wait()
            copy(i).start()

        @pl.loop(jnp.maximum(n - depth, 0), n)
        def _(i):
            copy(i).wait()


def move_rows(x, count, start_from, start_to, n_out):
    smem, hbm = pl.BlockSpec(memory_space=SMEM), pl.BlockSpec(memory_space=ANY)
    return pl.pallas_call(
        functools.partial(move_body, n_out), out_shape=jax.ShapeDtypeStruct((n_out,) + x.shape[1:], x.dtype),
        in_specs=[smem, smem, smem, hbm], out_specs=hbm, scratch_shapes=[pltpu.SemaphoreType.DMA((16,))],
        name="move_rows")(count, start_from, start_to, x)


def rms_scale(in_vals, gain_vec):
    vals_f32 = in_vals.astype(F32)
    inv_rms = lax.rsqrt(jnp.mean(vals_f32 * vals_f32, axis=-1, keepdims=True) + RMS_EPS)
    return (vals_f32 * inv_rms * gain_vec).astype(BF16)


def dot(a, b, dims):
    return lax.dot_general(a, b, dims, preferred_element_type=F32)


NN = (((1,), (0,)), ((), ()))


def pair_heads(w):
    r = w.shape[0]
    w = w.reshape(r, -1, 2, NOPE_DIM + ROPE_DIM)
    plain = w[..., :NOPE_DIM].reshape(r, -1, 2 * NOPE_DIM)
    rot = w[..., NOPE_DIM:].reshape(r, -1, 2 * ROPE_DIM)
    return jnp.concatenate([plain, rot], axis=-1).reshape(r, -1)


def unpair_heads(w):
    r = w.shape[0]
    w = w.reshape(r, -1, 2 * (NOPE_DIM + ROPE_DIM))
    plain = w[..., :2 * NOPE_DIM].reshape(r, -1, 2, NOPE_DIM)
    rot = w[..., 2 * NOPE_DIM:].reshape(r, -1, 2, ROPE_DIM)
    return jnp.concatenate([plain, rot], axis=-1).reshape(r, -1)


def solution(mesh):
    n_dev = mesh.shape['fsdp']
    tok_spec = P(('dp', 'fsdp'), None)
    seq_spec = P(('dp', 'fsdp'), None, None)
    part_vec = P(('dp', 'fsdp'))
    vec_spec = P('fsdp')
    mat_spec = P('fsdp', None)

    def device_step(tok_ids, grad_out, emb_table, norm_gain, w_query, w_kv_down, kv_gain, w_kv_up, w_out):
        seq_count, seq_len = tok_ids.shape
        vocab_dev, d_model = emb_table.shape
        tok = seq_count * seq_len
        me = lax.axis_index('fsdp')
        gather = lambda piece: lax.all_gather(piece, 'fsdp', tiled=True)
        scatter = lambda full: lax.psum_scatter(full, 'fsdp', scatter_dimension=0, tiled=True)
        rows_dev, q_width = w_query.shape
        kv_rank = kv_gain.shape[0] * n_dev
        latent_at = q_width
        rank_dev = kv_gain.shape[0]
        pe_at = q_width + kv_rank
        pad_at = pe_at + ROPE_DIM
        width = -(-(pad_at + 2) // LANES) * LANES
        cols = d_model // LANES
        dy = grad_out.reshape(tok, d_model)

        uniq, rank = unique_rows(tok_ids.reshape(tok))
        all_uniq = gather(uniq).reshape(n_dev, tok)
        owner_edges = jnp.arange(n_dev + 1, dtype=jnp.int32) * vocab_dev
        starts = jnp.sum(all_uniq[:, None, :] < owner_edges[None, :, None], axis=-1, dtype=jnp.int32)
        counts = starts[:, 1:] - starts[:, :-1]
        rows = all_uniq - me * vocab_dev
        block_edges = jnp.arange(vocab_dev // TABLE_BLOCK + 1, dtype=jnp.int32) * TABLE_BLOCK
        edges = jnp.sum(rows[:, None, :] < block_edges[None, :, None], axis=-1, dtype=jnp.int32)
        mine = lambda table, axis: lax.dynamic_index_in_dim(table, me, axis, keepdims=False)
        named, my_starts = mine(counts, 0), mine(starts, 0)[:-1]
        caps = [3 * tok // 8] + [tok // 12] * (n_dev - 1)
        offs = jnp.asarray(np.cumsum([0] + caps[:-1]), jnp.int32)
        fits = jnp.all(counts <= jnp.asarray(caps, jnp.int32)[None, :])
        shift = jnp.where(fits, offs - my_starts, 0)
        place = jnp.arange(tok, dtype=jnp.int32)
        slot = place + shift[0] + jnp.sum(jnp.where(place[:, None] >= my_starts[None, 1:], (shift[1:] - shift[:-1])[None, :], 0), axis=-1)
        slots = jnp.arange(n_dev, dtype=jnp.int32) * tok

        gains = jnp.zeros((rows_dev, width - pad_at), BF16)
        gains = gains.at[:, 0].set(norm_gain).at[:rank_dev, 1].set(kv_gain)
        w_x = gather(jnp.concatenate([pair_heads(w_query), w_kv_down, gains], axis=1))
        w_o, w_up = gather(w_out), gather(w_kv_up)
        gain_vec = w_x[:, pad_at].astype(F32)
        kv_gain_vec = w_x.reshape(n_dev, rows_dev, width)[:, :rank_dev, pad_at + 1].reshape(kv_rank).astype(F32)

        sent = pick_rows(emb_table, rows, edges)
        recv = lax.cond(fits, lambda v: exchange(v, caps, tok, True),
                        lambda v: move_rows(exchange(v, [tok] * n_dev, tok, True), named, slots, my_starts, tok), sent)
        h0, x = spread_rows(recv, rank, slot, gain_vec)

        d_mix = dot(dy, w_o, COL_DIMS).astype(BF16)
        qx = dot(x, w_x, NN).astype(BF16)
        down = qx[:, latent_at:pe_at]
        latent, latent_pull = jax.vjp(rms_scale, down, kv_gain_vec)
        kv = dot(latent, w_up, NN).astype(BF16)
        mix, d_q, d_kv, d_pe = attend(qx, kv, d_mix, seq_count, pe_at // LANES)
        d_w_out = dot(mix, dy, ROW_DIMS)
        d_w_up = dot(latent, d_kv, ROW_DIMS)
        d_latent = dot(d_kv, w_up, COL_DIMS).astype(BF16)
        d_down, d_kv_gain = latent_pull(d_latent)
        d_qx = jnp.concatenate([d_q, d_down, d_pe], axis=1)
        d_x = dot(d_qx, w_x, COL_DIMS).astype(BF16)
        merged, d_gain = merge_rows(d_x, h0, dy, gain_vec, rank, slot)
        out = (h0.astype(F32) + dot(mix, w_o, NN)).astype(BF16)

        back = lax.cond(fits, lambda v: exchange(v, caps, tok, False),
                        lambda v: exchange(move_rows(v, named, my_starts, slots, n_dev * tok), [tok] * n_dev, tok, False), merged)
        grad_table = add_rows(back, rows, edges, vocab_dev)
        d_w_x = dot(x, d_qx, ROW_DIMS)
        d_gains = jnp.stack([d_gain.reshape(n_dev, rows_dev), jnp.pad(d_kv_gain.reshape(n_dev, rank_dev), ((0, 0), (0, rows_dev - rank_dev)))], axis=-1)
        d_w_x = lax.dynamic_update_slice(d_w_x, d_gains.reshape(d_model, 2), (0, pad_at))
        g_out, g_up, g_x = scatter(d_w_out), scatter(d_w_up), scatter(d_w_x)
        return (out.reshape(seq_count, seq_len, d_model), grad_table, g_x[:, pad_at], unpair_heads(g_x[:, :q_width]),
                g_x[:, q_width:pad_at], g_x[:rank_dev, pad_at + 1], g_up, g_out)

    return jax.shard_map(device_step, mesh=mesh, in_specs=(tok_spec, seq_spec, mat_spec, vec_spec, mat_spec, mat_spec, vec_spec, mat_spec, mat_spec), out_specs=(seq_spec, tok_spec, part_vec, tok_spec, tok_spec, part_vec, tok_spec, tok_spec), check_vma=False)
```

```python
import functools
import math
import jax
import jax.numpy as jnp
import numpy as np
from jax import lax
from jax.experimental import pallas as pl
from jax.experimental.pallas import tpu as pltpu
from jax.sharding import PartitionSpec as P

NOPE_DIM = 128
ROPE_DIM = 64
VALUE_DIM = 128
ROPE_THETA = 50000.0
RMS_EPS = 1e-6
ATTN_SCALE = (NOPE_DIM + ROPE_DIM) ** -0.5 * (0.1 * math.log(32.0) + 1.0) ** 2
ROW_DIMS = (((0,), (0,)), ((), ()))
COL_DIMS = (((1,), (1,)), ((), ()))
LANES = 128
TABLE_BLOCK = 1024
PICK_CHUNK = 32
PICK_RING = 4
ADD_CHUNK = 32
ADD_RING = 4
UNROLL = 8
NO_ROW = 1 << 30
PITCH = 17
F32 = jnp.float32
BF16 = jnp.bfloat16
SMEM = pltpu.SMEM
ANY = pl.ANY
HBM = pl.BlockSpec(memory_space=ANY)
SCALARS = pl.BlockSpec(memory_space=SMEM)


def shift_of(x, n):
    return lax.shift_right_logical(x, n.bit_length() - 1)


def lane(j, n=1):
    return slice(j * LANES, (j + n) * LANES)


def rowsum(x):
    return jnp.sum(x, axis=-1, keepdims=True)


def tree_sum(terms):
    while len(terms) > 1:
        terms = [a + b for a, b in zip(terms[::2], terms[1::2])]
    return terms[0]


def inverse_rms(square_sum, width):
    return lax.rsqrt(square_sum * (1.0 / width) + RMS_EPS)


def row_spec(blk, width):
    return pl.BlockSpec((blk, width), lambda i, *_: (i, 0))


def whole_spec(shape, **kw):
    return pl.BlockSpec(shape, lambda *_: (0,) * len(shape), **kw)


def struct(shape, dtype):
    return jax.ShapeDtypeStruct(shape, dtype)


def cost(flops, size):
    return pl.CostEstimate(flops=int(flops), bytes_accessed=int(size), transcendentals=0)


def params(vmem_mib, **kw):
    return pltpu.CompilerParams(vmem_limit_bytes=vmem_mib << 20, **kw)


def unique_body(shift, keys_ref, uniq_ref, rank_ref, count_ref):
    n = keys_ref.shape[0]
    unroll = 8

    def step(i, carry):
        k, prev = carry
        for j in range(unroll):
            key = keys_ref[i * unroll + j]
            row = lax.shift_right_logical(key, shift)
            k = k + (row != prev).astype(jnp.int32)
            uniq_ref[k] = row
            rank_ref[key & ((1 << shift) - 1)] = k
            prev = row
        return k, prev

    k, _ = lax.fori_loop(0, n // unroll, step, (jnp.int32(-1), jnp.int32(-1)))
    count_ref[0] = k + 1


def unique_rows(ids):
    n = ids.shape[0]
    shift = max(1, (n - 1).bit_length())
    keys = lax.sort(ids * (1 << shift) + jnp.arange(n, dtype=jnp.int32))
    uniq, rank, count = pl.pallas_call(
        functools.partial(unique_body, shift),
        out_shape=[struct((n,), jnp.int32), struct((n,), jnp.int32), struct((1,), jnp.int32)],
        in_specs=[SCALARS], out_specs=[SCALARS] * 3, name="unique_rows")(keys)
    return jnp.where(jnp.arange(n, dtype=jnp.int32) < count[0], uniq, NO_ROW), rank


def pick_body(n_dev, n_tok, rows_ref, edge_ref, table_ref, out_ref, lin_ref, stage_ref, sems):
    b = pl.program_id(0)
    n_blk = pl.num_programs(0)
    rows_blk, d_model = table_ref.shape
    cols = d_model // LANES
    n_edge = edge_ref.shape[0] // n_dev
    size, ring = PICK_CHUNK, PICK_RING

    def chunk_copy(d, k):
        slot = k & (ring - 1)
        return pltpu.make_async_copy(stage_ref.at[d, pl.ds(slot * size, size)], out_ref.at[pl.ds(d * n_tok + k * size, size)], sems.at[d, slot])

    @pl.loop(0, rows_blk // 16)
    def _(g):
        for j in range(cols):
            lin_ref[pl.ds(g * 16 * PITCH + j, 16, stride=PITCH), :] = table_ref[pl.ds(g * 16, 16), lane(j)].astype(F32)

    @pl.loop(0, n_dev)
    def _(d):
        first = edge_ref[d * n_edge]
        lo = edge_ref[d * n_edge + b] - first
        hi = edge_ref[d * n_edge + b + 1] - first
        at = d * n_tok + first
        base = b * (rows_blk * PITCH)

        @pl.when(hi > lo)
        def _():
            @pl.loop(shift_of(lo, size), shift_of(hi - 1, size) + 1)
            def _(k):
                start = jnp.maximum(lo, k * size)
                stop = jnp.minimum(hi, (k + 1) * size)

                @pl.when((start == k * size) & (k + 1 >= ring))
                def _():
                    chunk_copy(d, k + 1 - ring).wait()

                @pl.loop(0, shift_of(stop - start + UNROLL - 1, UNROLL))
                def _(i):
                    p = start + i * UNROLL
                    vals = []
                    for u in range(UNROLL):
                        vals.append(lin_ref[pl.ds(jnp.minimum(rows_ref[at + p + u] - base, (rows_blk - 1) * PITCH), cols), :])
                    for u in range(UNROLL):
                        stage_ref[d, (p + u) & (ring * size - 1)] = vals[u].astype(BF16)

                @pl.when(stop == (k + 1) * size)
                def _():
                    chunk_copy(d, k).start()

    @pl.when(b == n_blk - 1)
    def _():
        @pl.loop(0, n_dev)
        def _(d):
            total = edge_ref[d * n_edge + n_blk] - edge_ref[d * n_edge]
            chunks = shift_of(total + size - 1, size)

            @pl.when((total & (size - 1)) != 0)
            def _():
                chunk_copy(d, chunks - 1).start()

            @pl.loop(jnp.maximum(chunks + 1 - ring, 0), chunks)
            def _(k):
                chunk_copy(d, k).wait()


def row_spots(rows):
    return jnp.pad(jnp.minimum(rows, NO_ROW // PITCH).reshape(-1) * PITCH, (0, UNROLL))


def pick_rows(table, rows, edges):
    n_dev, n_tok = rows.shape
    n_rows, d_model = table.shape
    cols = d_model // LANES
    return pl.pallas_call(
        functools.partial(pick_body, n_dev, n_tok),
        grid_spec=pltpu.PrefetchScalarGridSpec(
            num_scalar_prefetch=2, grid=(n_rows // TABLE_BLOCK,),
            in_specs=[row_spec(TABLE_BLOCK, d_model)],
            out_specs=HBM,
            scratch_shapes=[
                pltpu.VMEM((TABLE_BLOCK * PITCH, LANES), F32),
                pltpu.VMEM((n_dev, PICK_RING * PICK_CHUNK, cols, LANES), BF16),
                pltpu.SemaphoreType.DMA((n_dev, PICK_RING))]),
        out_shape=struct((n_dev * n_tok, cols, LANES), BF16),
        compiler_params=params(48), name="pick_rows",
        cost_estimate=cost(60_000_000, table.size * 2),
    )(row_spots(rows), edges.reshape(-1), table)


def spread_body(rank_ref, slot_ref, recv_ref, gain_ref, h0_ref, x_ref, lin_ref):
    i = pl.program_id(0)
    rows_blk, d_model = h0_ref.shape
    cols = d_model // LANES
    unroll = 8

    @pl.loop(0, rows_blk // unroll)
    def _(t0):
        for u in range(unroll):
            t = t0 * unroll + u
            lin_ref[pl.ds(t * PITCH, cols), :] = recv_ref[slot_ref[rank_ref[i * rows_blk + t]]].astype(F32)

    @pl.loop(0, rows_blk // 32)
    def _(g):
        groups = []
        for u in range(2):
            tiles = [lin_ref[pl.ds((g * 32 + u * 16) * PITCH + j, 16, stride=PITCH), :] for j in range(cols)]
            groups.append((tiles, rowsum(tree_sum([v * v for v in tiles]))))
        for u, (tiles, square) in enumerate(groups):
            inv = inverse_rms(square, d_model)
            for j, v in enumerate(tiles):
                at = (pl.ds(g * 32 + u * 16, 16), lane(j))
                h0_ref[at] = v.astype(BF16)
                x_ref[at] = (v * inv * gain_ref[:, lane(j)]).astype(BF16)


def spread_rows(recv, rank, slot, gain):
    n_tok, cols, _ = recv.shape
    d_model = cols * LANES
    blk = 128
    out = struct((n_tok, d_model), BF16)
    rows = row_spec(blk, d_model)
    return pl.pallas_call(
        spread_body,
        grid_spec=pltpu.PrefetchScalarGridSpec(
            num_scalar_prefetch=2, grid=(n_tok // blk,),
            in_specs=[whole_spec((n_tok, cols, LANES), pipeline_mode=pl.Buffered(1)), whole_spec((1, d_model))],
            out_specs=[rows, rows],
            scratch_shapes=[pltpu.VMEM((blk * PITCH, LANES), F32)]),
        out_shape=[out, out], compiler_params=params(32), name="spread_rows",
        cost_estimate=cost(60_000_000, n_tok * d_model * 6),
    )(rank, slot, recv, gain.reshape(1, d_model))


def rope_tables(seq_len):
    pos = np.arange(seq_len, dtype=np.float32)
    inv_freq = (np.float32(ROPE_THETA) ** (np.float32(-2.0) * np.arange(ROPE_DIM // 2, dtype=np.float32) / np.float32(ROPE_DIM))).astype(np.float32)
    angle = (pos[:, None] * inv_freq[None, :]).astype(np.float32).astype(np.float64)
    cos, sin, zero = np.cos(angle), np.sin(angle), np.zeros_like(angle)
    full = lambda lo, hi: np.concatenate([lo, hi, lo, hi], axis=1).astype(np.float32)
    return full(cos, cos), full(-sin, zero), full(zero, sin)


def turn(vals, cos, sin_lo, sin_hi, sign):
    half = ROPE_DIM // 2
    return vals * cos + sign * (pltpu.roll(vals, LANES - half, 1) * sin_lo + pltpu.roll(vals, half, 1) * sin_hi)


def attn_body(q_ref, pe_ref, kv_ref, do_ref, cos_ref, sin_lo_ref, sin_hi_ref,
              o_ref, dq_ref, dkv_ref, dpe_ref, krot_ref, qcat_ref, p_ref, ds_ref, dkrot_ref):
    pair = pl.program_id(1)
    seq_len = q_ref.shape[0]
    blk = 128
    n_blk = seq_len // blk
    low = lax.broadcasted_iota(jnp.int32, (1, LANES), 1) < ROPE_DIM

    @pl.when(pair == 0)
    def _():
        pe = pe_ref[...].astype(F32)
        pe = jnp.where(low, pe, pltpu.roll(pe, ROPE_DIM, 1))
        krot_ref[...] = turn(pe, cos_ref[...], sin_lo_ref[...], sin_hi_ref[...], 1.0).astype(BF16)
        dkrot_ref[...] = jnp.zeros_like(dkrot_ref)

    qrot = turn(q_ref[:, 2 * LANES:].astype(F32), cos_ref[...], sin_lo_ref[...], sin_hi_ref[...], 1.0)
    for h in range(2):
        mine = low if h == 0 else ~low
        qcat_ref[h, :, :LANES] = q_ref[:, lane(h)]
        qcat_ref[h, :, LANES:] = jnp.where(mine, qrot, 0.0).astype(BF16)
    causal = lax.broadcasted_iota(jnp.int32, (blk, blk), 0) >= lax.broadcasted_iota(jnp.int32, (blk, blk), 1)
    blocks = [(h, i, slice(i * blk, (i + 1) * blk), (i + 1) * blk) for i in reversed(range(n_blk)) for h in range(2)]
    key = lambda h: lane(2 * h)
    val = lambda h: lane(2 * h + 1)
    head = lane
    kcat = lambda h, seen: jnp.concatenate([kv_ref[:seen, key(h)], krot_ref[:seen]], axis=1)
    scores = [lax.dot_general(qcat_ref[h, here], kcat(h, seen), COL_DIMS, preferred_element_type=F32) for h, i, here, seen in blocks]
    dps = [lax.dot_general(do_ref[here, head(h)], kv_ref[:seen, val(h)], COL_DIMS, preferred_element_type=F32) for h, i, here, seen in blocks]
    for (h, i, here, seen), s, dp in zip(blocks, scores, dps):
        diag = jnp.where(causal, s[:, i * blk:], -1e30)
        s = diag if i == 0 else jnp.concatenate([s[:, :i * blk], diag], axis=1)
        e = jnp.exp2((s - jnp.max(s, axis=-1, keepdims=True)) * (ATTN_SCALE * math.log2(math.e)))
        p = e * (1.0 / rowsum(e))
        p_ref[h, here, :seen] = p.astype(BF16)
        ds_ref[h, here, :seen] = (p * (dp - rowsum(dp * p)) * ATTN_SCALE).astype(BF16)
    dqrots = [[], []]
    for h, i, here, seen in blocks:
        o_ref[here, head(h)] = jnp.dot(p_ref[h, here, :seen], kv_ref[:seen, val(h)], preferred_element_type=F32).astype(BF16)
        dqi = jnp.dot(ds_ref[h, here, :seen], kcat(h, seen), preferred_element_type=F32)
        dq_ref[here, head(h)] = dqi[:, :LANES].astype(BF16)
        dqrots[h].append(dqi[:, LANES:])
    for h in range(2):
        for j in range(n_blk):
            here, later = slice(j * blk, (j + 1) * blk), slice(j * blk, seq_len)
            dv = lax.dot_general(p_ref[h, later, here], do_ref[later, head(h)], ROW_DIMS, preferred_element_type=F32)
            dk = lax.dot_general(ds_ref[h, later, here], qcat_ref[h, later], ROW_DIMS, preferred_element_type=F32)
            dkv_ref[here, val(h)] = dv.astype(BF16)
            dkv_ref[here, key(h)] = dk[:, :LANES].astype(BF16)
            dkrot_ref[here] += dk[:, LANES:]
    for n, i in enumerate(reversed(range(n_blk))):
        here = slice(i * blk, (i + 1) * blk)
        dqr = jnp.where(low, dqrots[0][n], dqrots[1][n]).astype(BF16).astype(F32)
        dq_ref[here, 2 * LANES:] = turn(dqr, cos_ref[here], sin_lo_ref[here], sin_hi_ref[here], -1.0).astype(BF16)

    @pl.when(pair == pl.num_programs(1) - 1)
    def _():
        both = dkrot_ref[...]
        both = (both + pltpu.roll(both, ROPE_DIM, 1)).astype(BF16).astype(F32)
        dpe = turn(both, cos_ref[...], sin_lo_ref[...], sin_hi_ref[...], -1.0)
        dpe_ref[...] = jnp.where(low, dpe, 0.0).astype(BF16)


def attend(qx, kv, d_mix, seq_count, pe_block):
    tok = qx.shape[0]
    seq_len = tok // seq_count
    pairs = d_mix.shape[1] // (2 * VALUE_DIM)
    tabs = [jnp.asarray(t) for t in rope_tables(seq_len)]
    at = lambda width: pl.BlockSpec((seq_len, width), lambda s, j: (s, j))
    tab = whole_spec((seq_len, LANES))
    shape = lambda w: struct((tok, w), BF16)
    return pl.pallas_call(
        attn_body, grid=(seq_count, pairs),
        in_specs=[at(3 * LANES), pl.BlockSpec((seq_len, LANES), lambda s, j: (s, pe_block)), at(4 * LANES), at(2 * LANES), tab, tab, tab],
        out_specs=[at(2 * LANES), at(3 * LANES), at(4 * LANES), pl.BlockSpec((seq_len, LANES), lambda s, j: (s, 0))],
        out_shape=[shape(pairs * 2 * LANES), shape(qx.shape[1]), shape(pairs * 4 * LANES), shape(LANES)],
        scratch_shapes=[pltpu.VMEM((seq_len, LANES), BF16), pltpu.VMEM((2, seq_len, 2 * LANES), BF16),
                        pltpu.VMEM((2, seq_len, seq_len), BF16), pltpu.VMEM((2, seq_len, seq_len), BF16),
                        pltpu.VMEM((seq_len, LANES), F32)],
        compiler_params=params(40), name="attention",
        cost_estimate=cost(12e9, 1e8),
    )(qx, qx, kv, d_mix, *tabs)


def latent_body(w_ref, c_ref, pe_ref, gain_ref, _, out_ref, dgain_ref, gacc_ref):
    i = pl.program_id(0)
    rank = gain_ref.shape[1]

    @pl.when(i == 0)
    def _():
        gacc_ref[...] = jnp.zeros_like(gacc_ref)

    c = c_ref[...].astype(F32)
    w = w_ref[...].astype(F32)
    inv = inverse_rms(rowsum(c * c), rank)
    hat = c * inv
    gacc_ref[...] += jnp.sum((w * hat).reshape(-1, 8, rank), axis=0)
    w = w * gain_ref[...]
    out_ref[:, :rank] = (inv * (w - hat * (rowsum(w * hat) / rank))).astype(BF16)
    out_ref[:, rank:] = pe_ref[...]

    @pl.when(i == pl.num_programs(0) - 1)
    def _():
        dgain_ref[...] = jnp.sum(gacc_ref[...], axis=0, keepdims=True)


def latent_back(d_latent, qx, d_pe, gain, d_qx, latent_at):
    tok, rank = d_latent.shape
    blk = 256
    wide = lambda width, at: pl.BlockSpec((pl.Element(blk), pl.Element(width)), lambda i: (i * blk, at))
    return pl.pallas_call(
        latent_body, grid=(tok // blk,),
        in_specs=[row_spec(blk, rank), wide(rank, latent_at), row_spec(blk, LANES), whole_spec((1, rank)), HBM],
        out_specs=[wide(rank + LANES, latent_at), whole_spec((1, rank))],
        out_shape=[struct(d_qx.shape, BF16), struct((1, rank), F32)],
        scratch_shapes=[pltpu.VMEM((8, rank), F32)], input_output_aliases={4: 0}, name="latent_back",
        cost_estimate=cost(20_000_000, tok * rank * 6),
    )(d_latent, qx, d_pe, gain.reshape(1, rank), d_qx)


def merge_body(rank_ref, slot_ref, dx_ref, h0_ref, dy_ref, gain_ref, kv_note_ref, out_ref, note_ref, even_ref, odd_ref, acc_ref, gacc_ref, sem):
    i = pl.program_id(0)
    rows_blk, d_model = h0_ref.shape
    cols = d_model // LANES

    @pl.when(i == 0)
    def _():
        gacc_ref[...] = jnp.zeros_like(gacc_ref)

        @pl.loop(0, acc_ref.shape[0] // 8)
        def _(r):
            acc_ref[pl.ds(r * 8, 8)] = jnp.zeros((8,) + acc_ref.shape[1:], F32)

    lanes = [lane(j) for j in range(cols)]

    def derive(g, lin_ref):
        rows = pl.ds(g * 16, 16)
        squares, crosses = [], []
        for at in lanes:
            v = h0_ref[rows, at].astype(F32)
            squares.append(v * v)
            crosses.append(v * (dx_ref[rows, at].astype(F32) * gain_ref[:, at]))
        inv = inverse_rms(rowsum(tree_sum(squares)), d_model)
        mean = rowsum(tree_sum(crosses)) * inv / d_model
        for j, at in enumerate(lanes):
            hat = h0_ref[rows, at].astype(F32) * inv
            w = dx_ref[rows, at].astype(F32)
            gacc_ref[:, at] += w * hat
            lin_ref[pl.ds(j, 16, stride=PITCH), :] = inv * (w * gain_ref[:, at] - hat * mean) + dy_ref[rows, at].astype(F32)

    def add(g, lin_ref):
        for t in range(16):
            r = slot_ref[rank_ref[i * rows_blk + g * 16 + t]]
            acc_ref[r] = acc_ref[r] + lin_ref[pl.ds(t * PITCH, cols), :]

    derive(0, even_ref)
    pairs = rows_blk // 32

    @pl.loop(0, pairs - 1)
    def _(g):
        add(2 * g, even_ref)
        derive(2 * g + 1, odd_ref)
        add(2 * g + 1, odd_ref)
        derive(2 * g + 2, even_ref)

    add(2 * pairs - 2, even_ref)
    derive(2 * pairs - 1, odd_ref)
    add(2 * pairs - 1, odd_ref)

    @pl.when(i == pl.num_programs(0) - 1)
    def _():
        total = jnp.sum(gacc_ref[...], axis=0, keepdims=True)
        each = d_model // note_ref.shape[0]
        note_ref[...] = jnp.zeros_like(note_ref)
        for o in range(note_ref.shape[0]):
            for r in range(each // LANES):
                note_ref[o, pl.ds(r, 1), :] = total[:, o * each + r * LANES:o * each + (r + 1) * LANES]
            note_ref[o, pl.ds(each // LANES, 1), :] = kv_note_ref[pl.ds(o, 1), :]
        copy = pltpu.make_async_copy(acc_ref, out_ref, sem)
        copy.start()
        copy.wait()


def merge_rows(dx, h0, dy, gain, kv_note, rank, slot):
    note = struct((kv_note.shape[0], 8, LANES), F32)
    n_tok, d_model = h0.shape
    cols = d_model // LANES
    blk = 128
    rows = row_spec(blk, d_model)
    return pl.pallas_call(
        merge_body,
        grid_spec=pltpu.PrefetchScalarGridSpec(
            num_scalar_prefetch=2, grid=(n_tok // blk,),
            in_specs=[rows, rows, rows, whole_spec((1, d_model)), whole_spec(kv_note.shape)],
            out_specs=[HBM, whole_spec(note.shape)],
            scratch_shapes=[pltpu.VMEM((16 * PITCH, LANES), F32), pltpu.VMEM((16 * PITCH, LANES), F32), pltpu.VMEM((n_tok, cols, LANES), F32),
                            pltpu.VMEM((16, d_model), F32), pltpu.SemaphoreType.DMA]),
        out_shape=[struct((n_tok, cols, LANES), F32), note],
        compiler_params=params(40), name="merge_rows",
        cost_estimate=cost(100_000_000, n_tok * d_model * 10),
    )(rank, slot, dx, h0, dy, gain.reshape(1, d_model), kv_note)


def add_body(n_dev, n_tok, rows_ref, edge_ref, recv_ref, out_ref, acc_ref, ring_ref, sems):
    b = pl.program_id(0)
    n_blk = pl.num_programs(0)
    rows_blk, d_model = out_ref.shape
    cols = d_model // LANES
    n_edge = edge_ref.shape[0] // n_dev
    size, ring = ADD_CHUNK, ADD_RING

    def chunk_copy(s, k):
        slot = k & (ring - 1)
        return pltpu.make_async_copy(recv_ref.at[pl.ds(s * n_tok + k * size, size)], ring_ref.at[s, pl.ds(slot * size, size)], sems.at[s, slot])

    def chunks_of(s):
        return shift_of(edge_ref[s * n_edge + n_blk] - edge_ref[s * n_edge] + size - 1, size)

    @pl.when(b == 0)
    def _():
        @pl.loop(0, n_dev)
        def _(s):
            @pl.loop(0, jnp.minimum(chunks_of(s), ring))
            def _(k):
                chunk_copy(s, k).start()

    @pl.loop(0, rows_blk // 16)
    def _(r):
        for u in range(2 * PITCH):
            acc_ref[pl.ds((r * 2 * PITCH + u) * 8, 8), :] = jnp.zeros((8, LANES), F32)

    @pl.loop(0, n_dev)
    def _(s):
        first = edge_ref[s * n_edge]
        lo = edge_ref[s * n_edge + b] - first
        hi = edge_ref[s * n_edge + b + 1] - first
        at = s * n_tok + first
        base = b * (rows_blk * PITCH)

        @pl.when(hi > lo)
        def _():
            @pl.loop(shift_of(lo, size), shift_of(hi - 1, size) + 1)
            def _(k):
                start = jnp.maximum(lo, k * size)
                stop = jnp.minimum(hi, (k + 1) * size)

                @pl.when(start == k * size)
                def _():
                    chunk_copy(s, k).wait()

                @pl.loop(0, shift_of(stop - start + UNROLL - 1, UNROLL))
                def _(i):
                    p = start + i * UNROLL
                    spots, sums = [], []
                    for u in range(UNROLL):
                        spots.append(pl.ds(jnp.where(p + u < stop, rows_ref[at + p + u] - base, rows_blk * PITCH), cols))
                        sums.append(acc_ref[spots[u], :] + ring_ref[s, (p + u) & (ring * size - 1)])
                    for u in range(UNROLL):
                        acc_ref[spots[u], :] = sums[u]

                @pl.when((stop == (k + 1) * size) & (k + ring < chunks_of(s)))
                def _():
                    chunk_copy(s, k + ring).start()

    @pl.loop(0, rows_blk // 16)
    def _(g):
        for j in range(cols):
            out_ref[pl.ds(g * 16, 16), lane(j)] = acc_ref[pl.ds(g * 16 * PITCH + j, 16, stride=PITCH), :].astype(BF16)


def add_rows(recv, rows, edges, n_rows):
    n_dev, n_tok = rows.shape
    cols = recv.shape[1]
    d_model = cols * LANES
    return pl.pallas_call(
        functools.partial(add_body, n_dev, n_tok),
        grid_spec=pltpu.PrefetchScalarGridSpec(
            num_scalar_prefetch=2, grid=(n_rows // TABLE_BLOCK,),
            in_specs=[HBM],
            out_specs=row_spec(TABLE_BLOCK, d_model),
            scratch_shapes=[pltpu.VMEM(((TABLE_BLOCK + 1) * PITCH, LANES), F32),
                            pltpu.VMEM((n_dev, ADD_RING * ADD_CHUNK, cols, LANES), F32),
                            pltpu.SemaphoreType.DMA((n_dev, ADD_RING))]),
        out_shape=struct((n_rows, d_model), BF16),
        compiler_params=params(48), name="add_rows",
        cost_estimate=cost(60_000_000, n_rows * d_model * 2),
    )(row_spots(rows), edges.reshape(-1), recv)


def exchange_body(caps, tok, fetch, x_ref, *refs):
    if fetch:
        lhs_ref, rhs_ref, out_ref, via_ref, prod_ref, *sems = refs
    else:
        note_ref, out_ref, via_ref, note_out_ref, *sems = refs
    send_sems, recv_sems, hop_send, hop_recv, end_send, end_recv, note_send, note_recv, own_sems = sems
    n_dev = len(caps)
    offs = [sum(caps[:o]) for o in range(n_dev)]
    place = lax.axis_index('fsdp')
    far, side = 6, 4
    across = lambda m: [((m ^ far) & ~1) | c for c in range(2)]

    def rows(src, dst):
        at, to, n = (dst * tok, offs[src], caps[src]) if fetch else (offs[dst], src * tok, caps[dst])
        by = 0 if (src ^ dst) & far != far else {0: n // 2, 1: n, 2: 0, 3: n // 2}[src >> 1]
        return at, to, n - by, by

    def remote(src, dst, sems, to):
        return pltpu.make_async_remote_copy(src, dst, sems[0], sems[1], device_id={'fsdp': to}, device_id_type=pl.DeviceIdType.MESH)

    def direct(src, dst):
        at, to, n, _ = rows(src, dst)
        return [remote(x_ref.at[pl.ds(at, n)], out_ref.at[pl.ds(to, n)], (send_sems.at[dst], recv_sems.at[src]), dst)] if n else []

    def note(src, dst):
        return [] if fetch else [remote(note_ref.at[dst], note_out_ref.at[src], (note_send.at[dst], note_recv.at[src]), dst)]

    def hop(src, dst):
        at, _, n, by = rows(src, dst)
        c = dst & 1
        return [remote(x_ref.at[pl.ds(at + n, by)], via_ref.at[c, pl.ds(0, by)], (hop_send.at[c], hop_recv.at[c]), src ^ side)] if by else []

    def end(src, dst):
        _, to, n, by = rows(src, dst)
        return [remote(via_ref.at[dst & 1, pl.ds(0, by)], out_ref.at[pl.ds(to + n, by)], (end_send.at[dst & 1], end_recv.at[src & 1]), dst)] if by else []

    def own(m):
        at, to, n, _ = rows(m, m)
        copies = [pltpu.make_async_copy(x_ref.at[pl.ds(at, n)], out_ref.at[pl.ds(to, n)], own_sems.at[0])]
        return copies if fetch else copies + [pltpu.make_async_copy(note_ref.at[m], note_out_ref.at[m], own_sems.at[1])]

    each = lambda copies, act: [getattr(c, act)() for c in copies]

    @pl.when(pl.program_id(0) == 0)
    def _():
        for m in range(n_dev):
            @pl.when(place == m)
            def _():
                for dst in across(m):
                    each(hop(m, dst), 'start')
                for k in (6, 7, 4, 5, 2, 3, 1):
                    each(direct(m, m ^ k) + note(m, m ^ k), 'start')
                each(own(m), 'start')

    if fetch:
        for n in range(0, prod_ref.shape[1], 512):
            prod_ref[:, n:n + 512] = lax.dot_general(lhs_ref[...], rhs_ref[n:n + 512], COL_DIMS, preferred_element_type=F32).astype(BF16)

    @pl.when(pl.program_id(0) == pl.num_programs(0) - 1)
    def _():
        for m in range(n_dev):
            @pl.when(place == m)
            def _():
                for dst in across(m ^ side):
                    each(hop(m ^ side, dst), 'wait_recv')
                    each(end(m ^ side, dst), 'start')
                each(own(m), 'wait')
                for dst in across(m):
                    each(hop(m, dst), 'wait_send')
                for k in range(1, n_dev):
                    each(direct(m, m ^ k) + note(m, m ^ k), 'wait_send')
                    each(direct(m ^ k, m) + note(m ^ k, m), 'wait_recv')
                for dst in across(m ^ side):
                    each(end(m ^ side, dst), 'wait_send')
                for src in across(m):
                    each(end(src, m), 'wait_recv')


def exchange(x, caps, tok, note=None, lhs=None, rhs=None):
    n_dev = len(caps)
    fetch = note is None
    cols = x.shape[1:]
    n_out = tok if fetch and sum(caps) <= tok else n_dev * tok
    blk = 256
    pair, wide = pltpu.SemaphoreType.DMA((2,)), pltpu.SemaphoreType.DMA((n_dev,))
    out_shape = [struct((n_out,) + cols, x.dtype), struct((2, max(caps)) + cols, x.dtype)]
    if fetch:
        grid = (lhs.shape[0] // blk,)
        more_in, args = [row_spec(blk, lhs.shape[1]), whole_spec(rhs.shape, pipeline_mode=pl.Buffered(1))], (x, lhs, rhs)
        more_out, more_shape = row_spec(blk, rhs.shape[0]), struct((lhs.shape[0], rhs.shape[0]), BF16)
    else:
        grid, more_in, args, more_out, more_shape = (1,), [HBM], (x, note), HBM, struct(note.shape, note.dtype)
    rows, _, more = pl.pallas_call(
        functools.partial(exchange_body, tuple(caps), tok, fetch), grid=grid,
        out_shape=out_shape + [more_shape], in_specs=[HBM] + more_in, out_specs=[HBM, HBM, more_out],
        scratch_shapes=[wide, wide, pair, pair, pair, pair, wide, wide, pair],
        compiler_params=params(32, has_side_effects=True), name="exchange",
        cost_estimate=cost(200_000_000_000, x.size * 2),
    )(*args)
    return rows, more


def move_body(count_ref, from_ref, to_ref, x_ref, out_ref, sems):
    depth = sems.shape[0]

    @pl.loop(0, count_ref.shape[0])
    def _(o):
        n = count_ref[o]

        def copy(i):
            return pltpu.make_async_copy(x_ref.at[pl.ds(from_ref[o] + i, 1)], out_ref.at[pl.ds(to_ref[o] + i, 1)], sems.at[lax.rem(i, depth)])

        @pl.loop(0, n)
        def _(i):
            @pl.when(i >= depth)
            def _():
                copy(i - depth).wait()

            copy(i).start()

        @pl.loop(jnp.maximum(n - depth, 0), n)
        def _(i):
            copy(i).wait()


def move_rows(x, count, start_from, start_to, n_out):
    return pl.pallas_call(
        move_body, out_shape=struct((n_out,) + x.shape[1:], x.dtype),
        in_specs=[SCALARS] * 3 + [HBM], out_specs=HBM, scratch_shapes=[pltpu.SemaphoreType.DMA((16,))],
        name="move_rows")(count, start_from, start_to, x)


def rms_scale(in_vals, gain_vec):
    vals_f32 = in_vals.astype(F32)
    inv_rms = lax.rsqrt(jnp.mean(vals_f32 * vals_f32, axis=-1, keepdims=True) + RMS_EPS)
    return (vals_f32 * inv_rms * gain_vec).astype(BF16)


def dot(a, b, dims):
    return lax.dot_general(a, b, dims, preferred_element_type=F32)


NN = (((1,), (0,)), ((), ()))


def pack_body(q_ref, down_ref, tail_ref, out_ref):
    low = lax.broadcasted_iota(jnp.int32, (1, LANES), 1) < ROPE_DIM
    width = q_ref.shape[1] // LANES
    for j in range(0, width, 3):
        one, two, three = (q_ref[:, lane(j + k)].astype(F32) for k in range(3))
        out_ref[:, lane(j)] = one.astype(BF16)
        out_ref[:, lane(j + 1)] = jnp.where(low, pltpu.roll(two, ROPE_DIM, 1), pltpu.roll(three, ROPE_DIM, 1)).astype(BF16)
        out_ref[:, lane(j + 2)] = jnp.where(low, two, three).astype(BF16)
    out_ref[:, lane(width, down_ref.shape[1] // LANES)] = down_ref[...]
    out_ref[:, lane(out_ref.shape[1] // LANES - 1)] = tail_ref[...]


def pack_weights(w_query, w_kv_down, gains):
    rows, width = w_query.shape
    cut = w_kv_down.shape[1] // LANES * LANES
    tail = jnp.concatenate([w_kv_down[:, cut:]] + [jnp.pad(g, (0, rows - g.shape[0]))[:, None] for g in gains], axis=1)
    tail = jnp.pad(tail, ((0, 0), (0, LANES - tail.shape[1])))
    return pl.pallas_call(pack_body, out_shape=struct((rows, width + cut + LANES), BF16), name="pack_weights")(w_query, w_kv_down[:, :cut], tail)


def unpack_body(g_ref, q_ref, down_ref):
    low = lax.broadcasted_iota(jnp.int32, (1, LANES), 1) < ROPE_DIM
    width = q_ref.shape[1] // LANES
    for j in range(0, width, 3):
        plain, rot = pltpu.roll(g_ref[:, lane(j + 1)], ROPE_DIM, 1), g_ref[:, lane(j + 2)]
        q_ref[:, lane(j)] = g_ref[:, lane(j)]
        q_ref[:, lane(j + 1)] = jnp.where(low, rot, plain)
        q_ref[:, lane(j + 2)] = jnp.where(low, plain, rot)
    down_ref[...] = g_ref[:, q_ref.shape[1]:q_ref.shape[1] + down_ref.shape[1]]


def unpack_grads(g_x, q_width, down_width):
    rows = g_x.shape[0]
    return pl.pallas_call(unpack_body, out_shape=[struct((rows, q_width), F32), struct((rows, down_width), F32)], name="unpack_grads")(g_x)


def share_body(n_dev, x_ref, out_ref, send_sems, recv_sems):
    place = lax.axis_index('fsdp')
    for m in range(n_dev):
        @pl.when(place == m)
        def _():
            copies = [pltpu.make_async_remote_copy(x_ref, out_ref.at[m], send_sems.at[d], recv_sems.at[m], device_id={'fsdp': d}, device_id_type=pl.DeviceIdType.MESH)
                      for d in range(n_dev) if d != m]
            for copy in copies:
                copy.start()
            out_ref[m] = x_ref[...]
            for copy in copies:
                copy.wait_send()
            for s in range(n_dev):
                if s != m:
                    pltpu.make_async_remote_copy(x_ref, out_ref.at[s], send_sems.at[s], recv_sems.at[s], device_id={'fsdp': s}, device_id_type=pl.DeviceIdType.MESH).wait_recv()


def share(x, n_dev):
    vmem = pl.BlockSpec(memory_space=pltpu.VMEM)
    wide = pltpu.SemaphoreType.DMA((n_dev,))
    return pl.pallas_call(functools.partial(share_body, n_dev), out_shape=struct((n_dev,) + x.shape, x.dtype), in_specs=[vmem], out_specs=vmem,
                          scratch_shapes=[wide, wide], compiler_params=pltpu.CompilerParams(has_side_effects=True), name="share")(x)


def solution(mesh):
    n_dev = mesh.shape['fsdp']
    tok_spec = P(('dp', 'fsdp'), None)
    seq_spec = P(('dp', 'fsdp'), None, None)
    part_vec = P(('dp', 'fsdp'))
    vec_spec = P('fsdp')
    mat_spec = P('fsdp', None)

    def step(tok_ids, grad_out, emb_table, norm_gain, w_query, w_kv_down, kv_gain, w_kv_up, w_out):
        seq_count, seq_len = tok_ids.shape
        vocab_dev, d_model = emb_table.shape
        tok = seq_count * seq_len
        me = lax.axis_index('fsdp')
        gather = lambda piece: lax.all_gather(piece, 'fsdp', tiled=True)
        scatter = lambda full: lax.psum_scatter(full, 'fsdp', scatter_dimension=0, tiled=True)
        rows_dev, q_width = w_query.shape
        kv_rank = kv_gain.shape[0] * n_dev
        latent_at = q_width
        rank_dev = kv_gain.shape[0]
        pe_at = q_width + kv_rank
        pad_at = pe_at + ROPE_DIM
        dy = grad_out.reshape(tok, d_model)

        uniq, rank = unique_rows(tok_ids.reshape(tok))
        all_uniq = share(uniq.reshape(-1, LANES), n_dev).reshape(n_dev, tok)
        owner_edges = jnp.arange(n_dev + 1, dtype=jnp.int32) * vocab_dev
        starts = jnp.sum(all_uniq[:, None, :] < owner_edges[None, :, None], axis=-1, dtype=jnp.int32)
        counts = starts[:, 1:] - starts[:, :-1]
        rows = all_uniq - me * vocab_dev
        block_edges = jnp.arange(vocab_dev // TABLE_BLOCK + 1, dtype=jnp.int32) * TABLE_BLOCK
        edges = jnp.sum(rows[:, None, :] < block_edges[None, :, None], axis=-1, dtype=jnp.int32)
        mine = lambda table, axis: lax.dynamic_index_in_dim(table, me, axis, keepdims=False)
        named, my_starts = mine(counts, 0), mine(starts, 0)[:-1]
        even = lambda share: -(-round(tok * share) // 8) * 8
        plans = [[even(hot)] + [even(rest)] * (n_dev - 1) for hot, rest in ((0.35, 0.0764), (0.3646, 0.0833))]
        fit = [jnp.all(counts <= jnp.asarray(caps, jnp.int32)[None, :]) for caps in plans]
        plan = jnp.where(fit[0], 0, jnp.where(fit[1], 1, 2))
        offs = jnp.asarray(np.cumsum([[0] + caps[:-1] for caps in plans], axis=1), jnp.int32)
        shift = jnp.where(fit[0], offs[0] - my_starts, jnp.where(fit[1], offs[1] - my_starts, 0))
        place = jnp.arange(tok, dtype=jnp.int32)
        slot = place + shift[0] + jnp.sum(jnp.where(place[:, None] >= my_starts[None, 1:], (shift[1:] - shift[:-1])[None, :], 0), axis=-1)
        slots = jnp.arange(n_dev, dtype=jnp.int32) * tok

        tie = lax.optimization_barrier
        w_o = gather(w_out)
        w_x = gather(pack_weights(w_query, w_kv_down, (norm_gain, kv_gain)))

        def fetch(caps):
            return lambda v: exchange(v, caps, tok, lhs=dy, rhs=w_o)

        def fetch_any(v):
            far_rows, prod = fetch([tok] * n_dev)(v)
            return move_rows(far_rows, named, slots, my_starts, tok), prod

        sent = pick_rows(emb_table, rows, edges)
        recv, d_mix = lax.switch(plan, [fetch(caps) for caps in plans] + [fetch_any], sent)
        recv, w_x, w_up_dev = tie((recv, w_x, w_kv_up))
        w_up = gather(w_up_dev)
        gain_vec = w_x[:, pad_at].astype(F32)
        kv_gain_vec = w_x[:, pad_at + 1].reshape(n_dev, rows_dev)[:, :rank_dev].reshape(kv_rank).astype(F32)
        h0, x = spread_rows(recv, rank, slot, gain_vec)

        qx = dot(x, w_x, NN).astype(BF16)
        latent = rms_scale(qx[:, latent_at:pe_at], kv_gain_vec)
        kv = dot(latent, w_up, NN).astype(BF16)
        mix, d_qx, d_kv, d_pe = attend(qx, kv, d_mix, seq_count, pe_at // LANES)
        d_w_out = dot(mix, dy, ROW_DIMS)
        d_kv, d_w_out = tie((d_kv, d_w_out))
        d_latent = dot(d_kv, w_up, COL_DIMS).astype(BF16)
        d_w_up = dot(latent, d_kv, ROW_DIMS)
        d_latent, d_w_up = tie((d_latent, d_w_up))
        d_qx, d_kv_gain = latent_back(d_latent, qx, d_pe, kv_gain_vec, d_qx, latent_at)
        d_x = dot(d_qx, w_x, COL_DIMS).astype(BF16)
        kv_note = jnp.pad(d_kv_gain.reshape(n_dev, rank_dev), ((0, 0), (0, LANES - rank_dev)))
        merged, note = merge_rows(d_x, h0, dy, gain_vec, kv_note, rank, slot)

        d_w_x = dot(x, d_qx, ROW_DIMS)

        def bring(caps):
            return lambda v, n: exchange(v, caps, tok, note=n)

        def bring_any(v, n):
            return bring([tok] * n_dev)(move_rows(v, named, my_starts, slots, n_dev * tok), n)

        g_out = scatter(d_w_out)
        g_up = scatter(d_w_up)
        merged, note, g_out, d_w_x = tie((merged, note, g_out, d_w_x))
        back, note = lax.switch(plan, [bring(caps) for caps in plans] + [bring_any], merged, note)
        back, d_w_x = tie((back, d_w_x))
        g_x = scatter(d_w_x)
        out = (h0.astype(F32) + dot(mix, w_o, NN)).astype(BF16)
        grad_table = add_rows(back, rows, edges, vocab_dev)
        g_query, g_down = unpack_grads(g_x, q_width, pad_at - q_width)
        g_gain = jnp.sum(note, axis=0)
        gain_rows = rows_dev // LANES
        return (out.reshape(seq_count, seq_len, d_model), grad_table, g_gain[:gain_rows].reshape(rows_dev), g_query,
                g_down, g_gain[gain_rows, :rank_dev], g_up, g_out)

    return jax.shard_map(step, mesh=mesh, in_specs=(tok_spec, seq_spec, mat_spec, vec_spec, mat_spec, mat_spec, vec_spec, mat_spec, mat_spec), out_specs=(seq_spec, tok_spec, part_vec, tok_spec, tok_spec, part_vec, tok_spec, tok_spec), check_vma=False)
```

```python
import functools
import math
import jax
import jax.numpy as jnp
import numpy as np
from jax import lax
from jax.experimental import pallas as pl
from jax.experimental.pallas import tpu as pltpu
from jax.sharding import PartitionSpec as P

NOPE_DIM = 128
ROPE_DIM = 64
VALUE_DIM = 128
ROPE_THETA = 50000.0
RMS_EPS = 1e-6
ATTN_SCALE = (NOPE_DIM + ROPE_DIM) ** -0.5 * (0.1 * math.log(32.0) + 1.0) ** 2
ROW_DIMS = (((0,), (0,)), ((), ()))
COL_DIMS = (((1,), (1,)), ((), ()))
LANES = 128
HALVES = 2
PAIR = 2 * LANES
TABLE_BLOCK = 1024
CHUNK = 16
GROUP = 16
ADD_RING = 4
UNROLL = 8
NO_ROW = 1 << 30
PITCH = 17
F32 = jnp.float32
BF16 = jnp.bfloat16
SMEM = pltpu.SMEM
ANY = pl.ANY
HBM = pl.BlockSpec(memory_space=ANY)
SCALARS = pl.BlockSpec(memory_space=SMEM)


def step_id():
    return pl.program_id(0)


def last_step():
    return pl.program_id(0) == pl.num_programs(0) - 1


def shift_of(x, n):
    return lax.shift_right_logical(x, n.bit_length() - 1)


def lane(j, n=1):
    return slice(j * LANES, (j + n) * LANES)


def low_lanes():
    return lax.broadcasted_iota(jnp.int32, (1, LANES), 1) < ROPE_DIM


def rotate(x, n):
    return pltpu.roll(x, n, 1)


def column(g, j):
    return pl.ds(g * GROUP * PITCH + j, GROUP, stride=PITCH)


def group(g):
    return pl.ds(g * GROUP, GROUP)


def rowsum(x):
    return jnp.sum(x, axis=-1, keepdims=True)


def tree_sum(terms):
    while len(terms) > 1:
        terms = [a + b for a, b in zip(terms[::2], terms[1::2])]
    return terms[0]


def inverse_rms(square_sum, width):
    return lax.rsqrt(square_sum * (1.0 / width) + RMS_EPS)


def row_spec(blk, width):
    return pl.BlockSpec((blk, width), lambda i, *_: (i, 0))


def whole_spec(shape, **kw):
    return pl.BlockSpec(shape, lambda *_: (0,) * len(shape), **kw)


def struct(shape, dtype):
    return jax.ShapeDtypeStruct(shape, dtype)


def cost(flops, size):
    return pl.CostEstimate(flops=int(flops), bytes_accessed=int(size), transcendentals=0)


def params(vmem_mib, **kw):
    return pltpu.CompilerParams(vmem_limit_bytes=vmem_mib << 20, **kw)


def unique_body(shift, halves, keys_ref, uniq_ref, rank_ref, count_ref):
    n = keys_ref.shape[0] // halves
    for h in range(halves):
        def step(i, carry):
            k, prev = carry
            for j in range(UNROLL):
                key = keys_ref[h * n + i * UNROLL + j]
                row = lax.shift_right_logical(key, shift)
                k = k + (row != prev).astype(jnp.int32)
                uniq_ref[h * n + k] = row
                rank_ref[h * n + (key & ((1 << shift) - 1))] = k
                prev = row
            return k, prev

        k, _ = lax.fori_loop(0, n // UNROLL, step, (jnp.int32(-1), jnp.int32(-1)))
        count_ref[h] = k + 1


def unique_rows(ids):
    halves, n = ids.shape
    shift = (n - 1).bit_length()
    keys = lax.sort(ids * (1 << shift) + jnp.arange(n, dtype=jnp.int32), dimension=1)
    flat = struct((halves * n,), jnp.int32)
    uniq, rank, count = pl.pallas_call(
        functools.partial(unique_body, shift, halves), out_shape=[flat, flat, struct((halves,), jnp.int32)],
        in_specs=[SCALARS], out_specs=[SCALARS] * 3, name="unique_rows")(keys.reshape(-1))
    known = jnp.arange(n, dtype=jnp.int32) < count[:, None]
    return jnp.where(known, uniq.reshape(halves, n), NO_ROW), rank.reshape(halves, n)


def pick_body(n_list, n_dev, n_tok, base, extra, rows_ref, edge_ref, table_ref, *refs):
    halves = n_list // n_dev
    base_refs, extra_refs, (lin_ref, stage_ref, sems) = refs[:halves], refs[halves:-3], refs[-3:]
    b = step_id()
    last = last_step()
    rows_blk, d_model = table_ref.shape
    cols = d_model // LANES
    n_edge = edge_ref.shape[0] // n_list

    def chunk_copies(l, k, act):
        src, sem, at = stage_ref.at[l, pl.ds(k * CHUNK, CHUNK)], sems.at[l, k], k * CHUNK

        @pl.when(at < base)
        def _():
            getattr(pltpu.make_async_copy(src, base_refs[l // n_dev].at[pl.ds(l % n_dev * base + at, CHUNK)], sem), act)()

        if extra:
            @pl.when(at >= base)
            def _():
                getattr(pltpu.make_async_copy(src, extra_refs[l].at[pl.ds(at - base, CHUNK)], sem), act)()

    @pl.loop(0, rows_blk // GROUP)
    def _(g):
        for j in range(cols):
            lin_ref[column(g, j), :] = table_ref[group(g), lane(j)].astype(F32)

    origin = b * (rows_blk * PITCH)
    for l in range(n_list):
        first = edge_ref[l * n_edge]
        lo = jnp.minimum(edge_ref[l * n_edge + b] - first, base + extra)
        hi = jnp.minimum(edge_ref[l * n_edge + b + 1] - first, base + extra)
        at = l * n_tok + first

        @pl.loop(0, shift_of(hi - lo + UNROLL - 1, UNROLL))
        def _(i):
            p = lo + i * UNROLL
            vals = [lin_ref[pl.ds(jnp.minimum(rows_ref[at + p + u] - origin, (rows_blk - 1) * PITCH), cols), :] for u in range(UNROLL)]
            for u in range(UNROLL):
                stage_ref[l, p + u] = vals[u].astype(BF16)

        @pl.loop(shift_of(lo, CHUNK), jnp.where(last, shift_of(hi + CHUNK - 1, CHUNK), shift_of(hi, CHUNK)))
        def _(k):
            chunk_copies(l, k, 'start')

    @pl.when(last)
    def _():
        for l in range(n_list):
            total = jnp.minimum(edge_ref[(l + 1) * n_edge - 1] - edge_ref[l * n_edge], base + extra)

            @pl.loop(0, shift_of(total + CHUNK - 1, CHUNK))
            def _(k):
                chunk_copies(l, k, 'wait')


def row_spots(rows):
    return jnp.pad(jnp.minimum(rows, NO_ROW // PITCH).reshape(-1) * PITCH, (0, UNROLL))


def pick_rows(table, rows, edges, n_dev, base, extra):
    n_list, n_tok = rows.shape
    n_rows, d_model = table.shape
    cols = d_model // LANES
    out = [struct((n_dev * base, cols, LANES), BF16)] * (n_list // n_dev) + [struct((extra, cols, LANES), BF16)] * (n_list if extra else 0)
    return pl.pallas_call(
        functools.partial(pick_body, n_list, n_dev, n_tok, base, extra),
        grid_spec=pltpu.PrefetchScalarGridSpec(
            num_scalar_prefetch=2, grid=(n_rows // TABLE_BLOCK,), in_specs=[row_spec(TABLE_BLOCK, d_model)], out_specs=[HBM] * len(out),
            scratch_shapes=[
                pltpu.VMEM((TABLE_BLOCK * PITCH, LANES), F32),
                pltpu.VMEM((n_list, base + extra + UNROLL, cols, LANES), BF16),
                pltpu.SemaphoreType.DMA((n_list, (base + extra) // CHUNK))]),
        out_shape=out, compiler_params=params(62), name="pick_rows", cost_estimate=cost(6e7, table.size * 2),
    )(row_spots(rows), edges.reshape(-1), table)


def spread_body(pieces, rank_ref, slot_ref, gain_ref, *refs):
    piece_refs, (h0_ref, x_ref, lin_ref, recv_ref, sems) = refs[:len(pieces)], refs[len(pieces):]
    i = step_id()
    rows_blk, d_model = h0_ref.shape
    cols = d_model // LANES

    @pl.when(i == 0)
    def _():
        for act in ('start', 'wait'):
            for n, (to, size, device) in enumerate(pieces):
                @pl.when((lax.axis_index('fsdp') == device) if device is not None else (i == 0))
                def _():
                    getattr(pltpu.make_async_copy(piece_refs[n], recv_ref.at[pl.ds(to, size)], sems.at[n]), act)()

    @pl.loop(0, rows_blk // UNROLL)
    def _(t0):
        for u in range(UNROLL):
            t = t0 * UNROLL + u
            lin_ref[pl.ds(t * PITCH, cols), :] = recv_ref[slot_ref[rank_ref[i * rows_blk + t]]].astype(F32)

    @pl.loop(0, rows_blk // (HALVES * GROUP))
    def _(g):
        groups = []
        for u in range(HALVES):
            tiles = [lin_ref[column(2 * g + u, j), :] for j in range(cols)]
            groups.append((tiles, rowsum(tree_sum([v * v for v in tiles]))))
        for u, (tiles, square) in enumerate(groups):
            inv = inverse_rms(square, d_model)
            for j, v in enumerate(tiles):
                at = (group(2 * g + u), lane(j))
                h0_ref[at] = v.astype(BF16)
                x_ref[at] = (v * inv * gain_ref[:, lane(j)]).astype(BF16)


def spread_rows(pieces, rank, slot, gain, n_slots):
    n_tok, d_model = rank.shape[0], gain.shape[0]
    cols = d_model // LANES
    blk = 128
    rows = row_spec(blk, d_model)
    plan = [(to, v.shape[0], device) for v, to, device in pieces]
    return pl.pallas_call(
        functools.partial(spread_body, plan),
        grid_spec=pltpu.PrefetchScalarGridSpec(
            num_scalar_prefetch=2, grid=(n_tok // blk,), in_specs=[whole_spec((1, d_model))] + [HBM] * len(pieces), out_specs=[rows, rows],
            scratch_shapes=[pltpu.VMEM((blk * PITCH, LANES), F32), pltpu.VMEM((n_slots, cols, LANES), BF16), pltpu.SemaphoreType.DMA((len(pieces),))]),
        out_shape=[struct((n_tok, d_model), BF16)] * 2, compiler_params=params(32), name="spread_rows",
        cost_estimate=cost(6e7, n_tok * d_model * 6),
    )(rank, slot, gain.reshape(1, d_model), *[v for v, _, _ in pieces])


def rope_tables(seq_len):
    pos = np.arange(seq_len, dtype=np.float32)
    inv_freq = (np.float32(ROPE_THETA) ** (np.float32(-2.0) * np.arange(ROPE_DIM // 2, dtype=np.float32) / np.float32(ROPE_DIM))).astype(np.float32)
    angle = (pos[:, None] * inv_freq[None, :]).astype(np.float32).astype(np.float64)
    cos, sin, zero = np.cos(angle), np.sin(angle), np.zeros_like(angle)
    full = lambda lo, hi: np.concatenate([lo, hi, lo, hi], axis=1).astype(np.float32)
    return full(cos, cos), full(-sin, zero), full(zero, sin)


def turn(vals, cos, sin_lo, sin_hi, sign):
    half = ROPE_DIM // 2
    return vals * cos + sign * (rotate(vals, LANES - half) * sin_lo + rotate(vals, half) * sin_hi)


def attn_body(q_ref, pe_ref, kv_ref, do_ref, cos_ref, sin_lo_ref, sin_hi_ref,
              o_ref, dq_ref, dkv_ref, dpe_ref, krot_ref, qcat_ref, p_ref, ds_ref, dkrot_ref):
    pair = pl.program_id(1)
    seq_len = q_ref.shape[0]
    blk = 128
    n_blk = seq_len // blk
    low = low_lanes()

    @pl.when(pair == 0)
    def _():
        pe = pe_ref[...].astype(F32)
        pe = jnp.where(low, pe, rotate(pe, ROPE_DIM))
        krot_ref[...] = turn(pe, cos_ref[...], sin_lo_ref[...], sin_hi_ref[...], 1.0).astype(BF16)
        dkrot_ref[...] = jnp.zeros_like(dkrot_ref)

    qrot = turn(q_ref[:, PAIR:].astype(F32), cos_ref[...], sin_lo_ref[...], sin_hi_ref[...], 1.0)
    for h in range(HALVES):
        mine = low if h == 0 else ~low
        qcat_ref[h, :, :LANES] = q_ref[:, lane(h)]
        qcat_ref[h, :, LANES:] = jnp.where(mine, qrot, 0.0).astype(BF16)
    causal = lax.broadcasted_iota(jnp.int32, (blk, blk), 0) >= lax.broadcasted_iota(jnp.int32, (blk, blk), 1)
    blocks = [(h, i, slice(i * blk, (i + 1) * blk), (i + 1) * blk) for i in reversed(range(n_blk)) for h in range(HALVES)]
    key = lambda h: lane(2 * h)
    val = lambda h: lane(2 * h + 1)
    head = lane
    kcat = lambda h, seen: jnp.concatenate([kv_ref[:seen, key(h)], krot_ref[:seen]], axis=1)
    scores = [lax.dot_general(qcat_ref[h, here], kcat(h, seen), COL_DIMS, preferred_element_type=F32) for h, i, here, seen in blocks]
    dps = [lax.dot_general(do_ref[here, head(h)], kv_ref[:seen, val(h)], COL_DIMS, preferred_element_type=F32) for h, i, here, seen in blocks]
    for (h, i, here, seen), s, dp in zip(blocks, scores, dps):
        diag = jnp.where(causal, s[:, i * blk:], -1e30)
        s = diag if i == 0 else jnp.concatenate([s[:, :i * blk], diag], axis=1)
        e = jnp.exp2((s - jnp.max(s, axis=-1, keepdims=True)) * (ATTN_SCALE * math.log2(math.e)))
        p = e * (1.0 / rowsum(e))
        p_ref[h, here, :seen] = p.astype(BF16)
        ds_ref[h, here, :seen] = (p * (dp - rowsum(dp * p)) * ATTN_SCALE).astype(BF16)
    dqrots = [[], []]
    for h, i, here, seen in blocks:
        o_ref[here, head(h)] = jnp.dot(p_ref[h, here, :seen], kv_ref[:seen, val(h)], preferred_element_type=F32).astype(BF16)
        dqi = jnp.dot(ds_ref[h, here, :seen], kcat(h, seen), preferred_element_type=F32)
        dq_ref[here, head(h)] = dqi[:, :LANES].astype(BF16)
        dqrots[h].append(dqi[:, LANES:])
    for h in range(HALVES):
        for j in range(n_blk):
            here, later = slice(j * blk, (j + 1) * blk), slice(j * blk, seq_len)
            dv = lax.dot_general(p_ref[h, later, here], do_ref[later, head(h)], ROW_DIMS, preferred_element_type=F32)
            dk = lax.dot_general(ds_ref[h, later, here], qcat_ref[h, later], ROW_DIMS, preferred_element_type=F32)
            dkv_ref[here, val(h)] = dv.astype(BF16)
            dkv_ref[here, key(h)] = dk[:, :LANES].astype(BF16)
            dkrot_ref[here] += dk[:, LANES:]
    for n, i in enumerate(reversed(range(n_blk))):
        here = slice(i * blk, (i + 1) * blk)
        dqr = jnp.where(low, dqrots[0][n], dqrots[1][n]).astype(BF16).astype(F32)
        dq_ref[here, PAIR:] = turn(dqr, cos_ref[here], sin_lo_ref[here], sin_hi_ref[here], -1.0).astype(BF16)

    @pl.when(pair == pl.num_programs(1) - 1)
    def _():
        both = dkrot_ref[...]
        both = (both + rotate(both, ROPE_DIM)).astype(BF16).astype(F32)
        dpe = turn(both, cos_ref[...], sin_lo_ref[...], sin_hi_ref[...], -1.0)
        dpe_ref[...] = jnp.where(low, dpe, 0.0).astype(BF16)


def attend(qx, kv, d_mix, first_seq, seq_count, pe_block):
    tok = qx.shape[0]
    seq_len = tok // seq_count
    pairs = d_mix.shape[1] // (2 * VALUE_DIM)
    tabs = [jnp.asarray(t) for t in rope_tables(seq_len)]
    at = lambda width: pl.BlockSpec((seq_len, width), lambda s, j: (s, j))
    tab = whole_spec((seq_len, LANES))
    shape = lambda w: struct((tok, w), BF16)
    return pl.pallas_call(
        attn_body, grid=(seq_count, pairs),
        in_specs=[at(3 * LANES), pl.BlockSpec((seq_len, LANES), lambda s, j: (s, pe_block)), at(4 * LANES), pl.BlockSpec((seq_len, PAIR), lambda s, j: (s + first_seq, j)), tab, tab, tab],
        out_specs=[at(PAIR), at(3 * LANES), at(4 * LANES), pl.BlockSpec((seq_len, LANES), lambda s, j: (s, 0))],
        out_shape=[shape(pairs * PAIR), shape(qx.shape[1]), shape(pairs * 4 * LANES), shape(LANES)],
        scratch_shapes=[pltpu.VMEM((seq_len, LANES), BF16), pltpu.VMEM((2, seq_len, PAIR), BF16),
                        pltpu.VMEM((2, seq_len, seq_len), BF16), pltpu.VMEM((2, seq_len, seq_len), BF16),
                        pltpu.VMEM((seq_len, LANES), F32)],
        compiler_params=params(40), name="attention",
        cost_estimate=cost(12e9, 1e8),
    )(qx, qx, kv, d_mix, *tabs)


def latent_body(w_ref, c_ref, pe_ref, gain_ref, _, out_ref, dgain_ref, gacc_ref):
    i = step_id()
    rank = gain_ref.shape[1]

    @pl.when(i == 0)
    def _():
        gacc_ref[...] = jnp.zeros_like(gacc_ref)

    c = c_ref[...].astype(F32)
    w = w_ref[...].astype(F32)
    inv = inverse_rms(rowsum(c * c), rank)
    hat = c * inv
    gacc_ref[...] += jnp.sum((w * hat).reshape(-1, 8, rank), axis=0)
    w = w * gain_ref[...]
    out_ref[:, :rank] = (inv * (w - hat * (rowsum(w * hat) / rank))).astype(BF16)
    out_ref[:, rank:] = pe_ref[...]

    @pl.when(last_step())
    def _():
        dgain_ref[...] = jnp.sum(gacc_ref[...], axis=0, keepdims=True)


def latent_back(d_latent, qx, d_pe, gain, d_qx, latent_at):
    tok, rank = d_latent.shape
    blk = 3 * LANES
    wide = lambda width, at: pl.BlockSpec((pl.Element(blk), pl.Element(width)), lambda i: (i * blk, at))
    return pl.pallas_call(
        latent_body, grid=(tok // blk,),
        in_specs=[row_spec(blk, rank), wide(rank, latent_at), row_spec(blk, LANES), whole_spec((1, rank)), HBM],
        out_specs=[wide(rank + LANES, latent_at), whole_spec((1, rank))],
        out_shape=[struct(d_qx.shape, BF16), struct((1, rank), F32)],
        scratch_shapes=[pltpu.VMEM((8, rank), F32)], input_output_aliases={4: 0}, name="latent_back",
        cost_estimate=cost(20_000_000, tok * rank * 6),
    )(d_latent, qx, d_pe, gain.reshape(1, rank), d_qx)


def merge_body(rank_ref, slot_ref, dx_ref, h0_ref, dy_ref, gain_ref, kv_note_ref, base_ref, extra_ref, note_ref, even_ref, odd_ref, acc_ref, gacc_ref, sem):
    i = step_id()
    rows_blk, d_model = h0_ref.shape
    cols = d_model // LANES

    @pl.when(i == 0)
    def _():
        gacc_ref[...] = jnp.zeros_like(gacc_ref)

        @pl.loop(0, acc_ref.shape[0] // 8)
        def _(r):
            acc_ref[pl.ds(r * 8, 8)] = jnp.zeros((8,) + acc_ref.shape[1:], F32)

    lanes = [lane(j) for j in range(cols)]

    def derive(g, lin_ref):
        rows = group(g)
        squares, crosses = [], []
        for at in lanes:
            v = h0_ref[rows, at].astype(F32)
            squares.append(v * v)
            crosses.append(v * (dx_ref[rows, at].astype(F32) * gain_ref[:, at]))
        inv = inverse_rms(rowsum(tree_sum(squares)), d_model)
        mean = rowsum(tree_sum(crosses)) * inv / d_model
        for j, at in enumerate(lanes):
            hat = h0_ref[rows, at].astype(F32) * inv
            w = dx_ref[rows, at].astype(F32)
            gacc_ref[:, at] += w * hat
            lin_ref[column(0, j), :] = inv * (w * gain_ref[:, at] - hat * mean) + dy_ref[rows, at].astype(F32)

    def add(g, lin_ref):
        for t in range(GROUP):
            r = slot_ref[rank_ref[i * rows_blk + g * GROUP + t]]
            acc_ref[r] = acc_ref[r] + lin_ref[pl.ds(t * PITCH, cols), :]

    derive(0, even_ref)
    pairs = rows_blk // (HALVES * GROUP)

    @pl.loop(0, pairs - 1)
    def _(g):
        add(2 * g, even_ref)
        derive(2 * g + 1, odd_ref)
        add(2 * g + 1, odd_ref)
        derive(2 * g + 2, even_ref)

    add(2 * pairs - 2, even_ref)
    derive(2 * pairs - 1, odd_ref)
    add(2 * pairs - 1, odd_ref)

    @pl.when(last_step())
    def _():
        total = jnp.sum(gacc_ref[...], axis=0, keepdims=True)
        each = d_model // note_ref.shape[0]
        note_ref[...] = jnp.zeros_like(note_ref)
        for o in range(note_ref.shape[0]):
            for r in range(each // LANES):
                note_ref[o, pl.ds(r, 1), :] = total[:, o * each + r * LANES:o * each + (r + 1) * LANES]
            note_ref[o, pl.ds(each // LANES, 1), :] = kv_note_ref[pl.ds(o, 1), :]
        split = base_ref.shape[0]
        copies = [pltpu.make_async_copy(acc_ref.at[pl.ds(0, split)], base_ref, sem.at[0]),
                  pltpu.make_async_copy(acc_ref.at[pl.ds(split, extra_ref.shape[0])], extra_ref, sem.at[1])]
        for copy in copies:
            copy.start()
        for copy in copies:
            copy.wait()


def merge_rows(dx, h0, dy, dy_at, gain, kv_note, rank, slot, base, extra):
    note = struct((kv_note.shape[0], 8, LANES), F32)
    n_tok, d_model = h0.shape
    cols = d_model // LANES
    blk = 128
    rows = row_spec(blk, d_model)
    return pl.pallas_call(
        merge_body,
        grid_spec=pltpu.PrefetchScalarGridSpec(
            num_scalar_prefetch=2, grid=(n_tok // blk,),
            in_specs=[rows, rows, pl.BlockSpec((blk, d_model), lambda i, *_: (i + dy_at // blk, 0)), whole_spec((1, d_model)), whole_spec(kv_note.shape)],
            out_specs=[HBM, HBM, whole_spec(note.shape)],
            scratch_shapes=[pltpu.VMEM((GROUP * PITCH, LANES), F32)] * 2 + [ pltpu.VMEM((base + extra, cols, LANES), F32),
                            pltpu.VMEM((GROUP, d_model), F32), pltpu.SemaphoreType.DMA((2,))]),
        out_shape=[struct((base, cols, LANES), F32), struct((extra, cols, LANES), F32), note],
        compiler_params=params(40), name="merge_rows",
        cost_estimate=cost(100_000_000, n_tok * d_model * 10),
    )(rank, slot, dx, h0, dy, gain.reshape(1, d_model), kv_note)


def add_body(n_dev, n_tok, halves, rows_ref, edge_ref, *refs):
    flat, (out_ref, acc_ref, ring_ref, sems) = list(refs[:-4]), refs[-4:]
    sources = []
    for stride, base, extras in halves:
        first = flat.pop(0)
        more = [flat.pop(0) for _ in range(extras)]
        sources += [(first, d * stride, base, more[d] if extras else None) for d in range(n_dev)]
    b = step_id()
    n_blk = pl.num_programs(0)
    rows_blk, d_model = out_ref.shape
    cols = d_model // LANES
    n_edge = edge_ref.shape[0] // len(sources)
    size, ring = CHUNK, ADD_RING

    def landing(s, k):
        return ring_ref.at[s, pl.ds((k & (ring - 1)) * size, size)], sems.at[s, k & (ring - 1)]

    def chunk_start(s, k):
        first, at, base, more = sources[s]
        dst, sem = landing(s, k)

        @pl.when(k * size < base)
        def _():
            pltpu.make_async_copy(first.at[pl.ds(at + k * size, size)], dst, sem).start()

        if more is not None:
            @pl.when(k * size >= base)
            def _():
                pltpu.make_async_copy(more.at[pl.ds(k * size - base, size)], dst, sem).start()

    def chunk_wait(s, k):
        dst, sem = landing(s, k)
        pltpu.make_async_copy(sources[s][0].at[pl.ds(0, size)], dst, sem).wait()

    def chunks_of(s):
        return shift_of(edge_ref[s * n_edge + n_blk] - edge_ref[s * n_edge] + size - 1, size)

    @pl.when(b == 0)
    def _():
        for s in range(len(sources)):
            @pl.loop(0, jnp.minimum(chunks_of(s), ring))
            def _(k):
                chunk_start(s, k)

    @pl.loop(0, rows_blk // GROUP)
    def _(r):
        for u in range(HALVES * PITCH):
            acc_ref[pl.ds((r * HALVES * PITCH + u) * 8, 8), :] = jnp.zeros((8, LANES), F32)

    for s in range(len(sources)):
        first = edge_ref[s * n_edge]
        lo = edge_ref[s * n_edge + b] - first
        hi = edge_ref[s * n_edge + b + 1] - first
        at = s * n_tok + first
        origin = b * (rows_blk * PITCH)

        @pl.when(hi > lo)
        def _():
            @pl.loop(shift_of(lo, size), shift_of(hi - 1, size) + 1)
            def _(k):
                start = jnp.maximum(lo, k * size)
                stop = jnp.minimum(hi, (k + 1) * size)

                @pl.when(start == k * size)
                def _():
                    chunk_wait(s, k)

                @pl.loop(0, shift_of(stop - start + UNROLL - 1, UNROLL))
                def _(i):
                    p = start + i * UNROLL
                    spots, sums = [], []
                    for u in range(UNROLL):
                        spots.append(pl.ds(jnp.where(p + u < stop, rows_ref[at + p + u] - origin, rows_blk * PITCH), cols))
                        sums.append(acc_ref[spots[u], :] + ring_ref[s, (p + u) & (ring * size - 1)])
                    for u in range(UNROLL):
                        acc_ref[spots[u], :] = sums[u]

                @pl.when((stop == (k + 1) * size) & (k + ring < chunks_of(s)))
                def _():
                    chunk_start(s, k + ring)

    @pl.loop(0, rows_blk // GROUP)
    def _(g):
        for j in range(cols):
            out_ref[group(g), lane(j)] = acc_ref[column(g, j), :].astype(BF16)


def add_rows(halves, rows, edges, n_dev, n_rows):
    n_list, n_tok = rows.shape
    cols = halves[0][0].shape[1]
    d_model = cols * LANES
    arrays = [v for first, _, _, more in halves for v in [first] + more]
    return pl.pallas_call(
        functools.partial(add_body, n_dev, n_tok, [(stride, base, len(more)) for _, stride, base, more in halves]),
        grid_spec=pltpu.PrefetchScalarGridSpec(
            num_scalar_prefetch=2, grid=(n_rows // TABLE_BLOCK,), in_specs=[HBM] * len(arrays), out_specs=row_spec(TABLE_BLOCK, d_model),
            scratch_shapes=[pltpu.VMEM(((TABLE_BLOCK + 1) * PITCH, LANES), F32),
                            pltpu.VMEM((n_list, ADD_RING * CHUNK, cols, LANES), F32),
                            pltpu.SemaphoreType.DMA((n_list, ADD_RING))]),
        out_shape=struct((n_rows, d_model), BF16), compiler_params=params(48), name="add_rows", cost_estimate=cost(6e7, n_rows * d_model * 2),
    )(row_spots(rows), edges.reshape(-1), *arrays)


def exchange_body(base, extra, fetch, n_dev, *refs):
    base_ref, refs = refs[0], refs[1:]
    n_extra = (n_dev if fetch else 1) if extra else 0
    extra_refs, refs = refs[:n_extra], refs[n_extra:]
    if fetch:
        lhs_ref, rhs_ref, out_ref, via_ref, prod_ref, *sems = refs
    else:
        note_ref, out_ref, via_ref, note_out_ref, *sems = refs
    send_sems, recv_sems, hop_send, hop_recv, end_send, end_recv, note_send, note_recv, own_sems = sems
    place = lax.axis_index('fsdp')
    far, side = n_dev - 2, n_dev // 2
    across = lambda m: [((m ^ far) & ~1) | c for c in range(HALVES)]

    def moves(src, dst):
        runs = [(0, base_ref, dst * base, src * base if fetch else src * (base + extra), base)]
        if extra and (src if fetch else dst) == 0:
            runs.append((1, extra_refs[dst] if fetch else extra_refs[0], 0, n_dev * base if fetch else src * (base + extra) + base, extra))
        out = []
        for kind, ref, at, to, n in runs:
            by = 0 if (src ^ dst) & far != far else (n // 2, n, 0, n // 2)[src >> 1]
            out.append((kind, ref, at, to, n - by, by))
        return out

    def remote(src, dst, send, recv, to):
        return pltpu.make_async_remote_copy(src, dst, send, recv, device_id={'fsdp': to}, device_id_type=pl.DeviceIdType.MESH)

    def direct(src, dst):
        return [remote(ref.at[pl.ds(at, n)], out_ref.at[pl.ds(to, n)], send_sems.at[kind * n_dev + dst], recv_sems.at[kind * n_dev + src], dst)
                for kind, ref, at, to, n, _ in moves(src, dst) if n]

    def note(src, dst):
        return [] if fetch else [remote(note_ref.at[dst], note_out_ref.at[src], note_send.at[dst], note_recv.at[src], dst)]

    def hop(src, dst):
        out = []
        for kind, ref, at, _, n, by in moves(src, dst):
            lot = HALVES * kind + (dst & 1)
            if by:
                out.append(remote(ref.at[pl.ds(at + n, by)], via_ref.at[lot, pl.ds(0, by)], hop_send.at[lot], hop_recv.at[lot], src ^ side))
        return out

    def end(src, dst):
        return [remote(via_ref.at[HALVES * kind + (dst & 1), pl.ds(0, by)], out_ref.at[pl.ds(to + n, by)], end_send.at[HALVES * kind + (dst & 1)], end_recv.at[HALVES * kind + (src & 1)], dst)
                for kind, _, _, to, n, by in moves(src, dst) if by]

    def own(m):
        copies = [pltpu.make_async_copy(ref.at[pl.ds(at, n)], out_ref.at[pl.ds(to, n)], own_sems.at[kind]) for kind, ref, at, to, n, _ in moves(m, m)]
        return copies if fetch else copies + [pltpu.make_async_copy(note_ref.at[m], note_out_ref.at[m], own_sems.at[2])]

    each = lambda copies, act: [getattr(c, act)() for c in copies]

    @pl.when(step_id() == 0)
    def _():
        for m in range(n_dev):
            @pl.when(place == m)
            def _():
                for dst in across(m):
                    each(hop(m, dst), 'start')
                for k in reversed(range(1, n_dev)):
                    each(direct(m, m ^ k) + note(m, m ^ k), 'start')
                each(own(m), 'start')

    if fetch:
        for n in range(0, prod_ref.shape[1], 512):
            prod_ref[:, n:n + 512] = lax.dot_general(lhs_ref[...], rhs_ref[n:n + 512], COL_DIMS, preferred_element_type=F32).astype(BF16)

    @pl.when(last_step())
    def _():
        for m in range(n_dev):
            @pl.when(place == m)
            def _():
                for dst in across(m ^ side):
                    each(hop(m ^ side, dst), 'wait_recv')
                    each(end(m ^ side, dst), 'start')
                each(own(m), 'wait')
                for dst in across(m):
                    each(hop(m, dst), 'wait_send')
                for k in range(1, n_dev):
                    each(direct(m, m ^ k) + note(m, m ^ k), 'wait_send')
                    each(direct(m ^ k, m) + note(m ^ k, m), 'wait_recv')
                for dst in across(m ^ side):
                    each(end(m ^ side, dst), 'wait_send')
                for src in across(m):
                    each(end(src, m), 'wait_recv')


def exchange(rows, base, extra, n_dev, note=None, lhs=None, rhs=None):
    fetch = note is None
    cols = rows[0].shape[1:]
    blk = 256
    quad, wide, pair = (pltpu.SemaphoreType.DMA((n,)) for n in (4, n_dev, HALVES * n_dev))
    dtype = rows[0].dtype
    out_shape = [struct((n_dev * base + extra * (1 if fetch else n_dev),) + cols, dtype), struct((4, max(base, extra)) + cols, dtype)]
    if fetch:
        grid = (lhs.shape[0] // blk,)
        more_in, args = [row_spec(blk, lhs.shape[1]), whole_spec((rhs.shape[0], lhs.shape[1]), pipeline_mode=pl.Buffered(1))], (lhs, rhs)
        more_out, more_shape = row_spec(blk, rhs.shape[0]), struct((lhs.shape[0], rhs.shape[0]), BF16)
    else:
        grid, more_in, args, more_out, more_shape = (1,), [HBM], (note,), HBM, struct(note.shape, note.dtype)
    got, _, more = pl.pallas_call(
        functools.partial(exchange_body, base, extra, fetch, n_dev), grid=grid,
        out_shape=out_shape + [more_shape], in_specs=[HBM] * len(rows) + more_in, out_specs=[HBM, HBM, more_out],
        scratch_shapes=[pair, pair, quad, quad, quad, quad, wide, wide, quad],
        compiler_params=params(32, has_side_effects=True), name="exchange", cost_estimate=cost(1e11, 1e8),
    )(*rows, *args)
    return got, more


def fetch_beside(base, extras):
    got = lax.all_to_all(base, 'fsdp', 0, 0, tiled=True)
    more = [v if d == 0 else lax.ppermute(v, 'fsdp', [(0, d)]) for d, v in enumerate(extras)]
    return [got] + more


def bring_beside(base, extra, n_dev):
    got = lax.all_to_all(base, 'fsdp', 0, 0, tiled=True)
    last = n_dev - 1
    via = lax.ppermute(extra, 'fsdp', [(last, last ^ (n_dev // 2))])
    return got, [extra if s == 0 else lax.ppermute(extra, 'fsdp', [(s, 0)]) for s in range(last)], via


def weight_body(n_rhs, steps, lhs_a_ref, lhs_b_ref, *refs):
    rhs_refs, (out_ref, turned_ref, rhs_ref, sems) = refs[:n_rhs], refs[n_rhs:]
    i = step_id()
    half = lhs_a_ref.shape[0]
    width = rhs_ref.shape[1]
    rows = rhs_ref.shape[0] // n_rhs

    def fill(j, n):
        cols = pl.ds(pl.multiple_of(j * steps, steps), n)
        return [pltpu.make_async_copy(v.at[:, cols], rhs_ref.at[pl.ds(k * rows, rows), cols], sems.at[k, j]) for k, v in enumerate(rhs_refs)]

    pieces = [(j, min(steps, width - j * steps)) for j in range(-(-width // steps))]

    @pl.when(i == 0)
    def _():
        for j, n in pieces:
            for copy in fill(j, n):
                copy.start()

    turned_ref[:, :half] = lhs_a_ref[...].T
    turned_ref[:, half:] = lhs_b_ref[...].T

    def product(at, n):
        out_ref[:, pl.ds(at, n)] = jnp.dot(turned_ref[...], rhs_ref[:, pl.ds(at, n)], preferred_element_type=F32)

    whole = width // steps

    @pl.loop(0, whole)
    def _(j):
        @pl.when(i == 0)
        def _():
            for copy in fill(j, steps):
                copy.wait()

        product(pl.multiple_of(j * steps, steps), steps)

    for j, n in pieces[whole:]:
        @pl.when(i == 0)
        def _():
            for copy in fill(j, n):
                copy.wait()

        product(j * steps, n)


def weight_grad(lhs_a, lhs_b, *rhs, more=0):
    half, height = lhs_a.shape
    width = rhs[0].shape[1]
    steps = 512
    blk = min(512, height)
    left = pl.BlockSpec((half, blk), lambda i: (0, i))
    return pl.pallas_call(
        functools.partial(weight_body, len(rhs), steps), grid=(height // blk,), in_specs=[left, left] + [HBM] * len(rhs), out_specs=row_spec(blk, width),
        out_shape=struct((height, width + more), F32),
        scratch_shapes=[pltpu.VMEM((blk, HALVES * half), BF16), pltpu.VMEM((HALVES * half, width), BF16), pltpu.SemaphoreType.DMA((len(rhs), -(-width // steps)))],
        compiler_params=params(56), name="weight_grad", cost_estimate=cost(4 * half * height * width, height * width * 4),
    )(lhs_a, lhs_b, *rhs)


def beside_body(lhs_a_ref, lhs_b_ref, rhs_a_ref, rhs_b_ref, _, out_ref, turned_ref):
    half = lhs_a_ref.shape[0]

    @pl.when(step_id() == 0)
    def _():
        turned_ref[:, :half] = lhs_a_ref[...].T
        turned_ref[:, half:] = lhs_b_ref[...].T

    prod = jnp.dot(turned_ref[:, :half], rhs_a_ref[...], preferred_element_type=F32)
    prod = prod + jnp.dot(turned_ref[:, half:], rhs_b_ref[...], preferred_element_type=F32)
    out_ref[...] = prod.reshape(out_ref.shape)


def weight_grad_beside(big, at, lhs_a, lhs_b, rhs_a, rhs_b, n_dev):
    half, height = lhs_a.shape
    rows, width = big.shape
    part = width - at
    parts = rhs_a.shape[1] // part
    big = big.reshape(n_dev, rows // n_dev, width)
    right = pl.BlockSpec((half, part), lambda q: (0, q))
    return pl.pallas_call(
        beside_body, grid=(parts,), in_specs=[whole_spec(lhs_a.shape)] * 2 + [right, right, HBM],
        out_specs=pl.BlockSpec((n_dev, height // n_dev, part), lambda q: (0, q, at // part)), out_shape=struct(big.shape, F32),
        scratch_shapes=[pltpu.VMEM((height, HALVES * half), BF16)], input_output_aliases={4: 0}, compiler_params=params(48), name="weight_grad_beside",
        cost_estimate=cost(4 * half * height * part * parts, 1e7),
    )(lhs_a, lhs_b, rhs_a, rhs_b, big).reshape(rows, width)


def fresh(shape, dtype):
    return pl.pallas_call(lambda out_ref: None, out_shape=struct(shape, dtype), out_specs=HBM, name="fresh")()


def move_body(count_ref, from_ref, to_ref, x_ref, out_ref, sems):
    depth = sems.shape[0]

    @pl.loop(0, count_ref.shape[0])
    def _(o):
        n = count_ref[o]

        def copy(i):
            return pltpu.make_async_copy(x_ref.at[pl.ds(from_ref[o] + i, 1)], out_ref.at[pl.ds(to_ref[o] + i, 1)], sems.at[lax.rem(i, depth)])

        @pl.loop(0, n)
        def _(i):
            @pl.when(i >= depth)
            def _():
                copy(i - depth).wait()

            copy(i).start()

        @pl.loop(jnp.maximum(n - depth, 0), n)
        def _(i):
            copy(i).wait()


def move_rows(x, count, start_from, start_to, n_out):
    return pl.pallas_call(
        move_body, out_shape=struct((n_out,) + x.shape[1:], x.dtype),
        in_specs=[SCALARS] * 3 + [HBM], out_specs=HBM, scratch_shapes=[pltpu.SemaphoreType.DMA((16,))],
        name="move_rows")(count, start_from, start_to, x)


def rms_scale(in_vals, gain_vec):
    vals_f32 = in_vals.astype(F32)
    inv_rms = lax.rsqrt(jnp.mean(vals_f32 * vals_f32, axis=-1, keepdims=True) + RMS_EPS)
    return (vals_f32 * inv_rms * gain_vec).astype(BF16)


def dot(a, b, dims):
    return lax.dot_general(a, b, dims, preferred_element_type=F32)


NN = (((1,), (0,)), ((), ()))


def pack_body(o_ref, q_ref, down_ref, tail_ref, out_ref):
    low = low_lanes()
    start, width = o_ref.shape[1] // LANES, q_ref.shape[1] // LANES
    out_ref[:, lane(0, start)] = o_ref[...]
    for j in range(0, width, 3):
        one, two, three = (q_ref[:, lane(j + k)].astype(F32) for k in range(3))
        out_ref[:, lane(start + j)] = one.astype(BF16)
        out_ref[:, lane(start + j + 1)] = jnp.where(low, rotate(two, ROPE_DIM), rotate(three, ROPE_DIM)).astype(BF16)
        out_ref[:, lane(start + j + 2)] = jnp.where(low, two, three).astype(BF16)
    out_ref[:, lane(start + width, down_ref.shape[1] // LANES)] = down_ref[...]
    out_ref[:, lane(out_ref.shape[1] // LANES - 1)] = tail_ref[...]


def pack_weights(w_out, w_query, w_kv_down, gains):
    rows, width = w_query.shape
    cut = w_kv_down.shape[1] // LANES * LANES
    tail = jnp.concatenate([w_kv_down[:, cut:]] + [jnp.pad(g, (0, rows - g.shape[0]))[:, None] for g in gains], axis=1)
    tail = jnp.pad(tail, ((0, 0), (0, LANES - tail.shape[1])))
    return pl.pallas_call(pack_body, out_shape=struct((rows, w_out.shape[1] + width + cut + LANES), BF16),
                          name="pack_weights")(w_out, w_query, w_kv_down[:, :cut], tail)


def unpack_body(g_ref, q_ref, down_ref):
    low = low_lanes()
    width = q_ref.shape[1] // LANES
    for j in range(0, width, 3):
        plain, rot = rotate(g_ref[:, lane(j + 1)], ROPE_DIM), g_ref[:, lane(j + 2)]
        q_ref[:, lane(j)] = g_ref[:, lane(j)]
        q_ref[:, lane(j + 1)] = jnp.where(low, rot, plain)
        q_ref[:, lane(j + 2)] = jnp.where(low, plain, rot)
    down_ref[...] = g_ref[:, q_ref.shape[1]:q_ref.shape[1] + down_ref.shape[1]]


def unpack_grads(g_x, q_width, down_width):
    rows = g_x.shape[0]
    return pl.pallas_call(unpack_body, out_shape=[struct((rows, q_width), F32), struct((rows, down_width), F32)], name="unpack_grads")(g_x)


def share_body(n_dev, x_ref, out_ref, send_sems, recv_sems):
    place = lax.axis_index('fsdp')
    for m in range(n_dev):
        @pl.when(place == m)
        def _():
            copies = [pltpu.make_async_remote_copy(x_ref, out_ref.at[m], send_sems.at[d], recv_sems.at[m], device_id={'fsdp': d}, device_id_type=pl.DeviceIdType.MESH)
                      for d in range(n_dev) if d != m]
            for copy in copies:
                copy.start()
            out_ref[m] = x_ref[...]
            for copy in copies:
                copy.wait_send()
            for s in range(n_dev):
                if s != m:
                    pltpu.make_async_remote_copy(x_ref, out_ref.at[s], send_sems.at[s], recv_sems.at[s], device_id={'fsdp': s}, device_id_type=pl.DeviceIdType.MESH).wait_recv()


def share(x, n_dev):
    vmem = pl.BlockSpec(memory_space=pltpu.VMEM)
    wide = pltpu.SemaphoreType.DMA((n_dev,))
    return pl.pallas_call(functools.partial(share_body, n_dev), out_shape=struct((n_dev,) + x.shape, x.dtype), in_specs=[vmem], out_specs=vmem,
                          scratch_shapes=[wide, wide], compiler_params=pltpu.CompilerParams(has_side_effects=True), name="share")(x)


def solution(mesh):
    n_dev = mesh.shape['fsdp']
    tok_spec = P(('dp', 'fsdp'), None)
    seq_spec = P(('dp', 'fsdp'), None, None)
    part_vec = P(('dp', 'fsdp'))
    vec_spec = P('fsdp')
    mat_spec = P('fsdp', None)

    def step(tok_ids, grad_out, emb_table, norm_gain, w_query, w_kv_down, kv_gain, w_kv_up, w_out):
        seq_count, seq_len = tok_ids.shape
        vocab_dev, d_model = emb_table.shape
        tok = seq_count * seq_len
        half = tok // HALVES
        per_half = seq_count // HALVES
        me = lax.axis_index('fsdp')
        gather = lambda piece: lax.all_gather(piece, 'fsdp', tiled=True)
        scatter = lambda full: lax.psum_scatter(full, 'fsdp', scatter_dimension=0, tiled=True)
        tie = lax.optimization_barrier
        rows_dev, q_width = w_query.shape
        rank_dev, = kv_gain.shape
        kv_rank = rank_dev * n_dev
        pe_at = q_width + kv_rank
        pad_at = pe_at + ROPE_DIM
        dy = grad_out.reshape(tok, d_model)
        w_ox = gather(pack_weights(w_out, w_query, w_kv_down, (norm_gain, kv_gain)))

        base, extra = [-(-round(half * share) // CHUNK) * CHUNK for share in (0.09, 0.31)]
        n_slots = n_dev * base + extra
        uniq, rank = unique_rows(tok_ids.reshape(HALVES, half))
        all_uniq = share(uniq.reshape(-1, LANES), n_dev).reshape(n_dev, HALVES, half)
        below = lambda lists, edges: jnp.sum(lists[..., None, :] < edges[:, None], axis=-1, dtype=jnp.int32)
        starts = below(all_uniq, jnp.arange(n_dev + 1, dtype=jnp.int32) * vocab_dev)
        counts = starts[..., 1:] - starts[..., :-1]
        fits = jnp.all(counts <= jnp.asarray([base + extra] + [base] * (n_dev - 1), jnp.int32))
        lists = jnp.swapaxes(all_uniq, 0, 1).reshape(HALVES * n_dev, half) - me * vocab_dev
        edges = below(lists, jnp.arange(vocab_dev // TABLE_BLOCK + 1, dtype=jnp.int32) * TABLE_BLOCK)
        my_starts, named = (lax.dynamic_index_in_dim(v, me, keepdims=False) for v in (starts[..., :-1], counts))
        place = jnp.arange(half, dtype=jnp.int32)
        begun = place[:, None] >= my_starts[:, None, 1:]
        slot = place + jnp.sum(jnp.where(begun, base - named[:, None, :-1], 0), axis=-1)
        slot = jnp.where((place >= base) & ~begun[..., 0], place + (n_dev - 1) * base, slot)
        slot = jnp.where(fits, slot, place)
        slots = jnp.arange(n_dev, dtype=jnp.int32) * half
        (rank_a, rank_b), (slot_a, slot_b) = rank, slot

        base_a, base_b, *extras = pick_rows(emb_table, lists, edges, n_dev, base, extra)
        extras_a, extras_b = extras[:n_dev], extras[n_dev:]

        def fetch_any(h):
            mine = slice(h * n_dev, (h + 1) * n_dev)
            far, = pick_rows(emb_table, lists[mine], edges[mine], n_dev, half, 0)
            far, prod = exchange([far], half, 0, n_dev, lhs=dy, rhs=w_ox)
            return move_rows(far, named[h], slots, my_starts[h], n_slots), prod

        recv, d_mix = lax.cond(fits, lambda: exchange([base_a] + extras_a, base, extra, n_dev, lhs=dy, rhs=w_ox), lambda: fetch_any(0))
        recv, w_ox, w_kv_up, base_b, extras_b = tie((recv, w_ox, w_kv_up, base_b, extras_b))
        w_o, w_x = w_ox[:, :d_model], w_ox[:, d_model:]
        w_up = gather(w_kv_up)
        pieces = fetch_beside(base_b, extras_b)
        gain_vec = w_x[:, pad_at].astype(F32)
        kv_gain_vec = w_x[:, pad_at + 1].reshape(n_dev, rows_dev)[:, :rank_dev].reshape(kv_rank).astype(F32)

        def compute(h, x):
            qx = dot(x, w_x, NN).astype(BF16)
            latent = rms_scale(qx[:, q_width:pe_at], kv_gain_vec)
            kv = dot(latent, w_up, NN).astype(BF16)
            return (qx, latent) + tuple(attend(qx, kv, d_mix, h * per_half, per_half, pe_at // LANES))

        def descend(qx, d_qx, d_kv, d_pe, kv_note):
            d_latent = dot(d_kv, w_up, COL_DIMS).astype(BF16)
            d_qx, d_kv_gain = latent_back(d_latent, qx, d_pe, kv_gain_vec, d_qx, q_width)
            return d_qx, kv_note + jnp.pad(d_kv_gain.reshape(n_dev, rank_dev), ((0, 0), (0, LANES - rank_dev)))

        h0_a, x_a = spread_rows([(recv, 0, None)], rank_a, slot_a, gain_vec, n_slots)
        qx_a, latent_a, mix_a, d_qx_a, d_kv_a, d_pe_a = compute(0, x_a)
        no_note = jnp.zeros((n_dev, LANES), F32)
        d_qx_a, kv_note = descend(qx_a, d_qx_a, d_kv_a, d_pe_a, no_note)
        d_x = dot(d_qx_a, w_x, COL_DIMS).astype(BF16)
        *merged_a, note_a = merge_rows(d_x, h0_a, dy, 0, gain_vec, no_note, rank_a, slot_a, n_dev * base, extra)
        back_a = bring_beside(*merged_a, n_dev)

        pieces, note_a = tie((pieces, note_a))
        h0_b, x_b = lax.cond(
            fits, lambda v: spread_rows([(v[0], 0, None)] + [(p, n_dev * base, d) for d, p in enumerate(v[1:])], rank_b, slot_b, gain_vec, n_slots),
            lambda v: spread_rows([(fetch_any(1)[0], 0, None)], rank_b, slot_b, gain_vec, n_slots), pieces)
        qx_b, latent_b, mix_b, d_qx_b, d_kv_b, d_pe_b = compute(1, x_b)
        got_a, extra_a, via = back_a
        via, d_kv_b = tie((via, d_kv_b))
        extra_a = extra_a + [lax.ppermute(via, 'fsdp', [(n_dev // 2 - 1, 0)])]
        d_w_o = weight_grad(mix_a, mix_b, dy, more=w_up.size // d_model)
        d_w_o = weight_grad_beside(d_w_o, d_model, latent_a, latent_b, d_kv_a, d_kv_b, n_dev)
        d_kv_b, d_w_o = tie((d_kv_b, d_w_o))
        d_qx_b, kv_note = descend(qx_b, d_qx_b, d_kv_b, d_pe_b, kv_note)
        d_x = dot(d_qx_b, w_x, COL_DIMS).astype(BF16)
        d_w_x = weight_grad(x_a, x_b, d_qx_a, d_qx_b)
        *merged_b, note_b = merge_rows(d_x, h0_b, dy, half, gain_vec, kv_note, rank_b, slot_b, n_dev * base, extra)

        g_o = scatter(d_w_o)
        merged_b, note, d_w_x = tie((merged_b, note_a + note_b, d_w_x))

        def bring_any(h, merged, note):
            far = move_rows(jnp.concatenate(merged, axis=0), named[h], my_starts[h], slots, n_dev * half)
            return exchange([far], half, 0, n_dev, note=note)

        room = base + extra
        back_b, note = lax.cond(fits, lambda v, n: exchange(v, base, extra, n_dev, note=n),
                                lambda v, n: (fresh((n_dev * room, d_model // LANES, LANES), F32), bring_any(1, v, n)[1]), merged_b, note)
        back_b, d_w_x, h0_b, mix_b = tie((back_b, d_w_x, h0_b, mix_b))
        g_x = scatter(d_w_x)
        out = jnp.concatenate([(h0.astype(F32) + dot(mix, w_o, NN)).astype(BF16) for h0, mix in ((h0_a, mix_a), (h0_b, mix_b))], axis=0)
        grad_table = lax.cond(
            fits, lambda: add_rows([(got_a, base, base, extra_a), (back_b, room, room, [])], lists, edges, n_dev, vocab_dev),
            lambda: add_rows([(bring_any(h, v, note)[0], half, half, []) for h, v in enumerate((merged_a, merged_b))], lists, edges, n_dev, vocab_dev))
        g_up = jnp.swapaxes(g_o[:, d_model:].reshape(-1, rank_dev, g_o.shape[1] - d_model), 0, 1).reshape(w_kv_up.shape)
        g_query, g_down = unpack_grads(g_x, q_width, pad_at - q_width)
        g_gain = jnp.sum(note, axis=0)
        gain_rows = rows_dev // LANES
        return (out.reshape(seq_count, seq_len, d_model), grad_table, g_gain[:gain_rows].reshape(rows_dev), g_query,
                g_down, g_gain[gain_rows, :rank_dev], g_up, g_o[:, :d_model])

    return jax.shard_map(step, mesh=mesh, in_specs=(tok_spec, seq_spec, mat_spec, vec_spec, mat_spec, mat_spec, vec_spec, mat_spec, mat_spec), out_specs=(seq_spec, tok_spec, part_vec, tok_spec, tok_spec, part_vec, tok_spec, tok_spec), check_vma=False)
```

```python
import functools
import math
import jax
import jax.numpy as jnp
import numpy as np
from jax import lax
from jax.experimental import pallas as pl
from jax.experimental.pallas import tpu as pltpu
from jax.sharding import PartitionSpec as P

NOPE_DIM = 128
ROPE_DIM = 64
VALUE_DIM = 128
ROPE_THETA = 50000.0
RMS_EPS = 1e-6
ATTN_SCALE = (NOPE_DIM + ROPE_DIM) ** -0.5 * (0.1 * math.log(32.0) + 1.0) ** 2
ROW_DIMS = (((0,), (0,)), ((), ()))
COL_DIMS = (((1,), (1,)), ((), ()))
LANES = 128
HALVES = 2
PAIR = 2 * LANES
TABLE_BLOCK = 1024
CHUNK = 16
GROUP = 16
ADD_RING = 4
UNROLL = 8
NO_ROW = 1 << 30
PITCH = 17
F32 = jnp.float32
BF16 = jnp.bfloat16
SMEM = pltpu.SMEM
ANY = pl.ANY
HBM = pl.BlockSpec(memory_space=ANY)
SCALARS = pl.BlockSpec(memory_space=SMEM)


def step_id():
    return pl.program_id(0)


def last_step():
    return pl.program_id(0) == pl.num_programs(0) - 1


def shift_of(x, n):
    return lax.shift_right_logical(x, n.bit_length() - 1)


def lane(j, n=1):
    return slice(j * LANES, (j + n) * LANES)


def low_lanes():
    return lax.broadcasted_iota(jnp.int32, (1, LANES), 1) < ROPE_DIM


def rotate(x, n):
    return pltpu.roll(x, n, 1)


def column(g, j):
    return pl.ds(g * GROUP * PITCH + j, GROUP, stride=PITCH)


def group(g):
    return pl.ds(g * GROUP, GROUP)


def rowsum(x):
    return jnp.sum(x, axis=-1, keepdims=True)


def tree_sum(terms):
    while len(terms) > 1:
        terms = [a + b for a, b in zip(terms[::2], terms[1::2])]
    return terms[0]


def inverse_rms(square_sum, width):
    return lax.rsqrt(square_sum * (1.0 / width) + RMS_EPS)


def row_spec(blk, width):
    return pl.BlockSpec((blk, width), lambda i, *_: (i, 0))


def whole_spec(shape, **kw):
    return pl.BlockSpec(shape, lambda *_: (0,) * len(shape), **kw)


def struct(shape, dtype):
    return jax.ShapeDtypeStruct(shape, dtype)


def cost(flops, size):
    return pl.CostEstimate(flops=int(flops), bytes_accessed=int(size), transcendentals=0)


CHEAP = cost(6e7, 1e7)
SMALL, LARGE, FULL = 40, 48, 62


def params(vmem_mib, **kw):
    return pltpu.CompilerParams(vmem_limit_bytes=vmem_mib << 20, **kw)


def unique_body(shift, halves, keys_ref, uniq_ref, rank_ref, count_ref):
    n = keys_ref.shape[0] // halves
    for h in range(halves):
        def step(i, carry):
            k, prev = carry
            for j in range(UNROLL):
                key = keys_ref[h * n + i * UNROLL + j]
                row = lax.shift_right_logical(key, shift)
                k = k + (row != prev).astype(jnp.int32)
                uniq_ref[h * n + k] = row
                rank_ref[h * n + (key & ((1 << shift) - 1))] = k
                prev = row
            return k, prev

        k, _ = lax.fori_loop(0, n // UNROLL, step, (jnp.int32(-1), jnp.int32(-1)))
        count_ref[h] = k + 1


def unique_rows(ids):
    halves, n = ids.shape
    shift = (n - 1).bit_length()
    keys = lax.sort(ids * (1 << shift) + jnp.arange(n, dtype=jnp.int32), dimension=1)
    flat = struct((halves * n,), jnp.int32)
    uniq, rank, count = pl.pallas_call(
        functools.partial(unique_body, shift, halves), out_shape=[flat, flat, struct((halves,), jnp.int32)],
        in_specs=[SCALARS], out_specs=[SCALARS] * 3, name="unique_rows")(keys.reshape(-1))
    known = jnp.arange(n, dtype=jnp.int32) < count[:, None]
    return jnp.where(known, uniq.reshape(halves, n), NO_ROW), rank.reshape(halves, n)


def pick_body(n_list, n_dev, n_tok, base, extra, rows_ref, edge_ref, table_ref, *refs):
    halves = n_list // n_dev
    base_refs, extra_refs, (lin_ref, stage_ref, sems) = refs[:halves], refs[halves:-3], refs[-3:]
    b = step_id()
    last = last_step()
    rows_blk, d_model = table_ref.shape
    cols = d_model // LANES
    n_edge = edge_ref.shape[0] // n_list

    def chunk_copies(l, k, act):
        src, sem, at = stage_ref.at[l, pl.ds(k * CHUNK, CHUNK)], sems.at[l, k], k * CHUNK

        @pl.when(at < base)
        def _():
            getattr(pltpu.make_async_copy(src, base_refs[l // n_dev].at[pl.ds(l % n_dev * base + at, CHUNK)], sem), act)()

        if extra:
            @pl.when(at >= base)
            def _():
                getattr(pltpu.make_async_copy(src, extra_refs[l].at[pl.ds(at - base, CHUNK)], sem), act)()

    @pl.loop(0, rows_blk // GROUP)
    def _(g):
        for j in range(cols):
            lin_ref[column(g, j), :] = table_ref[group(g), lane(j)].astype(F32)

    origin = b * (rows_blk * PITCH)
    for l in range(n_list):
        first = edge_ref[l * n_edge]
        lo = jnp.minimum(edge_ref[l * n_edge + b] - first, base + extra)
        hi = jnp.minimum(edge_ref[l * n_edge + b + 1] - first, base + extra)
        at = l * n_tok + first

        @pl.loop(0, shift_of(hi - lo + UNROLL - 1, UNROLL))
        def _(i):
            p = lo + i * UNROLL
            vals = [lin_ref[pl.ds(jnp.minimum(rows_ref[at + p + u] - origin, (rows_blk - 1) * PITCH), cols), :] for u in range(UNROLL)]
            for u in range(UNROLL):
                stage_ref[l, p + u] = vals[u].astype(BF16)

        @pl.loop(shift_of(lo, CHUNK), jnp.where(last, shift_of(hi + CHUNK - 1, CHUNK), shift_of(hi, CHUNK)))
        def _(k):
            chunk_copies(l, k, 'start')

    @pl.when(last)
    def _():
        for l in range(n_list):
            total = jnp.minimum(edge_ref[(l + 1) * n_edge - 1] - edge_ref[l * n_edge], base + extra)

            @pl.loop(0, shift_of(total + CHUNK - 1, CHUNK))
            def _(k):
                chunk_copies(l, k, 'wait')


def row_spots(rows):
    return jnp.pad(jnp.minimum(rows, NO_ROW // PITCH).reshape(-1) * PITCH, (0, UNROLL))


def pick_rows(table, rows, edges, n_dev, base, extra):
    n_list, n_tok = rows.shape
    n_rows, d_model = table.shape
    cols = d_model // LANES
    out = [struct((n_dev * base, cols, LANES), BF16)] * (n_list // n_dev) + [struct((extra, cols, LANES), BF16)] * (n_list if extra else 0)
    return pl.pallas_call(
        functools.partial(pick_body, n_list, n_dev, n_tok, base, extra),
        grid_spec=pltpu.PrefetchScalarGridSpec(
            num_scalar_prefetch=2, grid=(n_rows // TABLE_BLOCK,), in_specs=[row_spec(TABLE_BLOCK, d_model)], out_specs=[HBM] * len(out),
            scratch_shapes=[
                pltpu.VMEM((TABLE_BLOCK * PITCH, LANES), F32),
                pltpu.VMEM((n_list, base + extra + UNROLL, cols, LANES), BF16),
                pltpu.SemaphoreType.DMA((n_list, (base + extra) // CHUNK))]),
        out_shape=out, compiler_params=params(FULL), name="pick_rows", cost_estimate=CHEAP,
    )(row_spots(rows), edges.reshape(-1), table)


def spread_body(pieces, rank_ref, slot_ref, gain_ref, *refs):
    piece_refs, (h0_ref, x_ref, lin_ref, recv_ref, sems) = refs[:len(pieces)], refs[len(pieces):]
    i = step_id()
    rows_blk, d_model = h0_ref.shape
    cols = d_model // LANES

    @pl.when(i == 0)
    def _():
        for act in ('start', 'wait'):
            for n, (to, size, device) in enumerate(pieces):
                @pl.when((lax.axis_index('fsdp') == device) if device is not None else (i == 0))
                def _():
                    getattr(pltpu.make_async_copy(piece_refs[n], recv_ref.at[pl.ds(to, size)], sems.at[n]), act)()

    @pl.loop(0, rows_blk // UNROLL)
    def _(t0):
        for u in range(UNROLL):
            t = t0 * UNROLL + u
            lin_ref[pl.ds(t * PITCH, cols), :] = recv_ref[slot_ref[rank_ref[i * rows_blk + t]]].astype(F32)

    @pl.loop(0, rows_blk // (HALVES * GROUP))
    def _(g):
        groups = []
        for u in range(HALVES):
            tiles = [lin_ref[column(2 * g + u, j), :] for j in range(cols)]
            groups.append((tiles, rowsum(tree_sum([v * v for v in tiles]))))
        for u, (tiles, square) in enumerate(groups):
            inv = inverse_rms(square, d_model)
            for j, v in enumerate(tiles):
                at = (group(2 * g + u), lane(j))
                h0_ref[at] = v.astype(BF16)
                x_ref[at] = (v * inv * gain_ref[:, lane(j)]).astype(BF16)


def spread_rows(pieces, rank, slot, gain, n_slots):
    n_tok, d_model = rank.shape[0], gain.shape[0]
    cols = d_model // LANES
    blk = 128
    rows = row_spec(blk, d_model)
    plan = [(to, v.shape[0], device) for v, to, device in pieces]
    return pl.pallas_call(
        functools.partial(spread_body, plan),
        grid_spec=pltpu.PrefetchScalarGridSpec(
            num_scalar_prefetch=2, grid=(n_tok // blk,), in_specs=[whole_spec((1, d_model))] + [HBM] * len(pieces), out_specs=[rows, rows],
            scratch_shapes=[pltpu.VMEM((blk * PITCH, LANES), F32), pltpu.VMEM((n_slots, cols, LANES), BF16), pltpu.SemaphoreType.DMA((len(pieces),))]),
        out_shape=[struct((n_tok, d_model), BF16)] * 2, compiler_params=params(SMALL), name="spread_rows",
        cost_estimate=CHEAP,
    )(rank, slot, gain.reshape(1, d_model), *[v for v, _, _ in pieces])


def rope_tables(seq_len):
    pos = np.arange(seq_len, dtype=np.float32)
    inv_freq = (np.float32(ROPE_THETA) ** (np.float32(-2.0) * np.arange(ROPE_DIM // 2, dtype=np.float32) / np.float32(ROPE_DIM))).astype(np.float32)
    angle = (pos[:, None] * inv_freq[None, :]).astype(np.float32).astype(np.float64)
    cos, sin, zero = np.cos(angle), np.sin(angle), np.zeros_like(angle)
    full = lambda lo, hi: np.concatenate([lo, hi, lo, hi], axis=1).astype(np.float32)
    return full(cos, cos), full(-sin, zero), full(zero, sin)


def turn(vals, cos, sin_lo, sin_hi, sign=1.0):
    half = ROPE_DIM // 2
    return vals * cos + sign * (rotate(vals, LANES - half) * sin_lo + rotate(vals, half) * sin_hi)


def attn_body(q_ref, pe_ref, kv_ref, do_ref, cos_ref, sin_lo_ref, sin_hi_ref,
              o_ref, dq_ref, dkv_ref, dpe_ref, krot_ref, qcat_ref, p_ref, ds_ref, dkrot_ref):
    pair = pl.program_id(1)
    seq_len = q_ref.shape[0]
    blk = 128
    n_blk = seq_len // blk
    low = low_lanes()

    @pl.when(pair == 0)
    def _():
        pe = pe_ref[:].astype(F32)
        pe = jnp.where(low, pe, rotate(pe, ROPE_DIM))
        krot_ref[:] = turn(pe, cos_ref[:], sin_lo_ref[:], sin_hi_ref[:]).astype(BF16)
        dkrot_ref[:] = jnp.zeros_like(dkrot_ref)

    qrot = turn(q_ref[:, PAIR:].astype(F32), cos_ref[:], sin_lo_ref[:], sin_hi_ref[:])
    for h in range(HALVES):
        mine = low if h == 0 else ~low
        qcat_ref[h, :, :LANES] = q_ref[:, lane(h)]
        qcat_ref[h, :, LANES:] = jnp.where(mine, qrot, 0.0).astype(BF16)
    causal = lax.broadcasted_iota(jnp.int32, (blk, blk), 0) >= lax.broadcasted_iota(jnp.int32, (blk, blk), 1)
    blocks = [(h, i, slice(i * blk, (i + 1) * blk), (i + 1) * blk) for i in reversed(range(n_blk)) for h in range(HALVES)]
    key = lambda h: lane(2 * h)
    val = lambda h: lane(2 * h + 1)
    head = lane
    kcat = lambda h, seen: jnp.concatenate([kv_ref[:seen, key(h)], krot_ref[:seen]], axis=1)
    scores = [lax.dot_general(qcat_ref[h, here], kcat(h, seen), COL_DIMS, preferred_element_type=F32) for h, i, here, seen in blocks]
    dps = [lax.dot_general(do_ref[here, head(h)], kv_ref[:seen, val(h)], COL_DIMS, preferred_element_type=F32) for h, i, here, seen in blocks]
    for (h, i, here, seen), s, dp in zip(blocks, scores, dps):
        diag = jnp.where(causal, s[:, i * blk:], -1e30)
        s = diag if i == 0 else jnp.concatenate([s[:, :i * blk], diag], axis=1)
        e = jnp.exp2((s - jnp.max(s, axis=-1, keepdims=True)) * (ATTN_SCALE * math.log2(math.e)))
        p = e * (1.0 / rowsum(e))
        p_ref[h, here, :seen] = p.astype(BF16)
        ds_ref[h, here, :seen] = (p * (dp - rowsum(dp * p)) * ATTN_SCALE).astype(BF16)
    dqrots = [[], []]
    for h, i, here, seen in blocks:
        o_ref[here, head(h)] = jnp.dot(p_ref[h, here, :seen], kv_ref[:seen, val(h)], preferred_element_type=F32).astype(BF16)
        dqi = jnp.dot(ds_ref[h, here, :seen], kcat(h, seen), preferred_element_type=F32)
        dq_ref[here, head(h)] = dqi[:, :LANES].astype(BF16)
        dqrots[h].append(dqi[:, LANES:])
    for h in range(HALVES):
        for j in range(n_blk):
            here, later = slice(j * blk, (j + 1) * blk), slice(j * blk, seq_len)
            dv = lax.dot_general(p_ref[h, later, here], do_ref[later, head(h)], ROW_DIMS, preferred_element_type=F32)
            dk = lax.dot_general(ds_ref[h, later, here], qcat_ref[h, later], ROW_DIMS, preferred_element_type=F32)
            dkv_ref[here, val(h)] = dv.astype(BF16)
            dkv_ref[here, key(h)] = dk[:, :LANES].astype(BF16)
            dkrot_ref[here] += dk[:, LANES:]
    for n, i in enumerate(reversed(range(n_blk))):
        here = slice(i * blk, (i + 1) * blk)
        dqr = jnp.where(low, dqrots[0][n], dqrots[1][n]).astype(BF16).astype(F32)
        dq_ref[here, PAIR:] = turn(dqr, cos_ref[here], sin_lo_ref[here], sin_hi_ref[here], -1.0).astype(BF16)

    @pl.when(pair == pl.num_programs(1) - 1)
    def _():
        both = dkrot_ref[:]
        both = (both + rotate(both, ROPE_DIM)).astype(BF16).astype(F32)
        dpe = turn(both, cos_ref[:], sin_lo_ref[:], sin_hi_ref[:], -1.0)
        dpe_ref[:] = jnp.where(low, dpe, 0.0).astype(BF16)


def attend(qx, kv, d_mix, first_seq, seq_count, pe_block):
    tok = qx.shape[0]
    seq_len = tok // seq_count
    pairs = d_mix.shape[1] // (2 * VALUE_DIM)
    tabs = [jnp.asarray(t) for t in rope_tables(seq_len)]
    at = lambda width: pl.BlockSpec((seq_len, width), lambda s, j: (s, j))
    tab = whole_spec((seq_len, LANES))
    shape = lambda w: struct((tok, w), BF16)
    return pl.pallas_call(
        attn_body, grid=(seq_count, pairs),
        in_specs=[at(3 * LANES), pl.BlockSpec((seq_len, LANES), lambda s, j: (s, pe_block)), at(4 * LANES), pl.BlockSpec((seq_len, PAIR), lambda s, j: (s + first_seq, j)), tab, tab, tab],
        out_specs=[at(PAIR), at(3 * LANES), at(4 * LANES), pl.BlockSpec((seq_len, LANES), lambda s, j: (s, 0))],
        out_shape=[shape(pairs * PAIR), shape(qx.shape[1]), shape(pairs * 4 * LANES), shape(LANES)],
        scratch_shapes=[pltpu.VMEM((seq_len, LANES), BF16), pltpu.VMEM((2, seq_len, PAIR), BF16),
                        pltpu.VMEM((2, seq_len, seq_len), BF16), pltpu.VMEM((2, seq_len, seq_len), BF16),
                        pltpu.VMEM((seq_len, LANES), F32)],
        compiler_params=params(SMALL), name="attention",
        cost_estimate=cost(qx.size * tok, qx.size),
    )(qx, qx, kv, d_mix, *tabs)


def latent_body(w_ref, c_ref, pe_ref, gain_ref, _, out_ref, dgain_ref, gacc_ref):
    i = step_id()
    rank = gain_ref.shape[1]

    @pl.when(i == 0)
    def _():
        gacc_ref[:] = jnp.zeros_like(gacc_ref)

    c = c_ref[:].astype(F32)
    w = w_ref[:].astype(F32)
    inv = inverse_rms(rowsum(c * c), rank)
    hat = c * inv
    gacc_ref[:] += jnp.sum((w * hat).reshape(-1, 8, rank), axis=0)
    w = w * gain_ref[:]
    out_ref[:, :rank] = (inv * (w - hat * (rowsum(w * hat) / rank))).astype(BF16)
    out_ref[:, rank:] = pe_ref[:]

    @pl.when(last_step())
    def _():
        dgain_ref[:] = jnp.sum(gacc_ref[:], axis=0, keepdims=True)


def latent_back(d_latent, qx, d_pe, gain, d_qx, latent_at):
    tok, rank = d_latent.shape
    blk = 3 * LANES
    wide = lambda width, at: pl.BlockSpec((pl.Element(blk), pl.Element(width)), lambda i: (i * blk, at))
    return pl.pallas_call(
        latent_body, grid=(tok // blk,),
        in_specs=[row_spec(blk, rank), wide(rank, latent_at), row_spec(blk, LANES), whole_spec((1, rank)), HBM],
        out_specs=[wide(rank + LANES, latent_at), whole_spec((1, rank))],
        out_shape=[struct(d_qx.shape, BF16), struct((1, rank), F32)],
        scratch_shapes=[pltpu.VMEM((8, rank), F32)], input_output_aliases={4: 0}, name="latent_back",
        cost_estimate=CHEAP,
    )(d_latent, qx, d_pe, gain.reshape(1, rank), d_qx)


def merge_body(rank_ref, slot_ref, dx_ref, h0_ref, dy_ref, gain_ref, base_ref, extra_ref, dgain_ref, even_ref, odd_ref, acc_ref, gacc_ref, sem):
    i = step_id()
    rows_blk, d_model = h0_ref.shape
    cols = d_model // LANES

    @pl.when(i == 0)
    def _():
        gacc_ref[:] = jnp.zeros_like(gacc_ref)

        @pl.loop(0, acc_ref.shape[0] // 8)
        def _(r):
            acc_ref[pl.ds(r * 8, 8)] = jnp.zeros((8,) + acc_ref.shape[1:], F32)

    lanes = [lane(j) for j in range(cols)]

    def derive(g, lin_ref):
        rows = group(g)
        squares, crosses = [], []
        for at in lanes:
            v = h0_ref[rows, at].astype(F32)
            squares.append(v * v)
            crosses.append(v * (dx_ref[rows, at].astype(F32) * gain_ref[:, at]))
        inv = inverse_rms(rowsum(tree_sum(squares)), d_model)
        mean = rowsum(tree_sum(crosses)) * inv / d_model
        for j, at in enumerate(lanes):
            hat = h0_ref[rows, at].astype(F32) * inv
            w = dx_ref[rows, at].astype(F32)
            gacc_ref[:, at] += w * hat
            lin_ref[column(0, j), :] = inv * (w * gain_ref[:, at] - hat * mean) + dy_ref[rows, at].astype(F32)

    def add(g, lin_ref):
        for t in range(GROUP):
            r = slot_ref[rank_ref[i * rows_blk + g * GROUP + t]]
            acc_ref[r] = acc_ref[r] + lin_ref[pl.ds(t * PITCH, cols), :]

    derive(0, even_ref)
    pairs = rows_blk // (HALVES * GROUP)

    @pl.loop(0, pairs - 1)
    def _(g):
        add(2 * g, even_ref)
        derive(2 * g + 1, odd_ref)
        add(2 * g + 1, odd_ref)
        derive(2 * g + 2, even_ref)

    add(2 * pairs - 2, even_ref)
    derive(2 * pairs - 1, odd_ref)
    add(2 * pairs - 1, odd_ref)

    @pl.when(last_step())
    def _():
        dgain_ref[:] = jnp.sum(gacc_ref[:], axis=0, keepdims=True)
        split = base_ref.shape[0]
        copies = [pltpu.make_async_copy(acc_ref.at[pl.ds(0, split)], base_ref, sem.at[0]),
                  pltpu.make_async_copy(acc_ref.at[pl.ds(split, extra_ref.shape[0])], extra_ref, sem.at[1])]
        for copy in copies:
            copy.start()
        for copy in copies:
            copy.wait()


def merge_rows(dx, h0, dy, dy_at, gain, rank, slot, base, extra):
    n_tok, d_model = h0.shape
    cols = d_model // LANES
    blk = 128
    rows = row_spec(blk, d_model)
    return pl.pallas_call(
        merge_body,
        grid_spec=pltpu.PrefetchScalarGridSpec(
            num_scalar_prefetch=2, grid=(n_tok // blk,),
            in_specs=[rows, rows, pl.BlockSpec((blk, d_model), lambda i, *_: (i + dy_at // blk, 0)), whole_spec((1, d_model))],
            out_specs=[HBM, HBM, whole_spec((1, d_model))],
            scratch_shapes=[pltpu.VMEM((GROUP * PITCH, LANES), F32)] * 2 + [ pltpu.VMEM((base + extra, cols, LANES), F32),
                            pltpu.VMEM((GROUP, d_model), F32), pltpu.SemaphoreType.DMA((2,))]),
        out_shape=[struct((base, cols, LANES), F32), struct((extra, cols, LANES), F32), struct((1, d_model), F32)],
        compiler_params=params(SMALL), name="merge_rows",
        cost_estimate=CHEAP,
    )(rank, slot, dx, h0, dy, gain.reshape(1, d_model))


def add_body(n_dev, n_tok, halves, rows_ref, edge_ref, *refs):
    flat, (out_ref, acc_ref, ring_ref, sems) = list(refs[:-4]), refs[-4:]
    sources = []
    for stride, base, extras in halves:
        first = flat.pop(0)
        more = [[flat.pop(0) for _ in range(n)] for n in extras]
        sources += [(first, d * stride, base, more[d] if extras else []) for d in range(n_dev)]
    b = step_id()
    n_blk = pl.num_programs(0)
    rows_blk, d_model = out_ref.shape
    cols = d_model // LANES
    n_edge = edge_ref.shape[0] // len(sources)
    size, ring = CHUNK, ADD_RING

    def landing(s, k):
        return ring_ref.at[s, pl.ds((k & (ring - 1)) * size, size)], sems.at[s, k & (ring - 1)]

    def chunk_start(s, k):
        first, at, base, more = sources[s]
        dst, sem = landing(s, k)

        @pl.when(k * size < base)
        def _():
            pltpu.make_async_copy(first.at[pl.ds(at + k * size, size)], dst, sem).start()

        for ref in more:
            @pl.when((k * size >= base) & (k * size < base + ref.shape[0]))
            def _():
                pltpu.make_async_copy(ref.at[pl.ds(k * size - base, size)], dst, sem).start()

            base = base + ref.shape[0]

    def chunk_wait(s, k):
        dst, sem = landing(s, k)
        pltpu.make_async_copy(sources[s][0].at[pl.ds(0, size)], dst, sem).wait()

    def chunks_of(s):
        return shift_of(edge_ref[s * n_edge + n_blk] - edge_ref[s * n_edge] + size - 1, size)

    @pl.when(b == 0)
    def _():
        for s in range(len(sources)):
            @pl.loop(0, jnp.minimum(chunks_of(s), ring))
            def _(k):
                chunk_start(s, k)

    @pl.loop(0, rows_blk // GROUP)
    def _(r):
        for u in range(HALVES * PITCH):
            acc_ref[pl.ds((r * HALVES * PITCH + u) * 8, 8), :] = jnp.zeros((8, LANES), F32)

    for s in range(len(sources)):
        first = edge_ref[s * n_edge]
        lo = edge_ref[s * n_edge + b] - first
        hi = edge_ref[s * n_edge + b + 1] - first
        at = s * n_tok + first
        origin = b * (rows_blk * PITCH)

        @pl.when(hi > lo)
        def _():
            @pl.loop(shift_of(lo, size), shift_of(hi - 1, size) + 1)
            def _(k):
                start = jnp.maximum(lo, k * size)
                stop = jnp.minimum(hi, (k + 1) * size)

                @pl.when(start == k * size)
                def _():
                    chunk_wait(s, k)

                @pl.loop(0, shift_of(stop - start + UNROLL - 1, UNROLL))
                def _(i):
                    p = start + i * UNROLL
                    spots, sums = [], []
                    for u in range(UNROLL):
                        spots.append(pl.ds(jnp.where(p + u < stop, rows_ref[at + p + u] - origin, rows_blk * PITCH), cols))
                        sums.append(acc_ref[spots[u], :] + ring_ref[s, (p + u) & (ring * size - 1)])
                    for u in range(UNROLL):
                        acc_ref[spots[u], :] = sums[u]

                @pl.when((stop == (k + 1) * size) & (k + ring < chunks_of(s)))
                def _():
                    chunk_start(s, k + ring)

    @pl.loop(0, rows_blk // GROUP)
    def _(g):
        for j in range(cols):
            out_ref[group(g), lane(j)] = acc_ref[column(g, j), :].astype(BF16)


def add_rows(halves, rows, edges, n_dev, n_rows):
    n_list, n_tok = rows.shape
    cols = halves[0][0].shape[1]
    d_model = cols * LANES
    runs = [[v if isinstance(v, tuple) else (v,) for v in more] for *_, more in halves]
    arrays = [v for half, more in zip(halves, runs) for v in [half[0]] + [u for run in more for u in run]]
    block = HALVES * TABLE_BLOCK
    edges = edges[:, ::HALVES]
    return pl.pallas_call(
        functools.partial(add_body, n_dev, n_tok, [(stride, base, [len(run) for run in more]) for (_, stride, base, _), more in zip(halves, runs)]),
        grid_spec=pltpu.PrefetchScalarGridSpec(
            num_scalar_prefetch=2, grid=(n_rows // block,), in_specs=[HBM] * len(arrays), out_specs=row_spec(block, d_model),
            scratch_shapes=[pltpu.VMEM(((block + 1) * PITCH, LANES), F32),
                            pltpu.VMEM((n_list, ADD_RING * CHUNK, cols, LANES), F32),
                            pltpu.SemaphoreType.DMA((n_list, ADD_RING))]),
        out_shape=struct((n_rows, d_model), BF16), compiler_params=params(FULL), name="add_rows", cost_estimate=CHEAP,
    )(row_spots(rows), edges.reshape(-1), *arrays)


def exchange_body(base, n_extra, n_dev, base_ref, *refs):
    extra_refs, (lhs_ref, rhs_ref, out_ref, via_ref, prod_ref, send_sems, recv_sems, hop_send, hop_recv, end_send, end_recv, own_sems) = refs[:n_extra], refs[n_extra:]
    place = lax.axis_index('fsdp')
    far, side = n_dev - 2, n_dev // 2
    across = lambda m: [((m ^ far) & ~1) | c for c in range(HALVES)]

    def moves(src, dst):
        runs = [(0, base_ref, dst * base, src * base, base)]
        if n_extra and src == 0:
            runs.append((1, extra_refs[dst], 0, n_dev * base, extra_refs[dst].shape[0]))
        out = []
        for kind, ref, at, to, n in runs:
            by = 0 if (src ^ dst) & far != far else (n // 2, n, 0, n // 2)[src >> 1]
            out.append((kind, ref, at, to, n - by, by))
        return out

    def remote(src, dst, send, recv, to):
        return pltpu.make_async_remote_copy(src, dst, send, recv, device_id={'fsdp': to}, device_id_type=pl.DeviceIdType.MESH)

    def direct(src, dst):
        return [remote(ref.at[pl.ds(at, n)], out_ref.at[pl.ds(to, n)], send_sems.at[kind * n_dev + dst], recv_sems.at[kind * n_dev + src], dst)
                for kind, ref, at, to, n, _ in moves(src, dst) if n]

    def hop(src, dst):
        out = []
        for kind, ref, at, _, n, by in moves(src, dst):
            lot = HALVES * kind + (dst & 1)
            if by:
                out.append(remote(ref.at[pl.ds(at + n, by)], via_ref.at[lot, pl.ds(0, by)], hop_send.at[lot], hop_recv.at[lot], src ^ side))
        return out

    def end(src, dst):
        return [remote(via_ref.at[HALVES * kind + (dst & 1), pl.ds(0, by)], out_ref.at[pl.ds(to + n, by)], end_send.at[HALVES * kind + (dst & 1)], end_recv.at[HALVES * kind + (src & 1)], dst)
                for kind, _, _, to, n, by in moves(src, dst) if by]

    def own(m):
        return [pltpu.make_async_copy(ref.at[pl.ds(at, n)], out_ref.at[pl.ds(to, n)], own_sems.at[kind]) for kind, ref, at, to, n, _ in moves(m, m)]

    each = lambda copies, act: [getattr(c, act)() for c in copies]

    @pl.when(step_id() == 0)
    def _():
        for m in range(n_dev):
            @pl.when(place == m)
            def _():
                for dst in across(m):
                    each(hop(m, dst), 'start')
                for k in reversed(range(1, n_dev)):
                    each(direct(m, m ^ k), 'start')
                each(own(m), 'start')

    for n in range(0, prod_ref.shape[1], PAIR * HALVES):
        cols = slice(n, n + PAIR * HALVES)
        prod_ref[:, cols] = lax.dot_general(lhs_ref[:], rhs_ref[cols], COL_DIMS, preferred_element_type=F32).astype(BF16)

    @pl.when(last_step())
    def _():
        for m in range(n_dev):
            @pl.when(place == m)
            def _():
                for dst in across(m ^ side):
                    each(hop(m ^ side, dst), 'wait_recv')
                    each(end(m ^ side, dst), 'start')
                each(own(m), 'wait')
                for dst in across(m):
                    each(hop(m, dst), 'wait_send')
                for k in range(1, n_dev):
                    each(direct(m, m ^ k), 'wait_send')
                    each(direct(m ^ k, m), 'wait_recv')
                for dst in across(m ^ side):
                    each(end(m ^ side, dst), 'wait_send')
                for src in across(m):
                    each(end(src, m), 'wait_recv')


def exchange(base_rows, extras, n_dev, lhs, rhs):
    rows, *cols = base_rows.shape
    base, extra = rows // n_dev, extras[0].shape[0] if extras else 0
    quad, pair = (pltpu.SemaphoreType.DMA((n,)) for n in (4, HALVES * n_dev))
    near = (rhs.shape[0], lhs.shape[1])
    shapes = [(rows + extra, *cols), (4, max(base, extra), *cols), (lhs.shape[0], near[0])]
    return pl.pallas_call(
        functools.partial(exchange_body, base, len(extras), n_dev), grid=(lhs.shape[0] // PAIR,), out_shape=[struct(v, BF16 if v == shapes[-1] else base_rows.dtype) for v in shapes],
        in_specs=[HBM] * (len(extras) + 1) + [row_spec(PAIR, near[1]), whole_spec(near, pipeline_mode=pl.Buffered(1))], out_specs=[HBM, HBM, row_spec(PAIR, near[0])],
        scratch_shapes=[pair, pair, quad, quad, quad, quad, quad],
        compiler_params=params(SMALL, has_side_effects=True), name="exchange", cost_estimate=cost(lhs.size * lhs.size, lhs.size),
    )(base_rows, *extras, lhs, rhs)[::HALVES]


def fetch_beside(base, extras):
    got = base_beside(base)
    more = [v if d == 0 else lax.ppermute(v, 'fsdp', [(0, d)]) for d, v in enumerate(extras)]
    return [got] + more


def bring_beside(extra, n_dev):
    last = n_dev - 1
    cut = extra.shape[0] // (HALVES * CHUNK) * CHUNK
    via = lax.ppermute(extra[cut:], 'fsdp', [(last, last ^ (n_dev // HALVES))])
    return [extra if s == 0 else lax.ppermute(extra if s < last else extra[:cut], 'fsdp', [(s, 0)]) for s in range(n_dev)], via


def join(extras, rest):
    return extras[:-1] + [(extras[-1], rest)]


def base_beside(base):
    return lax.all_to_all(base, 'fsdp', 0, 0, tiled=True)


def weight_body(n_rhs, steps, lhs_a_ref, lhs_b_ref, *refs):
    rhs_refs, (out_ref, turned_ref, rhs_ref, sems) = refs[:n_rhs], refs[n_rhs:]
    i = step_id()
    half = lhs_a_ref.shape[0]
    width = rhs_ref.shape[1]
    rows = rhs_ref.shape[0] // n_rhs

    def fill(j, n):
        cols = pl.ds(pl.multiple_of(j * steps, steps), n)
        return [pltpu.make_async_copy(v.at[:, cols], rhs_ref.at[pl.ds(k * rows, rows), cols], sems.at[k, j]) for k, v in enumerate(rhs_refs)]

    pieces = [(j, min(steps, width - j * steps)) for j in range(-(-width // steps))]

    @pl.when(i == 0)
    def _():
        for j, n in pieces:
            for copy in fill(j, n):
                copy.start()

    turned_ref[:, :half] = lhs_a_ref[:].T
    turned_ref[:, half:] = lhs_b_ref[:].T

    def product(at, n):
        out_ref[:, pl.ds(at, n)] = jnp.dot(turned_ref[:], rhs_ref[:, pl.ds(at, n)], preferred_element_type=F32)

    whole = width // steps

    @pl.loop(0, whole)
    def _(j):
        @pl.when(i == 0)
        def _():
            for copy in fill(j, steps):
                copy.wait()

        product(pl.multiple_of(j * steps, steps), steps)

    for j, n in pieces[whole:]:
        @pl.when(i == 0)
        def _():
            for copy in fill(j, n):
                copy.wait()

        product(j * steps, n)


def weight_grad(lhs_a, lhs_b, *rhs, more=0):
    half, height = lhs_a.shape
    width = rhs[0].shape[1]
    steps = 512
    blk = min(512, height)
    left = pl.BlockSpec((half, blk), lambda i: (0, i))
    return pl.pallas_call(
        functools.partial(weight_body, len(rhs), steps), grid=(height // blk,), in_specs=[left, left] + [HBM] * len(rhs), out_specs=row_spec(blk, width),
        out_shape=struct((height, width + more), F32),
        scratch_shapes=[pltpu.VMEM((blk, HALVES * half), BF16), pltpu.VMEM((HALVES * half, width), BF16), pltpu.SemaphoreType.DMA((len(rhs), -(-width // steps)))],
        compiler_params=params(FULL), name="weight_grad", cost_estimate=cost(lhs_a.size * width, lhs_a.size),
    )(lhs_a, lhs_b, *rhs)


def cut_body(order_ref, lhs_a_ref, lhs_b_ref, tail_ref, rhs_a_ref, rhs_b_ref, far_ref, near_ref, turned_ref, rhs_ref, sems):
    i = step_id()
    half = lhs_a_ref.shape[0]
    width = rhs_ref.shape[1]
    steps = 512
    whole = width // steps

    def fill(j, n, act):
        cols = pl.ds(pl.multiple_of(j * steps, steps), n)
        for k, v in enumerate((rhs_a_ref, rhs_b_ref)):
            getattr(pltpu.make_async_copy(v.at[:, cols], rhs_ref.at[pl.ds(k * half, half), cols], sems.at[k, j]), act)()

    @pl.when(i == 0)
    def _():
        @pl.loop(0, whole)
        def _(j):
            fill(j, steps, 'start')

        fill(whole, width - whole * steps, 'start')

    turned_ref[:, :half] = lhs_a_ref[:].T
    turned_ref[:, half:] = lhs_b_ref[:].T

    def product(j, n, out_ref):
        @pl.when(i == 0)
        def _():
            fill(j, n, 'wait')

        cols = pl.ds(pl.multiple_of(j * steps, steps), n)
        out_ref[:, cols] = jnp.dot(turned_ref[:], rhs_ref[:, cols], preferred_element_type=F32)

    far = i < pl.num_programs(0) // HALVES
    for mine, out_ref in ((far, far_ref), (~far, near_ref)):
        @pl.when(mine)
        def _():
            @pl.loop(0, whole)
            def _(j):
                product(j, steps, out_ref)

            product(whole, width - whole * steps, out_ref)
            out_ref[:, lane(width // LANES - 1)] += tail_ref[:]


def weight_grad_cut(lhs_a, lhs_b, tail, rhs_a, rhs_b, order):
    half, height = lhs_a.shape
    width = rhs_a.shape[1]
    n = order.shape[0]
    blk = height // n
    left = pl.BlockSpec((half, blk), lambda i, o: (0, o[i]))
    return pl.pallas_call(
        cut_body,
        grid_spec=pltpu.PrefetchScalarGridSpec(
            num_scalar_prefetch=1, grid=(n,), in_specs=[left, left, pl.BlockSpec((blk, LANES), lambda i, o: (o[i], 0)), HBM, HBM],
            out_specs=[pl.BlockSpec((blk, width), lambda i, o: (jnp.minimum(i, n // HALVES - 1), 0)),
                       pl.BlockSpec((blk, width), lambda i, o: (jnp.maximum(i - n // HALVES, 0), 0))],
            scratch_shapes=[pltpu.VMEM((blk, HALVES * half), BF16), pltpu.VMEM((HALVES * half, width), BF16), pltpu.SemaphoreType.DMA((HALVES, width // 512 + 1))]),
        out_shape=[struct((height // HALVES, width), F32)] * HALVES,
        compiler_params=params(FULL), name="weight_grad_cut", cost_estimate=cost(lhs_a.size * width, lhs_a.size),
    )(order, lhs_a, lhs_b, tail, rhs_a, rhs_b)


def sum_in_steps(far, near, n_dev, beside, hold):
    swap = lambda v, k: lax.ppermute(v, 'fsdp', [(i, i ^ k) for i in range(n_dev)])
    core, x, y = 1, 2, 4
    blocks = lambda v: v.reshape(n_dev // HALVES, -1, v.shape[1])
    at = far.shape[1] // PAIR * LANES
    other = swap(far, core)
    other, = beside(other)
    total = blocks(near) + blocks(other)
    left, right = hold(total[1::2, :, :at], total[2:, :, at:])
    left, right = swap(left, x), swap(right, y)
    keep_left, keep_right = total[::2, :, :at], total[:2, :, at:]
    left, right, keep_left, keep_right = beside(left, right, keep_left, keep_right)
    left, right = keep_left + left, keep_right + right
    last_left, last_right = swap(left[1], y), swap(right[1], x)
    return jnp.concatenate([left[0] + last_left, right[0] + last_right], axis=1)


def beside_body(lhs_a_ref, lhs_b_ref, rhs_a_ref, rhs_b_ref, _, out_ref, turned_ref):
    half = lhs_a_ref.shape[0]

    @pl.when(step_id() == 0)
    def _():
        turned_ref[:, :half] = lhs_a_ref[:].T
        turned_ref[:, half:] = lhs_b_ref[:].T

    prod = jnp.dot(turned_ref[:, :half], rhs_a_ref[:], preferred_element_type=F32)
    prod = prod + jnp.dot(turned_ref[:, half:], rhs_b_ref[:], preferred_element_type=F32)
    out_ref[:] = prod.reshape(out_ref.shape)


def weight_grad_beside(big, at, lhs_a, lhs_b, rhs_a, rhs_b, n_dev):
    half, height = lhs_a.shape
    rows, width = big.shape
    part = width - at
    parts = rhs_a.shape[1] // part
    big = big.reshape(n_dev, rows // n_dev, width)
    right = pl.BlockSpec((half, part), lambda q: (0, q))
    return pl.pallas_call(
        beside_body, grid=(parts,), in_specs=[whole_spec(lhs_a.shape)] * 2 + [right, right, HBM],
        out_specs=pl.BlockSpec((n_dev, height // n_dev, part), lambda q: (0, q, at // part)), out_shape=struct(big.shape, F32),
        scratch_shapes=[pltpu.VMEM((height, HALVES * half), BF16)], input_output_aliases={4: 0}, compiler_params=params(LARGE), name="weight_grad_beside",
        cost_estimate=cost(lhs_a.size * rhs_a.shape[1], lhs_a.size),
    )(lhs_a, lhs_b, rhs_a, rhs_b, big).reshape(rows, width)


def move_body(count_ref, from_ref, to_ref, x_ref, out_ref, sems):
    depth = sems.shape[0]

    @pl.loop(0, count_ref.shape[0])
    def _(o):
        n = count_ref[o]

        def copy(i):
            return pltpu.make_async_copy(x_ref.at[pl.ds(from_ref[o] + i, 1)], out_ref.at[pl.ds(to_ref[o] + i, 1)], sems.at[lax.rem(i, depth)])

        @pl.loop(0, n)
        def _(i):
            @pl.when(i >= depth)
            def _():
                copy(i - depth).wait()

            copy(i).start()

        @pl.loop(jnp.maximum(n - depth, 0), n)
        def _(i):
            copy(i).wait()


def move_rows(x, count, start_from, start_to, n_out):
    return pl.pallas_call(
        move_body, out_shape=struct((n_out,) + x.shape[1:], x.dtype),
        in_specs=[SCALARS] * 3 + [HBM], out_specs=HBM, scratch_shapes=[pltpu.SemaphoreType.DMA((16,))],
        name="move_rows")(count, start_from, start_to, x)


def rms_scale(in_vals, gain_vec):
    vals_f32 = in_vals.astype(F32)
    inv_rms = lax.rsqrt(jnp.mean(vals_f32 * vals_f32, axis=-1, keepdims=True) + RMS_EPS)
    return (vals_f32 * inv_rms * gain_vec).astype(BF16)


def dot(a, b, dims):
    return lax.dot_general(a, b, dims, preferred_element_type=F32)


NN = (((1,), (0,)), ((), ()))


def pack_body(o_ref, q_ref, down_ref, tail_ref, out_ref):
    low = low_lanes()
    start, width = o_ref.shape[1] // LANES, q_ref.shape[1] // LANES
    out_ref[:, lane(0, start)] = o_ref[:]
    for j in range(0, width, 3):
        one, two, three = (q_ref[:, lane(j + k)].astype(F32) for k in range(3))
        out_ref[:, lane(start + j)] = one.astype(BF16)
        out_ref[:, lane(start + j + 1)] = jnp.where(low, rotate(two, ROPE_DIM), rotate(three, ROPE_DIM)).astype(BF16)
        out_ref[:, lane(start + j + 2)] = jnp.where(low, two, three).astype(BF16)
    out_ref[:, lane(start + width, down_ref.shape[1] // LANES)] = down_ref[:]
    out_ref[:, lane(out_ref.shape[1] // LANES - 1)] = tail_ref[:]


def pack_weights(w_out, w_query, w_kv_down, gains):
    rows, width = w_query.shape
    cut = w_kv_down.shape[1] // LANES * LANES
    tail = jnp.concatenate([w_kv_down[:, cut:]] + [jnp.pad(g, (0, rows - g.shape[0]))[:, None] for g in gains], axis=1)
    tail = jnp.pad(tail, ((0, 0), (0, LANES - tail.shape[1])))
    return pl.pallas_call(pack_body, out_shape=struct((rows, w_out.shape[1] + width + cut + LANES), BF16),
                          name="pack_weights")(w_out, w_query, w_kv_down[:, :cut], tail)


def unpack_body(g_ref, q_ref, down_ref):
    low = low_lanes()
    width = q_ref.shape[1] // LANES
    for j in range(0, width, 3):
        plain, rot = rotate(g_ref[:, lane(j + 1)], ROPE_DIM), g_ref[:, lane(j + 2)]
        q_ref[:, lane(j)] = g_ref[:, lane(j)]
        q_ref[:, lane(j + 1)] = jnp.where(low, rot, plain)
        q_ref[:, lane(j + 2)] = jnp.where(low, plain, rot)
    down_ref[:] = g_ref[:, q_ref.shape[1]:q_ref.shape[1] + down_ref.shape[1]]


def unpack_grads(g_x, q_width, down_width):
    rows = g_x.shape[0]
    return pl.pallas_call(unpack_body, out_shape=[struct((rows, q_width), F32), struct((rows, down_width), F32)], name="unpack_grads")(g_x)


def share_body(n_dev, x_ref, out_ref, send_sems, recv_sems):
    place = lax.axis_index('fsdp')
    for m in range(n_dev):
        @pl.when(place == m)
        def _():
            copies = [pltpu.make_async_remote_copy(x_ref, out_ref.at[m], send_sems.at[d], recv_sems.at[m], device_id={'fsdp': d}, device_id_type=pl.DeviceIdType.MESH)
                      for d in range(n_dev) if d != m]
            for copy in copies:
                copy.start()
            out_ref[m] = x_ref[:]
            for copy in copies:
                copy.wait_send()
            for s in range(n_dev):
                if s != m:
                    pltpu.make_async_remote_copy(x_ref, out_ref.at[s], send_sems.at[s], recv_sems.at[s], device_id={'fsdp': s}, device_id_type=pl.DeviceIdType.MESH).wait_recv()


def share(x, n_dev):
    vmem = pl.BlockSpec(memory_space=pltpu.VMEM)
    wide = pltpu.SemaphoreType.DMA((n_dev,))
    return pl.pallas_call(functools.partial(share_body, n_dev), out_shape=struct((n_dev,) + x.shape, x.dtype), in_specs=[vmem], out_specs=vmem,
                          scratch_shapes=[wide, wide], compiler_params=pltpu.CompilerParams(has_side_effects=True), name="share")(x)


def solution(mesh):
    n_dev = mesh.shape['fsdp']
    tok_spec = P(('dp', 'fsdp'), None)
    seq_spec = P(('dp', 'fsdp'), None, None)
    part_vec = P(('dp', 'fsdp'))
    vec_spec = P('fsdp')
    mat_spec = P('fsdp', None)

    def step(tok_ids, grad_out, emb_table, norm_gain, w_query, w_kv_down, kv_gain, w_kv_up, w_out):
        seq_count, seq_len = tok_ids.shape
        vocab_dev, d_model = emb_table.shape
        tok = seq_count * seq_len
        half = tok // HALVES
        per_half = seq_count // HALVES
        me = lax.axis_index('fsdp')
        gather = lambda piece: lax.all_gather(piece, 'fsdp', tiled=True)
        scatter = lambda full: lax.psum_scatter(full, 'fsdp', scatter_dimension=0, tiled=True)
        tie = lax.optimization_barrier
        rows_dev, q_width = w_query.shape
        rank_dev, = kv_gain.shape
        kv_rank = rank_dev * n_dev
        pe_at = q_width + kv_rank
        pad_at = pe_at + ROPE_DIM
        dy = grad_out.reshape(tok, d_model)
        w_ox = gather(pack_weights(w_out, w_query, w_kv_down, (norm_gain, kv_gain)))

        base, extra = [-(-round(half * share) // CHUNK) * CHUNK for share in (0.09, 0.31)]
        n_slots = n_dev * base + extra
        uniq, rank = unique_rows(tok_ids.reshape(HALVES, half))
        all_uniq = share(uniq.reshape(-1, LANES), n_dev).reshape(n_dev, HALVES, half)
        below = lambda lists, edges: jnp.sum(lists[..., None, :] < edges[:, None], axis=-1, dtype=jnp.int32)
        starts = below(all_uniq, jnp.arange(n_dev + 1, dtype=jnp.int32) * vocab_dev)
        counts = starts[..., 1:] - starts[..., :-1]
        fits = jnp.all(counts <= jnp.asarray([base + extra] + [base] * (n_dev - 1), jnp.int32))
        lists = jnp.swapaxes(all_uniq, 0, 1).reshape(HALVES * n_dev, half) - me * vocab_dev
        edges = below(lists, jnp.arange(vocab_dev // TABLE_BLOCK + 1, dtype=jnp.int32) * TABLE_BLOCK)
        my_starts, named = (lax.dynamic_index_in_dim(v, me, keepdims=False) for v in (starts[..., :-1], counts))
        place = jnp.arange(half, dtype=jnp.int32)
        begun = place[:, None] >= my_starts[:, None, 1:]
        slot = place + jnp.sum(jnp.where(begun, base - named[:, None, :-1], 0), axis=-1)
        slot = jnp.where((place >= base) & ~begun[..., 0], place + (n_dev - 1) * base, slot)
        slot = jnp.where(fits, slot, place)
        slots = jnp.arange(n_dev, dtype=jnp.int32) * half
        (rank_a, rank_b), (slot_a, slot_b) = rank, slot

        base_a, base_b, *extras = pick_rows(emb_table, lists, edges, n_dev, base, extra)
        extras_a, extras_b = extras[:n_dev], extras[n_dev:]

        def fetch_any(h):
            mine = slice(h * n_dev, (h + 1) * n_dev)
            far, = pick_rows(emb_table, lists[mine], edges[mine], n_dev, half, 0)
            far, prod = exchange(far, [], n_dev, dy, w_ox)
            return move_rows(far, named[h], slots, my_starts[h], n_slots), prod

        recv, d_mix = lax.cond(fits, lambda: tuple(exchange(base_a, extras_a, n_dev, dy, w_ox)), lambda: fetch_any(0))
        recv, w_ox, w_kv_up, base_b, extras_b = tie((recv, w_ox, w_kv_up, base_b, extras_b))
        w_o, w_x = w_ox[:, :d_model], w_ox[:, d_model:]
        w_up = gather(w_kv_up)
        pieces = fetch_beside(base_b, extras_b)
        gain_vec = w_x[:, pad_at].astype(F32)
        kv_gain_vec = w_x[:, pad_at + 1].reshape(n_dev, rows_dev)[:, :rank_dev].reshape(kv_rank).astype(F32)

        def compute(h, x):
            qx = dot(x, w_x, NN).astype(BF16)
            latent = rms_scale(qx[:, q_width:pe_at], kv_gain_vec)
            kv = dot(latent, w_up, NN).astype(BF16)
            return (qx, latent) + tuple(attend(qx, kv, d_mix, h * per_half, per_half, pe_at // LANES))

        def descend(qx, d_qx, d_kv, d_pe):
            d_latent = dot(d_kv, w_up, COL_DIMS).astype(BF16)
            return latent_back(d_latent, qx, d_pe, kv_gain_vec, d_qx, q_width)

        h0_a, x_a = spread_rows([(recv, 0, None)], rank_a, slot_a, gain_vec, n_slots)
        qx_a, latent_a, mix_a, d_qx_a, d_kv_a, d_pe_a = compute(0, x_a)
        d_qx_a, kv_gain_a = descend(qx_a, d_qx_a, d_kv_a, d_pe_a)
        d_x = dot(d_qx_a, w_x, COL_DIMS).astype(BF16)
        *merged_a, gain_a = merge_rows(d_x, h0_a, dy, 0, gain_vec, rank_a, slot_a, n_dev * base, extra)
        (extra_a, via), got_a = bring_beside(merged_a[1], n_dev), base_beside(merged_a[0])

        pieces, gain_a = tie((pieces, gain_a))
        h0_b, x_b = lax.cond(
            fits, lambda v: spread_rows([(v[0], 0, None)] + [(p, n_dev * base, d) for d, p in enumerate(v[1:])], rank_b, slot_b, gain_vec, n_slots),
            lambda v: spread_rows([(fetch_any(1)[0], 0, None)], rank_b, slot_b, gain_vec, n_slots), pieces)
        qx_b, latent_b, mix_b, d_qx_b, d_kv_b, d_pe_b = compute(1, x_b)
        via, d_kv_b = tie((via, d_kv_b))
        extra_a = join(extra_a, lax.ppermute(via, 'fsdp', [(n_dev // HALVES - 1, 0)]))
        d_qx_b, kv_gain_b = descend(qx_b, d_qx_b, d_kv_b, d_pe_b)
        d_x = dot(d_qx_b, w_x, COL_DIMS).astype(BF16)
        *merged_b, gain_b = merge_rows(d_x, h0_b, dy, half, gain_vec, rank_b, slot_b, n_dev * base, extra)
        extra_b, via = bring_beside(merged_b[1], n_dev)

        mix_a, gain_b = tie((mix_a, gain_b))
        d_w_o = weight_grad(mix_a, mix_b, dy, more=w_up.size // d_model)
        d_w_o = weight_grad_beside(d_w_o, d_model, latent_a, latent_b, d_kv_a, d_kv_b, n_dev)
        g_o = scatter(d_w_o)
        x_a, d_w_o, merged_b[0], got_a, via = tie((x_a, d_w_o, merged_b[0], got_a, via))
        extra_b = join(extra_b, lax.ppermute(via, 'fsdp', [(n_dev // HALVES - 1, 0)]))
        got_b = base_beside(merged_b[0])
        kv_rows = jnp.pad((kv_gain_a + kv_gain_b).reshape(n_dev, rank_dev), ((0, 0), (0, rows_dev - rank_dev)))
        tail = jnp.stack([(gain_a + gain_b).reshape(d_model), kv_rows.reshape(d_model)], axis=1)
        tail = jnp.pad(tail, ((0, 0), (ROPE_DIM, LANES - ROPE_DIM - HALVES)))
        steps = jnp.arange(n_dev, dtype=jnp.int32)
        order = me ^ (jnp.where(steps < n_dev // HALVES, HALVES * steps + 1, HALVES * steps - n_dev))
        far, near = weight_grad_cut(x_a, x_b, tail, d_qx_a, d_qx_b, order)

        def bring_any(h, merged):
            far = move_rows(jnp.concatenate(merged, axis=0), named[h], my_starts[h], slots, n_dev * half)
            return exchange(far, [], n_dev, dy, w_ox)[0]

        made, rows_b = [], [(got_b, extra_b)]

        def hold(left, right):
            left, right, rows_b[0] = tie((left, right, rows_b[0]))
            return left, right

        def beside(*values):
            if not made:
                h0, mix, *values = tie((h0_a, mix_a, far))[:2] + tuple(values)
                outs = [(h0.astype(F32) + dot(mix, w_o, NN)).astype(BF16), (h0_b.astype(F32) + dot(mix_b, w_o, NN)).astype(BF16)]
                *outs, values[0] = tie((*outs, values[0]))
                made.append(jnp.concatenate(outs, axis=0))
            else:
                values = list(values)
                edges_now, values[2] = tie((edges, values[2]))
                made.append(lax.cond(
                    fits, lambda: add_rows([(got_a, base, base, extra_a), (rows_b[0][0], base, base, rows_b[0][1])], lists, edges_now, n_dev, vocab_dev),
                    lambda: add_rows([(bring_any(h, v), half, half, []) for h, v in enumerate((merged_a, merged_b))], lists, edges_now, n_dev, vocab_dev)))
                made[1], values[0] = tie((made[1], values[0]))
            return values

        g_x = sum_in_steps(far, near, n_dev, beside, hold)
        out, grad_table = made
        g_up = jnp.swapaxes(g_o[:, d_model:].reshape(-1, rank_dev, g_o.shape[1] - d_model), 0, 1).reshape(w_kv_up.shape)
        g_query, g_down = unpack_grads(g_x, q_width, pad_at - q_width)
        return (out.reshape(seq_count, seq_len, d_model), grad_table, g_x[:, pad_at], g_query,
                g_down, g_x[:rank_dev, pad_at + 1], g_up, g_o[:, :d_model])

    return jax.shard_map(step, mesh=mesh, in_specs=(tok_spec, seq_spec, mat_spec, vec_spec, mat_spec, mat_spec, vec_spec, mat_spec, mat_spec), out_specs=(seq_spec, tok_spec, part_vec, tok_spec, tok_spec, part_vec, tok_spec, tok_spec), check_vma=False)
```

```python
import functools
import math
import jax
import jax.numpy as jnp
import numpy as np
from jax import lax
from jax.experimental import pallas as pl
from jax.experimental.pallas import tpu as pltpu
from jax.sharding import PartitionSpec as P

NOPE_DIM = 128
ROPE_DIM = 64
VALUE_DIM = 128
ROPE_THETA = 50000.0
RMS_EPS = 1e-6
ATTN_SCALE = (NOPE_DIM + ROPE_DIM) ** -0.5 * (0.1 * math.log(32.0) + 1.0) ** 2
ROW_DIMS = (((0,), (0,)), ((), ()))
COL_DIMS = (((1,), (1,)), ((), ()))
LANES = 128
HALVES = 2
PAIR = 2 * LANES
TABLE_BLOCK = 1024
CHUNK = 16
GROUP = 16
ADD_RING = 4
UNROLL = 8
NO_ROW = 1 << 30
PITCH = 17
F32 = jnp.float32
BF16 = jnp.bfloat16
SMEM = pltpu.SMEM
ANY = pl.ANY
HBM = pl.BlockSpec(memory_space=ANY)
SCALARS = pl.BlockSpec(memory_space=SMEM)


def step_id():
    return pl.program_id(0)


def last_step():
    return pl.program_id(0) == pl.num_programs(0) - 1


def shift_of(x, n):
    return lax.shift_right_logical(x, n.bit_length() - 1)


def lane(j, n=1):
    return slice(j * LANES, (j + n) * LANES)


def low_lanes():
    return lax.broadcasted_iota(jnp.int32, (1, LANES), 1) < ROPE_DIM


def rotate(x, n):
    return pltpu.roll(x, n, 1)


def column(g, j):
    return pl.ds(g * GROUP * PITCH + j, GROUP, stride=PITCH)


def group(g):
    return pl.ds(g * GROUP, GROUP)


def rowsum(x):
    return jnp.sum(x, axis=-1, keepdims=True)


def tree_sum(terms):
    while len(terms) > 1:
        terms = [a + b for a, b in zip(terms[::2], terms[1::2])]
    return terms[0]


def inverse_rms(square_sum, width):
    return lax.rsqrt(square_sum * (1.0 / width) + RMS_EPS)


def row_spec(blk, width):
    return pl.BlockSpec((blk, width), lambda i, *_: (i, 0))


def whole_spec(shape, **kw):
    return pl.BlockSpec(shape, lambda *_: (0,) * len(shape), **kw)


def struct(shape, dtype):
    return jax.ShapeDtypeStruct(shape, dtype)


def cost(flops, size):
    return pl.CostEstimate(flops=int(flops), bytes_accessed=int(size), transcendentals=0)


CHEAP = cost(6e7, 1e7)
SMALL, LARGE, FULL = 40, 48, 62


def params(vmem_mib, **kw):
    return pltpu.CompilerParams(vmem_limit_bytes=vmem_mib << 20, **kw)


def unique_body(shift, halves, keys_ref, uniq_ref, rank_ref, count_ref):
    n = keys_ref.shape[0] // halves
    for h in range(halves):
        def step(i, carry):
            k, prev = carry
            for j in range(UNROLL):
                key = keys_ref[h * n + i * UNROLL + j]
                row = lax.shift_right_logical(key, shift)
                k = k + (row != prev).astype(jnp.int32)
                uniq_ref[h * n + k] = row
                rank_ref[h * n + (key & ((1 << shift) - 1))] = k
                prev = row
            return k, prev

        k, _ = lax.fori_loop(0, n // UNROLL, step, (jnp.int32(-1), jnp.int32(-1)))
        count_ref[h] = k + 1


def unique_rows(ids):
    halves, n = ids.shape
    shift = (n - 1).bit_length()
    keys = lax.sort(ids * (1 << shift) + jnp.arange(n, dtype=jnp.int32), dimension=1)
    flat = struct((halves * n,), jnp.int32)
    uniq, rank, count = pl.pallas_call(
        functools.partial(unique_body, shift, halves), out_shape=[flat, flat, struct((halves,), jnp.int32)],
        in_specs=[SCALARS], out_specs=[SCALARS] * 3, name="unique_rows")(keys.reshape(-1))
    known = jnp.arange(n, dtype=jnp.int32) < count[:, None]
    return jnp.where(known, uniq.reshape(halves, n), NO_ROW), rank.reshape(halves, n)


def pick_body(n_list, n_dev, n_tok, base, extra, rows_ref, edge_ref, table_ref, *refs):
    halves = n_list // n_dev
    base_refs, extra_refs, (lin_ref, stage_ref, sems) = refs[:halves], refs[halves:-3], refs[-3:]
    b = step_id()
    last = last_step()
    rows_blk, d_model = table_ref.shape
    cols = d_model // LANES
    n_edge = edge_ref.shape[0] // n_list

    def chunk_copies(l, k, act):
        src, sem, at = stage_ref.at[l, pl.ds(k * CHUNK, CHUNK)], sems.at[l, k], k * CHUNK

        @pl.when(at < base)
        def _():
            getattr(pltpu.make_async_copy(src, base_refs[l // n_dev].at[pl.ds(l % n_dev * base + at, CHUNK)], sem), act)()

        if extra:
            @pl.when(at >= base)
            def _():
                getattr(pltpu.make_async_copy(src, extra_refs[l].at[pl.ds(at - base, CHUNK)], sem), act)()

    @pl.loop(0, rows_blk // GROUP)
    def _(g):
        for j in range(cols):
            lin_ref[column(g, j), :] = table_ref[group(g), lane(j)].astype(F32)

    origin = b * (rows_blk * PITCH)
    for l in range(n_list):
        first = edge_ref[l * n_edge]
        lo = jnp.minimum(edge_ref[l * n_edge + b] - first, base + extra)
        hi = jnp.minimum(edge_ref[l * n_edge + b + 1] - first, base + extra)
        at = l * n_tok + first

        @pl.loop(0, shift_of(hi - lo + UNROLL - 1, UNROLL))
        def _(i):
            p = lo + i * UNROLL
            vals = [lin_ref[pl.ds(jnp.minimum(rows_ref[at + p + u] - origin, (rows_blk - 1) * PITCH), cols), :] for u in range(UNROLL)]
            for u in range(UNROLL):
                stage_ref[l, p + u] = vals[u].astype(BF16)

        @pl.loop(shift_of(lo, CHUNK), jnp.where(last, shift_of(hi + CHUNK - 1, CHUNK), shift_of(hi, CHUNK)))
        def _(k):
            chunk_copies(l, k, 'start')

    @pl.when(last)
    def _():
        for l in range(n_list):
            total = jnp.minimum(edge_ref[(l + 1) * n_edge - 1] - edge_ref[l * n_edge], base + extra)

            @pl.loop(0, shift_of(total + CHUNK - 1, CHUNK))
            def _(k):
                chunk_copies(l, k, 'wait')


def row_spots(rows):
    return jnp.pad(jnp.minimum(rows, NO_ROW // PITCH).reshape(-1) * PITCH, (0, UNROLL))


def pick_rows(table, rows, edges, n_dev, base, extra):
    n_list, n_tok = rows.shape
    n_rows, d_model = table.shape
    cols = d_model // LANES
    out = [struct((n_dev * base, cols, LANES), BF16)] * (n_list // n_dev) + [struct((extra, cols, LANES), BF16)] * (n_list if extra else 0)
    return pl.pallas_call(
        functools.partial(pick_body, n_list, n_dev, n_tok, base, extra),
        grid_spec=pltpu.PrefetchScalarGridSpec(
            num_scalar_prefetch=2, grid=(n_rows // TABLE_BLOCK,), in_specs=[row_spec(TABLE_BLOCK, d_model)], out_specs=[HBM] * len(out),
            scratch_shapes=[
                pltpu.VMEM((TABLE_BLOCK * PITCH, LANES), F32),
                pltpu.VMEM((n_list, base + extra + UNROLL, cols, LANES), BF16),
                pltpu.SemaphoreType.DMA((n_list, (base + extra) // CHUNK))]),
        out_shape=out, compiler_params=params(FULL), name="pick_rows", cost_estimate=CHEAP,
    )(row_spots(rows), edges.reshape(-1), table)


def spread_body(pieces, rank_ref, slot_ref, gain_ref, *refs):
    piece_refs, (h0_ref, x_ref, lin_ref, recv_ref, sems) = refs[:len(pieces)], refs[len(pieces):]
    i = step_id()
    rows_blk, d_model = h0_ref.shape
    cols = d_model // LANES

    @pl.when(i == 0)
    def _():
        for act in ('start', 'wait'):
            for n, (to, size, device) in enumerate(pieces):
                @pl.when((lax.axis_index('fsdp') == device) if device is not None else (i == 0))
                def _():
                    getattr(pltpu.make_async_copy(piece_refs[n], recv_ref.at[pl.ds(to, size)], sems.at[n]), act)()

    @pl.loop(0, rows_blk // UNROLL)
    def _(t0):
        for u in range(UNROLL):
            t = t0 * UNROLL + u
            lin_ref[pl.ds(t * PITCH, cols), :] = recv_ref[slot_ref[rank_ref[i * rows_blk + t]]].astype(F32)

    @pl.loop(0, rows_blk // (HALVES * GROUP))
    def _(g):
        groups = []
        for u in range(HALVES):
            tiles = [lin_ref[column(2 * g + u, j), :] for j in range(cols)]
            groups.append((tiles, rowsum(tree_sum([v * v for v in tiles]))))
        for u, (tiles, square) in enumerate(groups):
            inv = inverse_rms(square, d_model)
            for j, v in enumerate(tiles):
                at = (group(2 * g + u), lane(j))
                h0_ref[at] = v.astype(BF16)
                x_ref[at] = (v * inv * gain_ref[:, lane(j)]).astype(BF16)


def spread_rows(pieces, rank, slot, gain, n_slots):
    n_tok, d_model = rank.shape[0], gain.shape[0]
    cols = d_model // LANES
    blk = 128
    rows = row_spec(blk, d_model)
    plan = [(to, v.shape[0], device) for v, to, device in pieces]
    return pl.pallas_call(
        functools.partial(spread_body, plan),
        grid_spec=pltpu.PrefetchScalarGridSpec(
            num_scalar_prefetch=2, grid=(n_tok // blk,), in_specs=[whole_spec((1, d_model))] + [HBM] * len(pieces), out_specs=[rows, rows],
            scratch_shapes=[pltpu.VMEM((blk * PITCH, LANES), F32), pltpu.VMEM((n_slots, cols, LANES), BF16), pltpu.SemaphoreType.DMA((len(pieces),))]),
        out_shape=[struct((n_tok, d_model), BF16)] * 2, compiler_params=params(SMALL), name="spread_rows",
        cost_estimate=CHEAP,
    )(rank, slot, gain.reshape(1, d_model), *[v for v, _, _ in pieces])


def rope_tables(seq_len):
    pos = np.arange(seq_len, dtype=np.float32)
    inv_freq = (np.float32(ROPE_THETA) ** (np.float32(-2.0) * np.arange(ROPE_DIM // 2, dtype=np.float32) / np.float32(ROPE_DIM))).astype(np.float32)
    angle = (pos[:, None] * inv_freq[None, :]).astype(np.float32).astype(np.float64)
    cos, sin, zero = np.cos(angle), np.sin(angle), np.zeros_like(angle)
    full = lambda lo, hi: np.concatenate([lo, hi, lo, hi], axis=1).astype(np.float32)
    return full(cos, cos), full(-sin, zero), full(zero, sin)


def turn(vals, cos, sin_lo, sin_hi, sign=1.0):
    half = ROPE_DIM // 2
    return vals * cos + sign * (rotate(vals, LANES - half) * sin_lo + rotate(vals, half) * sin_hi)


def attn_body(q_ref, pe_ref, kv_ref, do_ref, cos_ref, sin_lo_ref, sin_hi_ref,
              o_ref, dq_ref, dkv_ref, dpe_ref, krot_ref, qcat_ref, p_ref, ds_ref, dkrot_ref):
    pair = pl.program_id(1)
    seq_len = q_ref.shape[0]
    blk = 128
    n_blk = seq_len // blk
    low = low_lanes()

    @pl.when(pair == 0)
    def _():
        pe = pe_ref[:].astype(F32)
        pe = jnp.where(low, pe, rotate(pe, ROPE_DIM))
        krot_ref[:] = turn(pe, cos_ref[:], sin_lo_ref[:], sin_hi_ref[:]).astype(BF16)
        dkrot_ref[:] = jnp.zeros_like(dkrot_ref)

    qrot = turn(q_ref[:, PAIR:].astype(F32), cos_ref[:], sin_lo_ref[:], sin_hi_ref[:])
    for h in range(HALVES):
        mine = low if h == 0 else ~low
        qcat_ref[h, :, :LANES] = q_ref[:, lane(h)]
        qcat_ref[h, :, LANES:] = jnp.where(mine, qrot, 0.0).astype(BF16)
    causal = lax.broadcasted_iota(jnp.int32, (blk, blk), 0) >= lax.broadcasted_iota(jnp.int32, (blk, blk), 1)
    blocks = [(h, i, slice(i * blk, (i + 1) * blk), (i + 1) * blk) for i in reversed(range(n_blk)) for h in range(HALVES)]
    key = lambda h: lane(2 * h)
    val = lambda h: lane(2 * h + 1)
    head = lane
    kcat = lambda h, seen: jnp.concatenate([kv_ref[:seen, key(h)], krot_ref[:seen]], axis=1)
    scores = [lax.dot_general(qcat_ref[h, here], kcat(h, seen), COL_DIMS, preferred_element_type=F32) for h, i, here, seen in blocks]
    dps = [lax.dot_general(do_ref[here, head(h)], kv_ref[:seen, val(h)], COL_DIMS, preferred_element_type=F32) for h, i, here, seen in blocks]
    for (h, i, here, seen), s, dp in zip(blocks, scores, dps):
        diag = jnp.where(causal, s[:, i * blk:], -1e30)
        s = diag if i == 0 else jnp.concatenate([s[:, :i * blk], diag], axis=1)
        e = jnp.exp2((s - jnp.max(s, axis=-1, keepdims=True)) * (ATTN_SCALE * math.log2(math.e)))
        p = e * (1.0 / rowsum(e))
        p_ref[h, here, :seen] = p.astype(BF16)
        ds_ref[h, here, :seen] = (p * (dp - rowsum(dp * p)) * ATTN_SCALE).astype(BF16)
    dqrots = [[], []]
    for h, i, here, seen in blocks:
        o_ref[here, head(h)] = jnp.dot(p_ref[h, here, :seen], kv_ref[:seen, val(h)], preferred_element_type=F32).astype(BF16)
        dqi = jnp.dot(ds_ref[h, here, :seen], kcat(h, seen), preferred_element_type=F32)
        dq_ref[here, head(h)] = dqi[:, :LANES].astype(BF16)
        dqrots[h].append(dqi[:, LANES:])
    for h in range(HALVES):
        for j in range(n_blk):
            here, later = slice(j * blk, (j + 1) * blk), slice(j * blk, seq_len)
            dv = lax.dot_general(p_ref[h, later, here], do_ref[later, head(h)], ROW_DIMS, preferred_element_type=F32)
            dk = lax.dot_general(ds_ref[h, later, here], qcat_ref[h, later], ROW_DIMS, preferred_element_type=F32)
            dkv_ref[here, val(h)] = dv.astype(BF16)
            dkv_ref[here, key(h)] = dk[:, :LANES].astype(BF16)
            dkrot_ref[here] += dk[:, LANES:]
    for n, i in enumerate(reversed(range(n_blk))):
        here = slice(i * blk, (i + 1) * blk)
        dqr = jnp.where(low, dqrots[0][n], dqrots[1][n]).astype(BF16).astype(F32)
        dq_ref[here, PAIR:] = turn(dqr, cos_ref[here], sin_lo_ref[here], sin_hi_ref[here], -1.0).astype(BF16)

    @pl.when(pair == pl.num_programs(1) - 1)
    def _():
        both = dkrot_ref[:]
        both = (both + rotate(both, ROPE_DIM)).astype(BF16).astype(F32)
        dpe = turn(both, cos_ref[:], sin_lo_ref[:], sin_hi_ref[:], -1.0)
        dpe_ref[:] = jnp.where(low, dpe, 0.0).astype(BF16)


def attend(qx, kv, d_mix, first_seq, seq_count, pe_block):
    tok = qx.shape[0]
    seq_len = tok // seq_count
    pairs = d_mix.shape[1] // (2 * VALUE_DIM)
    tabs = [jnp.asarray(t) for t in rope_tables(seq_len)]
    at = lambda width: pl.BlockSpec((seq_len, width), lambda s, j: (s, j))
    tab = whole_spec((seq_len, LANES))
    shape = lambda w: struct((tok, w), BF16)
    return pl.pallas_call(
        attn_body, grid=(seq_count, pairs),
        in_specs=[at(3 * LANES), pl.BlockSpec((seq_len, LANES), lambda s, j: (s, pe_block)), at(4 * LANES), pl.BlockSpec((seq_len, PAIR), lambda s, j: (s + first_seq, j)), tab, tab, tab],
        out_specs=[at(PAIR), at(3 * LANES), at(4 * LANES), pl.BlockSpec((seq_len, LANES), lambda s, j: (s, 0))],
        out_shape=[shape(pairs * PAIR), shape(qx.shape[1]), shape(pairs * 4 * LANES), shape(LANES)],
        scratch_shapes=[pltpu.VMEM((seq_len, LANES), BF16), pltpu.VMEM((2, seq_len, PAIR), BF16),
                        pltpu.VMEM((2, seq_len, seq_len), BF16), pltpu.VMEM((2, seq_len, seq_len), BF16),
                        pltpu.VMEM((seq_len, LANES), F32)],
        compiler_params=params(SMALL), name="attention",
        cost_estimate=cost(qx.size * tok, qx.size),
    )(qx, qx, kv, d_mix, *tabs)


def latent_body(w_ref, c_ref, pe_ref, gain_ref, _, out_ref, dgain_ref, gacc_ref):
    i = step_id()
    rank = gain_ref.shape[1]

    @pl.when(i == 0)
    def _():
        gacc_ref[:] = jnp.zeros_like(gacc_ref)

    c = c_ref[:].astype(F32)
    w = w_ref[:].astype(F32)
    inv = inverse_rms(rowsum(c * c), rank)
    hat = c * inv
    gacc_ref[:] += jnp.sum((w * hat).reshape(-1, 8, rank), axis=0)
    w = w * gain_ref[:]
    out_ref[:, :rank] = (inv * (w - hat * (rowsum(w * hat) / rank))).astype(BF16)
    out_ref[:, rank:] = pe_ref[:]

    @pl.when(last_step())
    def _():
        dgain_ref[:] = jnp.sum(gacc_ref[:], axis=0, keepdims=True)


def latent_back(d_latent, qx, d_pe, gain, d_qx, latent_at):
    tok, rank = d_latent.shape
    blk = 3 * LANES
    wide = lambda width, at: pl.BlockSpec((pl.Element(blk), pl.Element(width)), lambda i: (i * blk, at))
    return pl.pallas_call(
        latent_body, grid=(tok // blk,),
        in_specs=[row_spec(blk, rank), wide(rank, latent_at), row_spec(blk, LANES), whole_spec((1, rank)), HBM],
        out_specs=[wide(rank + LANES, latent_at), whole_spec((1, rank))],
        out_shape=[struct(d_qx.shape, BF16), struct((1, rank), F32)],
        scratch_shapes=[pltpu.VMEM((8, rank), F32)], input_output_aliases={4: 0}, name="latent_back",
        cost_estimate=CHEAP,
    )(d_latent, qx, d_pe, gain.reshape(1, rank), d_qx)


def merge_body(rank_ref, slot_ref, dx_ref, h0_ref, dy_ref, gain_ref, base_ref, extra_ref, dgain_ref, even_ref, odd_ref, acc_ref, gacc_ref, sem):
    i = step_id()
    rows_blk, d_model = h0_ref.shape
    cols = d_model // LANES

    @pl.when(i == 0)
    def _():
        gacc_ref[:] = jnp.zeros_like(gacc_ref)

        @pl.loop(0, acc_ref.shape[0] // 8)
        def _(r):
            acc_ref[pl.ds(r * 8, 8)] = jnp.zeros((8,) + acc_ref.shape[1:], F32)

    lanes = [lane(j) for j in range(cols)]

    def derive(g, lin_ref):
        rows = group(g)
        squares, crosses = [], []
        for at in lanes:
            v = h0_ref[rows, at].astype(F32)
            squares.append(v * v)
            crosses.append(v * (dx_ref[rows, at].astype(F32) * gain_ref[:, at]))
        inv = inverse_rms(rowsum(tree_sum(squares)), d_model)
        mean = rowsum(tree_sum(crosses)) * inv / d_model
        for j, at in enumerate(lanes):
            hat = h0_ref[rows, at].astype(F32) * inv
            w = dx_ref[rows, at].astype(F32)
            gacc_ref[:, at] += w * hat
            lin_ref[column(0, j), :] = inv * (w * gain_ref[:, at] - hat * mean) + dy_ref[rows, at].astype(F32)

    def add(g, lin_ref):
        for t in range(GROUP):
            r = slot_ref[rank_ref[i * rows_blk + g * GROUP + t]]
            acc_ref[r] = acc_ref[r] + lin_ref[pl.ds(t * PITCH, cols), :]

    derive(0, even_ref)
    pairs = rows_blk // (HALVES * GROUP)

    @pl.loop(0, pairs - 1)
    def _(g):
        add(2 * g, even_ref)
        derive(2 * g + 1, odd_ref)
        add(2 * g + 1, odd_ref)
        derive(2 * g + 2, even_ref)

    add(2 * pairs - 2, even_ref)
    derive(2 * pairs - 1, odd_ref)
    add(2 * pairs - 1, odd_ref)

    @pl.when(last_step())
    def _():
        dgain_ref[:] = jnp.sum(gacc_ref[:], axis=0, keepdims=True)
        split = base_ref.shape[0]
        copies = [pltpu.make_async_copy(acc_ref.at[pl.ds(0, split)], base_ref, sem.at[0]),
                  pltpu.make_async_copy(acc_ref.at[pl.ds(split, extra_ref.shape[0])], extra_ref, sem.at[1])]
        for copy in copies:
            copy.start()
        for copy in copies:
            copy.wait()


def merge_rows(dx, h0, dy, dy_at, gain, rank, slot, base, extra):
    n_tok, d_model = h0.shape
    cols = d_model // LANES
    blk = 128
    rows = row_spec(blk, d_model)
    return pl.pallas_call(
        merge_body,
        grid_spec=pltpu.PrefetchScalarGridSpec(
            num_scalar_prefetch=2, grid=(n_tok // blk,),
            in_specs=[rows, rows, pl.BlockSpec((blk, d_model), lambda i, *_: (i + dy_at // blk, 0)), whole_spec((1, d_model))],
            out_specs=[HBM, HBM, whole_spec((1, d_model))],
            scratch_shapes=[pltpu.VMEM((GROUP * PITCH, LANES), F32)] * 2 + [ pltpu.VMEM((base + extra, cols, LANES), F32),
                            pltpu.VMEM((GROUP, d_model), F32), pltpu.SemaphoreType.DMA((2,))]),
        out_shape=[struct((base, cols, LANES), F32), struct((extra, cols, LANES), F32), struct((1, d_model), F32)],
        compiler_params=params(SMALL), name="merge_rows",
        cost_estimate=CHEAP,
    )(rank, slot, dx, h0, dy, gain.reshape(1, d_model))


def add_body(n_dev, n_tok, halves, rows_ref, edge_ref, *refs):
    flat, (out_ref, acc_ref, ring_ref, sems) = list(refs[:-4]), refs[-4:]
    sources = []
    for stride, base, extras in halves:
        first = flat.pop(0)
        more = [flat.pop(0) for _ in range(extras)]
        sources += [(first, d * stride, base, more[d] if extras else None) for d in range(n_dev)]
    b = step_id()
    n_blk = pl.num_programs(0)
    rows_blk, d_model = out_ref.shape
    cols = d_model // LANES
    n_edge = edge_ref.shape[0] // len(sources)
    size, ring = CHUNK, ADD_RING

    def landing(s, k):
        return ring_ref.at[s, pl.ds((k & (ring - 1)) * size, size)], sems.at[s, k & (ring - 1)]

    def chunk_start(s, k):
        first, at, base, more = sources[s]
        dst, sem = landing(s, k)

        @pl.when(k * size < base)
        def _():
            pltpu.make_async_copy(first.at[pl.ds(at + k * size, size)], dst, sem).start()

        if more is not None:
            @pl.when(k * size >= base)
            def _():
                pltpu.make_async_copy(more.at[pl.ds(k * size - base, size)], dst, sem).start()

    def chunk_wait(s, k):
        dst, sem = landing(s, k)
        pltpu.make_async_copy(sources[s][0].at[pl.ds(0, size)], dst, sem).wait()

    def chunks_of(s):
        return shift_of(edge_ref[s * n_edge + n_blk] - edge_ref[s * n_edge] + size - 1, size)

    @pl.when(b == 0)
    def _():
        for s in range(len(sources)):
            @pl.loop(0, jnp.minimum(chunks_of(s), ring))
            def _(k):
                chunk_start(s, k)

    @pl.loop(0, rows_blk // GROUP)
    def _(r):
        for u in range(HALVES * PITCH):
            acc_ref[pl.ds((r * HALVES * PITCH + u) * 8, 8), :] = jnp.zeros((8, LANES), F32)

    for s in range(len(sources)):
        first = edge_ref[s * n_edge]
        lo = edge_ref[s * n_edge + b] - first
        hi = edge_ref[s * n_edge + b + 1] - first
        at = s * n_tok + first
        origin = b * (rows_blk * PITCH)

        @pl.when(hi > lo)
        def _():
            @pl.loop(shift_of(lo, size), shift_of(hi - 1, size) + 1)
            def _(k):
                start = jnp.maximum(lo, k * size)
                stop = jnp.minimum(hi, (k + 1) * size)

                @pl.when(start == k * size)
                def _():
                    chunk_wait(s, k)

                @pl.loop(0, shift_of(stop - start + UNROLL - 1, UNROLL))
                def _(i):
                    p = start + i * UNROLL
                    spots, sums = [], []
                    for u in range(UNROLL):
                        spots.append(pl.ds(jnp.where(p + u < stop, rows_ref[at + p + u] - origin, rows_blk * PITCH), cols))
                        sums.append(acc_ref[spots[u], :] + ring_ref[s, (p + u) & (ring * size - 1)])
                    for u in range(UNROLL):
                        acc_ref[spots[u], :] = sums[u]

                @pl.when((stop == (k + 1) * size) & (k + ring < chunks_of(s)))
                def _():
                    chunk_start(s, k + ring)

    @pl.loop(0, rows_blk // GROUP)
    def _(g):
        for j in range(cols):
            out_ref[group(g), lane(j)] = acc_ref[column(g, j), :].astype(BF16)


def add_rows(halves, rows, edges, n_dev, n_rows):
    n_list, n_tok = rows.shape
    cols = halves[0][0].shape[1]
    d_model = cols * LANES
    arrays = [v for first, _, _, more in halves for v in [first] + more]
    block = HALVES * TABLE_BLOCK
    edges = edges[:, ::HALVES]
    return pl.pallas_call(
        functools.partial(add_body, n_dev, n_tok, [(stride, base, len(more)) for _, stride, base, more in halves]),
        grid_spec=pltpu.PrefetchScalarGridSpec(
            num_scalar_prefetch=2, grid=(n_rows // block,), in_specs=[HBM] * len(arrays), out_specs=row_spec(block, d_model),
            scratch_shapes=[pltpu.VMEM(((block + 1) * PITCH, LANES), F32),
                            pltpu.VMEM((n_list, ADD_RING * CHUNK, cols, LANES), F32),
                            pltpu.SemaphoreType.DMA((n_list, ADD_RING))]),
        out_shape=struct((n_rows, d_model), BF16), compiler_params=params(FULL), name="add_rows", cost_estimate=CHEAP,
    )(row_spots(rows), edges.reshape(-1), *arrays)


def exchange_body(base, n_extra, n_dev, base_ref, *refs):
    extra_refs, (lhs_ref, rhs_ref, out_ref, via_ref, prod_ref, send_sems, recv_sems, hop_send, hop_recv, end_send, end_recv, own_sems) = refs[:n_extra], refs[n_extra:]
    place = lax.axis_index('fsdp')
    far, side = n_dev - 2, n_dev // 2
    across = lambda m: [((m ^ far) & ~1) | c for c in range(HALVES)]

    def moves(src, dst):
        runs = [(0, base_ref, dst * base, src * base, base)]
        if n_extra and src == 0:
            runs.append((1, extra_refs[dst], 0, n_dev * base, extra_refs[dst].shape[0]))
        out = []
        for kind, ref, at, to, n in runs:
            by = 0 if (src ^ dst) & far != far else (n // 2, n, 0, n // 2)[src >> 1]
            out.append((kind, ref, at, to, n - by, by))
        return out

    def remote(src, dst, send, recv, to):
        return pltpu.make_async_remote_copy(src, dst, send, recv, device_id={'fsdp': to}, device_id_type=pl.DeviceIdType.MESH)

    def direct(src, dst):
        return [remote(ref.at[pl.ds(at, n)], out_ref.at[pl.ds(to, n)], send_sems.at[kind * n_dev + dst], recv_sems.at[kind * n_dev + src], dst)
                for kind, ref, at, to, n, _ in moves(src, dst) if n]

    def hop(src, dst):
        out = []
        for kind, ref, at, _, n, by in moves(src, dst):
            lot = HALVES * kind + (dst & 1)
            if by:
                out.append(remote(ref.at[pl.ds(at + n, by)], via_ref.at[lot, pl.ds(0, by)], hop_send.at[lot], hop_recv.at[lot], src ^ side))
        return out

    def end(src, dst):
        return [remote(via_ref.at[HALVES * kind + (dst & 1), pl.ds(0, by)], out_ref.at[pl.ds(to + n, by)], end_send.at[HALVES * kind + (dst & 1)], end_recv.at[HALVES * kind + (src & 1)], dst)
                for kind, _, _, to, n, by in moves(src, dst) if by]

    def own(m):
        return [pltpu.make_async_copy(ref.at[pl.ds(at, n)], out_ref.at[pl.ds(to, n)], own_sems.at[kind]) for kind, ref, at, to, n, _ in moves(m, m)]

    each = lambda copies, act: [getattr(c, act)() for c in copies]

    @pl.when(step_id() == 0)
    def _():
        for m in range(n_dev):
            @pl.when(place == m)
            def _():
                for dst in across(m):
                    each(hop(m, dst), 'start')
                for k in reversed(range(1, n_dev)):
                    each(direct(m, m ^ k), 'start')
                each(own(m), 'start')

    for n in range(0, prod_ref.shape[1], PAIR * HALVES):
        cols = slice(n, n + PAIR * HALVES)
        prod_ref[:, cols] = lax.dot_general(lhs_ref[:], rhs_ref[cols], COL_DIMS, preferred_element_type=F32).astype(BF16)

    @pl.when(last_step())
    def _():
        for m in range(n_dev):
            @pl.when(place == m)
            def _():
                for dst in across(m ^ side):
                    each(hop(m ^ side, dst), 'wait_recv')
                    each(end(m ^ side, dst), 'start')
                each(own(m), 'wait')
                for dst in across(m):
                    each(hop(m, dst), 'wait_send')
                for k in range(1, n_dev):
                    each(direct(m, m ^ k), 'wait_send')
                    each(direct(m ^ k, m), 'wait_recv')
                for dst in across(m ^ side):
                    each(end(m ^ side, dst), 'wait_send')
                for src in across(m):
                    each(end(src, m), 'wait_recv')


def exchange(base_rows, extras, n_dev, lhs, rhs):
    rows, *cols = base_rows.shape
    base, extra = rows // n_dev, extras[0].shape[0] if extras else 0
    quad, pair = (pltpu.SemaphoreType.DMA((n,)) for n in (4, HALVES * n_dev))
    near = (rhs.shape[0], lhs.shape[1])
    shapes = [(rows + extra, *cols), (4, max(base, extra), *cols), (lhs.shape[0], near[0])]
    return pl.pallas_call(
        functools.partial(exchange_body, base, len(extras), n_dev), grid=(lhs.shape[0] // PAIR,), out_shape=[struct(v, BF16 if v == shapes[-1] else base_rows.dtype) for v in shapes],
        in_specs=[HBM] * (len(extras) + 1) + [row_spec(PAIR, near[1]), whole_spec(near, pipeline_mode=pl.Buffered(1))], out_specs=[HBM, HBM, row_spec(PAIR, near[0])],
        scratch_shapes=[pair, pair, quad, quad, quad, quad, quad],
        compiler_params=params(SMALL, has_side_effects=True), name="exchange", cost_estimate=cost(lhs.size * lhs.size, lhs.size),
    )(base_rows, *extras, lhs, rhs)[::HALVES]


def between(src, dst, n_dev):
    return [(src, dst), (dst, src)] + [(i, i) for i in range(n_dev) if i not in (src, dst)]


def fetch_beside(base, extras):
    got = base_beside(base)
    more = [v if d == 0 else lax.ppermute(v, 'fsdp', between(0, d, len(extras))) for d, v in enumerate(extras)]
    return [got] + more


def bring_beside(extra, n_dev):
    last = n_dev - 1
    via = lax.ppermute(extra, 'fsdp', [(last, last ^ (n_dev // HALVES))])
    return [extra if s == 0 else lax.ppermute(extra, 'fsdp', [(s, 0)]) for s in range(last)], via


def base_beside(base):
    return lax.all_to_all(base, 'fsdp', 0, 0, tiled=True)


def weight_body(n_rhs, steps, lhs_a_ref, lhs_b_ref, *refs):
    rhs_refs, (out_ref, turned_ref, rhs_ref, sems) = refs[:n_rhs], refs[n_rhs:]
    i = step_id()
    half = lhs_a_ref.shape[0]
    width = rhs_ref.shape[1]
    rows = rhs_ref.shape[0] // n_rhs

    def fill(j, n):
        cols = pl.ds(pl.multiple_of(j * steps, steps), n)
        return [pltpu.make_async_copy(v.at[:, cols], rhs_ref.at[pl.ds(k * rows, rows), cols], sems.at[k, j]) for k, v in enumerate(rhs_refs)]

    pieces = [(j, min(steps, width - j * steps)) for j in range(-(-width // steps))]

    @pl.when(i == 0)
    def _():
        for j, n in pieces:
            for copy in fill(j, n):
                copy.start()

    turned_ref[:, :half] = lhs_a_ref[:].T
    turned_ref[:, half:] = lhs_b_ref[:].T

    def product(at, n):
        out_ref[:, pl.ds(at, n)] = jnp.dot(turned_ref[:], rhs_ref[:, pl.ds(at, n)], preferred_element_type=F32)

    whole = width // steps

    @pl.loop(0, whole)
    def _(j):
        @pl.when(i == 0)
        def _():
            for copy in fill(j, steps):
                copy.wait()

        product(pl.multiple_of(j * steps, steps), steps)

    for j, n in pieces[whole:]:
        @pl.when(i == 0)
        def _():
            for copy in fill(j, n):
                copy.wait()

        product(j * steps, n)


def weight_grad(lhs_a, lhs_b, *rhs, more=0):
    half, height = lhs_a.shape
    width = rhs[0].shape[1]
    steps = 512
    blk = min(512, height)
    left = pl.BlockSpec((half, blk), lambda i: (0, i))
    return pl.pallas_call(
        functools.partial(weight_body, len(rhs), steps), grid=(height // blk,), in_specs=[left, left] + [HBM] * len(rhs), out_specs=row_spec(blk, width),
        out_shape=struct((height, width + more), F32),
        scratch_shapes=[pltpu.VMEM((blk, HALVES * half), BF16), pltpu.VMEM((HALVES * half, width), BF16), pltpu.SemaphoreType.DMA((len(rhs), -(-width // steps)))],
        compiler_params=params(FULL), name="weight_grad", cost_estimate=cost(lhs_a.size * width, lhs_a.size),
    )(lhs_a, lhs_b, *rhs)


def cut_body(order_ref, lhs_a_ref, lhs_b_ref, tail_ref, rhs_a_ref, rhs_b_ref, far_ref, near_ref, turned_ref, rhs_ref, sems):
    i = step_id()
    half = lhs_a_ref.shape[0]
    width = rhs_ref.shape[1]
    steps = 512
    whole = width // steps

    def fill(j, n, act):
        cols = pl.ds(pl.multiple_of(j * steps, steps), n)
        for k, v in enumerate((rhs_a_ref, rhs_b_ref)):
            getattr(pltpu.make_async_copy(v.at[:, cols], rhs_ref.at[pl.ds(k * half, half), cols], sems.at[k, j]), act)()

    @pl.when(i == 0)
    def _():
        @pl.loop(0, whole)
        def _(j):
            fill(j, steps, 'start')

        fill(whole, width - whole * steps, 'start')

    turned_ref[:, :half] = lhs_a_ref[:].T
    turned_ref[:, half:] = lhs_b_ref[:].T

    def product(j, n, out_ref):
        @pl.when(i == 0)
        def _():
            fill(j, n, 'wait')

        cols = pl.ds(pl.multiple_of(j * steps, steps), n)
        out_ref[:, cols] = jnp.dot(turned_ref[:], rhs_ref[:, cols], preferred_element_type=F32)

    far = i < pl.num_programs(0) // HALVES
    for mine, out_ref in ((far, far_ref), (~far, near_ref)):
        @pl.when(mine)
        def _():
            @pl.loop(0, whole)
            def _(j):
                product(j, steps, out_ref)

            product(whole, width - whole * steps, out_ref)
            out_ref[:, lane(width // LANES - 1)] += tail_ref[:]


def weight_grad_cut(lhs_a, lhs_b, tail, rhs_a, rhs_b, order):
    half, height = lhs_a.shape
    width = rhs_a.shape[1]
    n = order.shape[0]
    blk = height // n
    left = pl.BlockSpec((half, blk), lambda i, o: (0, o[i]))
    return pl.pallas_call(
        cut_body,
        grid_spec=pltpu.PrefetchScalarGridSpec(
            num_scalar_prefetch=1, grid=(n,), in_specs=[left, left, pl.BlockSpec((blk, LANES), lambda i, o: (o[i], 0)), HBM, HBM],
            out_specs=[pl.BlockSpec((blk, width), lambda i, o: (jnp.minimum(i, n // HALVES - 1), 0)),
                       pl.BlockSpec((blk, width), lambda i, o: (jnp.maximum(i - n // HALVES, 0), 0))],
            scratch_shapes=[pltpu.VMEM((blk, HALVES * half), BF16), pltpu.VMEM((HALVES * half, width), BF16), pltpu.SemaphoreType.DMA((HALVES, width // 512 + 1))]),
        out_shape=[struct((height // HALVES, width), F32)] * HALVES,
        compiler_params=params(FULL), name="weight_grad_cut", cost_estimate=cost(lhs_a.size * width, lhs_a.size),
    )(order, lhs_a, lhs_b, tail, rhs_a, rhs_b)


def sum_in_steps(far, near, n_dev, beside, hold):
    swap = lambda v, k: lax.ppermute(v, 'fsdp', [(i, i ^ k) for i in range(n_dev)])
    core, x, y = 1, 2, 4
    blocks = lambda v: v.reshape(n_dev // HALVES, -1, v.shape[1])
    at = far.shape[1] // PAIR * LANES
    other = swap(far, core)
    other, = beside(other)
    total = blocks(near) + blocks(other)
    left, right = hold(total[1::2, :, :at], total[2:, :, at:])
    left, right = swap(left, x), swap(right, y)
    keep_left, keep_right = total[::2, :, :at], total[:2, :, at:]
    left, right, keep_left, keep_right = beside(left, right, keep_left, keep_right)
    left, right = keep_left + left, keep_right + right
    last_left, last_right = swap(left[1], y), swap(right[1], x)
    return jnp.concatenate([left[0] + last_left, right[0] + last_right], axis=1)


def beside_body(lhs_a_ref, lhs_b_ref, rhs_a_ref, rhs_b_ref, _, out_ref, turned_ref):
    half = lhs_a_ref.shape[0]

    @pl.when(step_id() == 0)
    def _():
        turned_ref[:, :half] = lhs_a_ref[:].T
        turned_ref[:, half:] = lhs_b_ref[:].T

    prod = jnp.dot(turned_ref[:, :half], rhs_a_ref[:], preferred_element_type=F32)
    prod = prod + jnp.dot(turned_ref[:, half:], rhs_b_ref[:], preferred_element_type=F32)
    out_ref[:] = prod.reshape(out_ref.shape)


def weight_grad_beside(big, at, lhs_a, lhs_b, rhs_a, rhs_b, n_dev):
    half, height = lhs_a.shape
    rows, width = big.shape
    part = width - at
    parts = rhs_a.shape[1] // part
    big = big.reshape(n_dev, rows // n_dev, width)
    right = pl.BlockSpec((half, part), lambda q: (0, q))
    return pl.pallas_call(
        beside_body, grid=(parts,), in_specs=[whole_spec(lhs_a.shape)] * 2 + [right, right, HBM],
        out_specs=pl.BlockSpec((n_dev, height // n_dev, part), lambda q: (0, q, at // part)), out_shape=struct(big.shape, F32),
        scratch_shapes=[pltpu.VMEM((height, HALVES * half), BF16)], input_output_aliases={4: 0}, compiler_params=params(LARGE), name="weight_grad_beside",
        cost_estimate=cost(lhs_a.size * rhs_a.shape[1], lhs_a.size),
    )(lhs_a, lhs_b, rhs_a, rhs_b, big).reshape(rows, width)


def move_body(count_ref, from_ref, to_ref, x_ref, out_ref, sems):
    depth = sems.shape[0]

    @pl.loop(0, count_ref.shape[0])
    def _(o):
        n = count_ref[o]

        def copy(i):
            return pltpu.make_async_copy(x_ref.at[pl.ds(from_ref[o] + i, 1)], out_ref.at[pl.ds(to_ref[o] + i, 1)], sems.at[lax.rem(i, depth)])

        @pl.loop(0, n)
        def _(i):
            @pl.when(i >= depth)
            def _():
                copy(i - depth).wait()

            copy(i).start()

        @pl.loop(jnp.maximum(n - depth, 0), n)
        def _(i):
            copy(i).wait()


def move_rows(x, count, start_from, start_to, n_out):
    return pl.pallas_call(
        move_body, out_shape=struct((n_out,) + x.shape[1:], x.dtype),
        in_specs=[SCALARS] * 3 + [HBM], out_specs=HBM, scratch_shapes=[pltpu.SemaphoreType.DMA((16,))],
        name="move_rows")(count, start_from, start_to, x)


def rms_scale(in_vals, gain_vec):
    vals_f32 = in_vals.astype(F32)
    inv_rms = lax.rsqrt(jnp.mean(vals_f32 * vals_f32, axis=-1, keepdims=True) + RMS_EPS)
    return (vals_f32 * inv_rms * gain_vec).astype(BF16)


def dot(a, b, dims):
    return lax.dot_general(a, b, dims, preferred_element_type=F32)


NN = (((1,), (0,)), ((), ()))


def pack_body(o_ref, q_ref, down_ref, tail_ref, out_ref):
    low = low_lanes()
    start, width = o_ref.shape[1] // LANES, q_ref.shape[1] // LANES
    out_ref[:, lane(0, start)] = o_ref[:]
    for j in range(0, width, 3):
        one, two, three = (q_ref[:, lane(j + k)].astype(F32) for k in range(3))
        out_ref[:, lane(start + j)] = one.astype(BF16)
        out_ref[:, lane(start + j + 1)] = jnp.where(low, rotate(two, ROPE_DIM), rotate(three, ROPE_DIM)).astype(BF16)
        out_ref[:, lane(start + j + 2)] = jnp.where(low, two, three).astype(BF16)
    out_ref[:, lane(start + width, down_ref.shape[1] // LANES)] = down_ref[:]
    out_ref[:, lane(out_ref.shape[1] // LANES - 1)] = tail_ref[:]


def pack_weights(w_out, w_query, w_kv_down, gains):
    rows, width = w_query.shape
    cut = w_kv_down.shape[1] // LANES * LANES
    tail = jnp.concatenate([w_kv_down[:, cut:]] + [jnp.pad(g, (0, rows - g.shape[0]))[:, None] for g in gains], axis=1)
    tail = jnp.pad(tail, ((0, 0), (0, LANES - tail.shape[1])))
    return pl.pallas_call(pack_body, out_shape=struct((rows, w_out.shape[1] + width + cut + LANES), BF16),
                          name="pack_weights")(w_out, w_query, w_kv_down[:, :cut], tail)


def unpack_body(g_ref, q_ref, down_ref):
    low = low_lanes()
    width = q_ref.shape[1] // LANES
    for j in range(0, width, 3):
        plain, rot = rotate(g_ref[:, lane(j + 1)], ROPE_DIM), g_ref[:, lane(j + 2)]
        q_ref[:, lane(j)] = g_ref[:, lane(j)]
        q_ref[:, lane(j + 1)] = jnp.where(low, rot, plain)
        q_ref[:, lane(j + 2)] = jnp.where(low, plain, rot)
    down_ref[:] = g_ref[:, q_ref.shape[1]:q_ref.shape[1] + down_ref.shape[1]]


def unpack_grads(g_x, q_width, down_width):
    rows = g_x.shape[0]
    return pl.pallas_call(unpack_body, out_shape=[struct((rows, q_width), F32), struct((rows, down_width), F32)], name="unpack_grads")(g_x)


def share_body(n_dev, x_ref, out_ref, send_sems, recv_sems):
    place = lax.axis_index('fsdp')
    for m in range(n_dev):
        @pl.when(place == m)
        def _():
            copies = [pltpu.make_async_remote_copy(x_ref, out_ref.at[m], send_sems.at[d], recv_sems.at[m], device_id={'fsdp': d}, device_id_type=pl.DeviceIdType.MESH)
                      for d in range(n_dev) if d != m]
            for copy in copies:
                copy.start()
            out_ref[m] = x_ref[:]
            for copy in copies:
                copy.wait_send()
            for s in range(n_dev):
                if s != m:
                    pltpu.make_async_remote_copy(x_ref, out_ref.at[s], send_sems.at[s], recv_sems.at[s], device_id={'fsdp': s}, device_id_type=pl.DeviceIdType.MESH).wait_recv()


def share(x, n_dev):
    vmem = pl.BlockSpec(memory_space=pltpu.VMEM)
    wide = pltpu.SemaphoreType.DMA((n_dev,))
    return pl.pallas_call(functools.partial(share_body, n_dev), out_shape=struct((n_dev,) + x.shape, x.dtype), in_specs=[vmem], out_specs=vmem,
                          scratch_shapes=[wide, wide], compiler_params=pltpu.CompilerParams(has_side_effects=True), name="share")(x)


def solution(mesh):
    n_dev = mesh.shape['fsdp']
    tok_spec = P(('dp', 'fsdp'), None)
    seq_spec = P(('dp', 'fsdp'), None, None)
    part_vec = P(('dp', 'fsdp'))
    vec_spec = P('fsdp')
    mat_spec = P('fsdp', None)

    def step(tok_ids, grad_out, emb_table, norm_gain, w_query, w_kv_down, kv_gain, w_kv_up, w_out):
        seq_count, seq_len = tok_ids.shape
        vocab_dev, d_model = emb_table.shape
        tok = seq_count * seq_len
        half = tok // HALVES
        per_half = seq_count // HALVES
        me = lax.axis_index('fsdp')
        gather = lambda piece: lax.all_gather(piece, 'fsdp', tiled=True)
        scatter = lambda full: lax.psum_scatter(full, 'fsdp', scatter_dimension=0, tiled=True)
        tie = lax.optimization_barrier
        rows_dev, q_width = w_query.shape
        rank_dev, = kv_gain.shape
        kv_rank = rank_dev * n_dev
        pe_at = q_width + kv_rank
        pad_at = pe_at + ROPE_DIM
        dy = grad_out.reshape(tok, d_model)
        w_ox = gather(pack_weights(w_out, w_query, w_kv_down, (norm_gain, kv_gain)))

        base, extra = [-(-round(half * share) // CHUNK) * CHUNK for share in (0.09, 0.31)]
        n_slots = n_dev * base + extra
        uniq, rank = unique_rows(tok_ids.reshape(HALVES, half))
        all_uniq = share(uniq.reshape(-1, LANES), n_dev).reshape(n_dev, HALVES, half)
        below = lambda lists, edges: jnp.sum(lists[..., None, :] < edges[:, None], axis=-1, dtype=jnp.int32)
        starts = below(all_uniq, jnp.arange(n_dev + 1, dtype=jnp.int32) * vocab_dev)
        counts = starts[..., 1:] - starts[..., :-1]
        fits = jnp.all(counts <= jnp.asarray([base + extra] + [base] * (n_dev - 1), jnp.int32))
        lists = jnp.swapaxes(all_uniq, 0, 1).reshape(HALVES * n_dev, half) - me * vocab_dev
        edges = below(lists, jnp.arange(vocab_dev // TABLE_BLOCK + 1, dtype=jnp.int32) * TABLE_BLOCK)
        my_starts, named = (lax.dynamic_index_in_dim(v, me, keepdims=False) for v in (starts[..., :-1], counts))
        place = jnp.arange(half, dtype=jnp.int32)
        begun = place[:, None] >= my_starts[:, None, 1:]
        slot = place + jnp.sum(jnp.where(begun, base - named[:, None, :-1], 0), axis=-1)
        slot = jnp.where((place >= base) & ~begun[..., 0], place + (n_dev - 1) * base, slot)
        slot = jnp.where(fits, slot, place)
        slots = jnp.arange(n_dev, dtype=jnp.int32) * half
        (rank_a, rank_b), (slot_a, slot_b) = rank, slot

        base_a, base_b, *extras = pick_rows(emb_table, lists, edges, n_dev, base, extra)
        extras_a, extras_b = extras[:n_dev], extras[n_dev:]

        def fetch_any(h):
            mine = slice(h * n_dev, (h + 1) * n_dev)
            far, = pick_rows(emb_table, lists[mine], edges[mine], n_dev, half, 0)
            far, prod = exchange(far, [], n_dev, dy, w_ox)
            return move_rows(far, named[h], slots, my_starts[h], n_slots), prod

        recv, d_mix = lax.cond(fits, lambda: tuple(exchange(base_a, extras_a, n_dev, dy, w_ox)), lambda: fetch_any(0))
        recv, w_ox, w_kv_up, base_b, extras_b = tie((recv, w_ox, w_kv_up, base_b, extras_b))
        w_o, w_x = w_ox[:, :d_model], w_ox[:, d_model:]
        w_up = gather(w_kv_up)
        pieces = fetch_beside(base_b, extras_b)
        gain_vec = w_x[:, pad_at].astype(F32)
        kv_gain_vec = w_x[:, pad_at + 1].reshape(n_dev, rows_dev)[:, :rank_dev].reshape(kv_rank).astype(F32)

        def compute(h, x):
            qx = dot(x, w_x, NN).astype(BF16)
            latent = rms_scale(qx[:, q_width:pe_at], kv_gain_vec)
            kv = dot(latent, w_up, NN).astype(BF16)
            return (qx, latent) + tuple(attend(qx, kv, d_mix, h * per_half, per_half, pe_at // LANES))

        def descend(qx, d_qx, d_kv, d_pe):
            d_latent = dot(d_kv, w_up, COL_DIMS).astype(BF16)
            return latent_back(d_latent, qx, d_pe, kv_gain_vec, d_qx, q_width)

        h0_a, x_a = spread_rows([(recv, 0, None)], rank_a, slot_a, gain_vec, n_slots)
        qx_a, latent_a, mix_a, d_qx_a, d_kv_a, d_pe_a = compute(0, x_a)
        d_qx_a, kv_gain_a = descend(qx_a, d_qx_a, d_kv_a, d_pe_a)
        d_x = dot(d_qx_a, w_x, COL_DIMS).astype(BF16)
        *merged_a, gain_a = merge_rows(d_x, h0_a, dy, 0, gain_vec, rank_a, slot_a, n_dev * base, extra)
        (extra_a, via), got_a = bring_beside(merged_a[1], n_dev), base_beside(merged_a[0])

        pieces, gain_a = tie((pieces, gain_a))
        h0_b, x_b = lax.cond(
            fits, lambda v: spread_rows([(v[0], 0, None)] + [(p, n_dev * base, d) for d, p in enumerate(v[1:])], rank_b, slot_b, gain_vec, n_slots),
            lambda v: spread_rows([(fetch_any(1)[0], 0, None)], rank_b, slot_b, gain_vec, n_slots), pieces)
        qx_b, latent_b, mix_b, d_qx_b, d_kv_b, d_pe_b = compute(1, x_b)
        via, d_kv_b = tie((via, d_kv_b))
        extra_a = extra_a + [lax.ppermute(via, 'fsdp', [(n_dev // 2 - 1, 0)])]
        d_qx_b, kv_gain_b = descend(qx_b, d_qx_b, d_kv_b, d_pe_b)
        d_x = dot(d_qx_b, w_x, COL_DIMS).astype(BF16)
        *merged_b, gain_b = merge_rows(d_x, h0_b, dy, half, gain_vec, rank_b, slot_b, n_dev * base, extra)
        extra_b, via = bring_beside(merged_b[1], n_dev)

        mix_a, gain_b = tie((mix_a, gain_b))
        d_w_o = weight_grad(mix_a, mix_b, dy, more=w_up.size // d_model)
        d_w_o = weight_grad_beside(d_w_o, d_model, latent_a, latent_b, d_kv_a, d_kv_b, n_dev)
        g_o = scatter(d_w_o)
        x_a, d_w_o, merged_b[0], got_a = tie((x_a, d_w_o, merged_b[0], got_a))
        got_b = base_beside(merged_b[0])
        kv_rows = jnp.pad((kv_gain_a + kv_gain_b).reshape(n_dev, rank_dev), ((0, 0), (0, rows_dev - rank_dev)))
        tail = jnp.stack([(gain_a + gain_b).reshape(d_model), kv_rows.reshape(d_model)], axis=1)
        tail = jnp.pad(tail, ((0, 0), (ROPE_DIM, LANES - ROPE_DIM - HALVES)))
        steps = jnp.arange(n_dev, dtype=jnp.int32)
        order = me ^ (jnp.where(steps < n_dev // HALVES, HALVES * steps + 1, HALVES * steps - n_dev))
        far, near = weight_grad_cut(x_a, x_b, tail, d_qx_a, d_qx_b, order)
        via, far = tie((via, far))
        extra_b = extra_b + [lax.ppermute(via, 'fsdp', [(n_dev // HALVES - 1, 0)])]

        def bring_any(h, merged):
            far = move_rows(jnp.concatenate(merged, axis=0), named[h], my_starts[h], slots, n_dev * half)
            return exchange(far, [], n_dev, dy, w_ox)[0]

        made, rows_b = [], [(got_b, extra_b)]

        def hold(left, right):
            left, right, rows_b[0] = tie((left, right, rows_b[0]))
            return left, right

        def beside(*values):
            if not made:
                h0, mix, *values = tie((h0_a, mix_a, far))[:2] + tuple(values)
                outs = [(h0.astype(F32) + dot(mix, w_o, NN)).astype(BF16), (h0_b.astype(F32) + dot(mix_b, w_o, NN)).astype(BF16)]
                *outs, values[0] = tie((*outs, values[0]))
                made.append(jnp.concatenate(outs, axis=0))
            else:
                values = list(values)
                edges_now, values[2] = tie((edges, values[2]))
                made.append(lax.cond(
                    fits, lambda: add_rows([(got_a, base, base, extra_a), (rows_b[0][0], base, base, rows_b[0][1])], lists, edges_now, n_dev, vocab_dev),
                    lambda: add_rows([(bring_any(h, v), half, half, []) for h, v in enumerate((merged_a, merged_b))], lists, edges_now, n_dev, vocab_dev)))
                made[1], values[0] = tie((made[1], values[0]))
            return values

        g_x = sum_in_steps(far, near, n_dev, beside, hold)
        out, grad_table = made
        g_up = jnp.swapaxes(g_o[:, d_model:].reshape(-1, rank_dev, g_o.shape[1] - d_model), 0, 1).reshape(w_kv_up.shape)
        g_query, g_down = unpack_grads(g_x, q_width, pad_at - q_width)
        return (out.reshape(seq_count, seq_len, d_model), grad_table, g_x[:, pad_at], g_query,
                g_down, g_x[:rank_dev, pad_at + 1], g_up, g_o[:, :d_model])

    return jax.shard_map(step, mesh=mesh, in_specs=(tok_spec, seq_spec, mat_spec, vec_spec, mat_spec, mat_spec, vec_spec, mat_spec, mat_spec), out_specs=(seq_spec, tok_spec, part_vec, tok_spec, tok_spec, part_vec, tok_spec, tok_spec), check_vma=False)
```
